128 devices in a mesh: scan: 32 (over z, y, core), grp: 4 (over x).
Axes of the slice: x: 4, y: 4, z: 4, core: 2. Of those that a mesh axis runs over, the one named last changes fastest.
Arguments:
- samples: float32 [512, 64, 6, 128], P('scan', 'grp'), may hold values from -6 to 6
- point_count: int32 [512], P('scan'), may hold values from 4096 to 8192
- corr_scan: int32 [512, 64], P('scan', 'grp'), may hold values from 0 to 511, as said below
- corr_tile: int32 [512, 64], P('scan', 'grp'), may hold values from 0 to 63
- corr_src: int32 [512, 64, 128], P('scan', 'grp'), may hold values from 0 to 2047
Outputs:
- hessian: float32 [512, 6, 6, 512], P('scan', None, None, 'grp')
- gradient: float32 [512, 6], P(('scan', 'grp'))
The draws below stay inside these ranges and needn't reach their ends.
Inputs may be any that keep to these rules, and one draw needn't show every extreme that they name: Never the scan of the entry's own row. A named tile is held by the device with scan index corr_scan // 16 and grp index corr_tile // 16; the 256 entries of one device name at most 4 tiles held by any one device, and in every draw some device is named exactly 4 times by every device.
All inputs are finite; a program needn't handle non-finite values.
Results may differ from the reference program's by a relative error of at most 0.00021.
Values sent between devices are 32-bit elements; how exact they have to be, the bound alone decides.
A program may use at most 64 MiB of HBM per device.

```python
import jax
import jax.numpy as jnp
from jax import lax

SCAN_LOC = 16
TILES_G = 16
CT = 16
SCANS = 512
TILES = 64
N_SCAN = 32
N_GRP = 4
DEVICES = 128


def pair_plan(key):
    half_count = DEVICES // 2
    slot_cap = 2 * SCAN_LOC * CT // DEVICES
    request_count = SCAN_LOC * CT
    hub_device = jax.random.randint(jax.random.fold_in(key, 1), (), 0, DEVICES)

    def one_device(device):
        dev_key = jax.random.fold_in(key, device + 100)

        def one_round(round_idx):
            round_key = jax.random.fold_in(dev_key, round_idx)
            shuffled = jax.random.permutation(round_key, DEVICES - 1) + 1
            offsets = jnp.concatenate([jnp.zeros((1,), jnp.int32), shuffled[:half_count - 1].astype(jnp.int32)])
            return (hub_device + offsets) % DEVICES
        destination = jax.vmap(one_round)(jnp.arange(slot_cap)).reshape(request_count)
        own_index = device // N_GRP
        dest_index = destination // N_GRP
        dest_group = destination % N_GRP
        local_scan = jnp.arange(request_count) // CT
        chosen = jax.random.randint(jax.random.fold_in(dev_key, 5000), (request_count,), 0, SCAN_LOC)
        clashes = (dest_index == own_index) & (chosen == local_scan)
        chosen = jnp.where(clashes, (chosen + 1) % SCAN_LOC, chosen)
        target_scan = dest_index * SCAN_LOC + chosen
        tile_ids = dest_group * TILES_G + jax.random.randint(jax.random.fold_in(dev_key, 6000), (request_count,), 0, TILES_G)
        return (target_scan.astype(jnp.int32), tile_ids.astype(jnp.int32))
    targets, tile_ids = jax.vmap(one_device)(jnp.arange(DEVICES))
    grid_shape = (N_SCAN, N_GRP, SCAN_LOC, CT)
    targets = targets.reshape(grid_shape).transpose(0, 2, 1, 3).reshape(N_SCAN * SCAN_LOC, N_GRP * CT)
    tile_ids = tile_ids.reshape(grid_shape).transpose(0, 2, 1, 3).reshape(N_SCAN * SCAN_LOC, N_GRP * CT)
    return (targets, tile_ids)


def draw_corr_scan(key, part):
    return pair_plan(key)[0]


def draw_corr_tile(key, part):
    return pair_plan(key)[1]


def set_ends(result, stream_key, smallest, top_value):
    longest = result.shape.index(max(result.shape))
    spots = []
    for shift in (0, 1):
        where = [jax.random.randint(jax.random.fold_in(stream_key, axis), (), 0, length) for axis, length in enumerate(result.shape)]
        where[longest] = (where[longest] + shift) % result.shape[longest]
        spots.append(tuple(where))
    return result.at[spots[0]].set(smallest).at[spots[1]].set(top_value)


def steps_of(own_key, extent, pieces, low, high):
    level, own = 1.0, jax.random.fold_in(own_key, 6)
    for dim, blocks in pieces:
        draws = jnp.exp(jax.random.uniform(jax.random.fold_in(own, dim), (blocks,), jnp.float32, low / len(pieces), high / len(pieces)))
        level = level * jnp.repeat(draws, extent[dim] // blocks).reshape([-1 if axis == dim else 1 for axis in range(len(extent))])
    return level


def scatter_about(key, shape, scale, limit, split=(), held_as=jnp.bfloat16):
    array = scale * jax.random.normal(key, shape, jnp.float32)
    if split:
        array = array * steps_of(key, shape, split, -0.22, 0.18)
    return jnp.clip(array, -limit, limit).astype(held_as)


def setup_inputs(seed: int = 0) -> dict:
    seeds = jax.random.split(jax.random.key(seed), 6)
    samples = scatter_about(seeds[0], (SCANS, TILES, 6, 128), 1.0, 6.0, ((0, 32), (1, 4)), jnp.float32)
    point_count = set_ends(jax.random.randint(seeds[1], (SCANS,), TILES_G * N_GRP * 64, TILES_G * N_GRP * 128 + 1), jax.random.fold_in(seeds[1], 1), TILES_G * N_GRP * 64, TILES_G * N_GRP * 128).astype(jnp.int32)
    corr_scan = draw_corr_scan(jax.random.fold_in(seeds[5], 71), 0)
    corr_tile = draw_corr_tile(jax.random.fold_in(seeds[5], 71), 0)
    corr_src = set_ends(jax.random.randint(seeds[4], (SCANS, N_GRP * CT, 128), 0, TILES_G * 128), jax.random.fold_in(seeds[4], 1), 0, (TILES_G * 128) - 1).astype(jnp.int32)
    return {"samples": samples, "point_count": point_count, "corr_scan": corr_scan, "corr_tile": corr_tile, "corr_src": corr_src}


def pair_blocks(pos_x, pos_y, pos_z, source_mask, tile_data):
    diff_x = pos_x - tile_data[:, 0, :]
    diff_y = pos_y - tile_data[:, 1, :]
    diff_z = pos_z - tile_data[:, 2, :]
    normal_x = tile_data[:, 3, :]
    normal_y = tile_data[:, 4, :]
    normal_z = tile_data[:, 5, :]
    residual = normal_x * diff_x + normal_y * diff_y + normal_z * diff_z
    weight = source_mask / (1.0 + residual * residual)
    jacobian = jnp.stack([pos_y * normal_z - pos_z * normal_y, pos_z * normal_x - pos_x * normal_z, pos_x * normal_y - pos_y * normal_x, normal_x, normal_y, normal_z], axis=1)
    blocks = jnp.einsum("nik,njk->nij", jacobian * weight[:, None, :], jacobian, precision=lax.Precision.HIGHEST)
    vectors = jnp.einsum("nik,nk->ni", jacobian, weight * residual, precision=lax.Precision.HIGHEST)
    return blocks.reshape(-1, 36), vectors


def reference(samples, point_count, corr_scan, corr_tile, corr_src):
    scan_count = samples.shape[0]
    tile_count = samples.shape[1]
    column_count = corr_scan.shape[1]
    per_group = column_count // N_GRP
    group_points = (tile_count // N_GRP) * 128
    groups = (jnp.arange(column_count) // per_group).astype(jnp.int32)
    point_ids = groups[None, :, None] * group_points + corr_src
    flat_samples = samples.reshape(scan_count, tile_count * 768)
    offsets = ((point_ids // 128) * 768 + point_ids % 128).reshape(scan_count, column_count * 128)
    coords = [jnp.take_along_axis(flat_samples, offsets + axis_id * 128, axis=1).reshape(-1, 128) for axis_id in range(3)]
    source_mask = (point_ids < point_count[:, None, None]).astype(jnp.float32).reshape(-1, 128)
    target_scan = corr_scan.reshape(-1)
    target_tile = corr_tile.reshape(-1)
    tile_data = samples[target_scan, target_tile]
    row_ids = jnp.arange(128).astype(jnp.int32)
    target_mask = ((target_tile[:, None] * 128 + row_ids[None, :]) < point_count[target_scan][:, None]).astype(jnp.float32)
    tile_data = jnp.concatenate([tile_data[:, 0:3, :], tile_data[:, 3:6, :] * target_mask[:, None, :]], axis=1)
    blocks, vectors = pair_blocks(coords[0], coords[1], coords[2], source_mask, tile_data)
    source_scan = (jnp.arange(scan_count * column_count) // column_count).astype(jnp.int32)
    pairwise = jnp.zeros((scan_count, scan_count, 36), jnp.float32)
    pairwise = pairwise.at[source_scan, source_scan].add(blocks)
    pairwise = pairwise.at[target_scan, target_scan].add(blocks)
    pairwise = pairwise.at[source_scan, target_scan].add(-blocks)
    pairwise = pairwise.at[target_scan, source_scan].add(-blocks)
    hessian = pairwise.reshape(scan_count, scan_count, 6, 6).transpose(0, 2, 3, 1)
    gradient = jnp.zeros((scan_count, 6), jnp.float32)
    gradient = gradient.at[source_scan].add(vectors).at[target_scan].add(-vectors)
    return hessian, gradient
```

```python
import functools

import jax
import jax.numpy as jnp
from jax import lax
from jax.experimental import pallas as pl
from jax.experimental.pallas import tpu as pltpu
from jax.sharding import PartitionSpec as P

F32 = jnp.float32
BF16 = jnp.bfloat16
I32 = jnp.int32
MESH = pl.DeviceIdType.MESH

NS = 32
NG = 4
ND = NS * NG
LOC = 16
TL = 16
CT = 16
REQ = LOC * CT
CAP = 4
STRIDE = 16
USED = 13
FAR = 1000.0
LANES = 128
PAIRS = [(i, j) for i in range(6) for j in range(i, 6)]
PAIR_AT = {}
for _n, (_i, _j) in enumerate(PAIRS):
    PAIR_AT[(_i, _j)] = _n
    PAIR_AT[(_j, _i)] = _n
SUMS = 27
L_SRC, L_DST, L_TILE = 27, 28, 29


def iota(shape, dim):
    return lax.broadcasted_iota(I32, shape, dim)


def dot(a, b):
    return lax.dot_general(a, b, (((1,), (0,)), ((), ())), preferred_element_type=F32)


def parts_of(x, count):
    terms = []
    for _ in range(count):
        term = x.astype(BF16)
        terms.append(term)
        x = x - term.astype(F32)
    return terms


def onehot(cond):
    return jnp.where(cond, 1.0, 0.0).astype(BF16)


def pick_points(pc_ref, src_ref, sm_ref, pay_ref, group):
    first = group * (TL * LANES)

    @pl.loop(0, LOC)
    def _(s):
        picks = src_ref[s]
        tile = lax.shift_right_logical(picks, 7)
        lane = lax.bitwise_and(picks, 127)
        acc = [jnp.zeros((CT, LANES), F32) for _ in range(3)]
        for t in range(TL):
            here = tile == t
            for x in range(3):
                row = jnp.broadcast_to(sm_ref[s, t, pl.ds(x, 1), :], (CT, LANES))
                got = jnp.take_along_axis(row, lane, axis=1, mode="promise_in_bounds")
                acc[x] = jnp.where(here, got, acc[x])
        acc[0] = jnp.where(first + picks < pc_ref[s], acc[0], FAR)
        at = pl.multiple_of(s * CT, CT)
        for x in range(3):
            for n, term in enumerate(parts_of(acc[x], 3)):
                pay_ref[pl.ds(n * REQ + at, CT), x * LANES : (x + 1) * LANES] = term


def pack(cs_ref, ct_ref, pay_ref, msg_ref):
    cs = cs_ref[...]
    ct = ct_ref[...]
    dest = (lax.shift_right_logical(cs, 4) * NG + lax.shift_right_logical(ct, 4)).astype(F32)
    code = (lax.bitwise_and(cs, 15) * TL + lax.bitwise_and(ct, 15) + 1).astype(F32)
    wide = dot(dest.astype(BF16), onehot(iota((CT, REQ), 1) % CT == iota((CT, REQ), 0)))
    wide = jnp.where(iota((LOC, REQ), 1) // CT == iota((LOC, REQ), 0), wide, 0.0)
    dest_t = dot(jnp.ones((ND, LOC), BF16), wide.astype(BF16))
    to_me = dest_t == iota((ND, REQ), 0).astype(F32)
    rank = dot(onehot(to_me), onehot(iota((REQ, REQ), 0) < iota((REQ, REQ), 1)))
    takes = [onehot(to_me & (rank == float(r))) for r in range(CAP)]
    tall = dot(onehot(iota((REQ, LOC), 0) // CT == iota((REQ, LOC), 1)), code.astype(BF16))
    tall = jnp.where(iota((REQ, CT), 0) % CT == iota((REQ, CT), 1), tall, 0.0)
    code_b = dot(tall.astype(BF16), jnp.ones((CT, LANES), BF16))
    place = iota((REQ, LANES), 1) % 32
    target = lax.shift_right_logical(code_b.astype(I32) - 1, 4).astype(F32)
    source = (iota((REQ, LANES), 0) // CT).astype(F32)
    codes = jnp.where(place == L_SRC, source, 0.0)
    codes = jnp.where(place == L_DST, target, codes)
    codes = jnp.where(place == L_TILE, code_b, codes).astype(BF16)
    slot_of_lane = iota((ND, LANES), 1) // 32
    row = jnp.zeros((ND, LANES), F32)
    for r in range(CAP):
        row = jnp.where(slot_of_lane == r, dot(takes[r], codes), row)
    msg_ref[pl.ds(12, ND, stride=STRIDE), :] = row
    for r in range(CAP):
        got = dot(jnp.concatenate([takes[r]] * 3, axis=1), pay_ref[...])
        for x in range(3):
            msg_ref[pl.ds(x * CAP + r, ND, stride=STRIDE), :] = got[:, x * LANES : (x + 1) * LANES]


def pack_kernel(pc_ref, cs_ref, ct_ref, src_ref, sm_ref, msg_ref, pay_ref):
    pick_points(pc_ref, src_ref, sm_ref, pay_ref, lax.axis_index("grp"))
    pack(cs_ref, ct_ref, pay_ref, msg_ref)


def where_is(device):
    return (device // NG, device % NG)


def exchange_kernel(msg_ref, out_ref, send_sem, recv_sem, own_sem):
    me = lax.axis_index("scan") * NG + lax.axis_index("grp")
    barrier = pltpu.get_barrier_semaphore()

    @pl.loop(1, ND)
    def _(step):
        pl.semaphore_signal(barrier, inc=1, device_id=where_is((me + step) % ND), device_id_type=MESH)

    own = pltpu.make_async_copy(
        msg_ref.at[pl.ds(me * STRIDE, STRIDE)], out_ref.at[pl.ds(me * STRIDE, STRIDE)], own_sem
    )
    own.start()
    pl.semaphore_wait(barrier, ND - 1)

    def copy(to, sem_from):
        return pltpu.make_async_remote_copy(
            src_ref=msg_ref.at[pl.ds(to * STRIDE, STRIDE)],
            dst_ref=out_ref.at[pl.ds(sem_from * STRIDE, STRIDE)],
            send_sem=send_sem.at[to],
            recv_sem=recv_sem.at[sem_from],
            device_id=where_is(to),
            device_id_type=MESH,
        )

    @pl.loop(1, ND)
    def _(step):
        copy((me + step) % ND, me).start()

    @pl.loop(1, ND)
    def _(step):
        other = (me + step) % ND
        copy(other, me).wait_send()
        copy(other, other).wait_recv()

    own.wait()


def tile_table(pc_ref, sm_ref, rows_ref, table_ref, group):
    for s in range(LOC):
        for t in range(TL):
            rows_ref[pl.ds((s * TL + t) * 8, 6), :] = sm_ref[s, t]
    point = (group * TL + iota((TL, LANES), 0)) * LANES + iota((TL, LANES), 1)

    @pl.loop(0, LOC)
    def _(s):
        valid = point < pc_ref[s]
        at = pl.multiple_of(s * TL, TL)
        for x in range(6):
            value = rows_ref[pl.ds(s * TL * 8 + x, TL, stride=8), :]
            if x >= 3:
                value = jnp.where(valid, value, 0.0)
            for n, term in enumerate(parts_of(value, 3)):
                table_ref[pl.ds(n * LOC * TL + at, TL), x * LANES : (x + 1) * LANES] = term


def fetch_tiles(msg_ref, table_ref, got_ref):
    codes = msg_ref[pl.ds(12, ND, stride=STRIDE), :]
    for r in range(CAP):
        lane = r * 32 + L_TILE
        wanted = jnp.broadcast_to(codes[:, lane : lane + 1], (ND, LOC * TL))
        take = onehot(wanted == (iota((ND, LOC * TL), 1) + 1).astype(F32))
        got_ref[pl.ds(r * ND, ND), :] = dot(jnp.concatenate([take] * 3, axis=1), table_ref[...])


def tile_sums(msg_ref, got_ref, sums_ref):
    @pl.loop(0, ND // 8)
    def _(block):
        lane = iota((8, LANES), 1)
        at = pl.multiple_of(block * 8, 8)
        bits = [lax.bitwise_and(lane, 1 << b) == 0 for b in range(7)]

        def combine(a, b, level):
            if a is None and b is None:
                return None
            clear = bits[level]
            if b is None:
                return jnp.where(clear, a, 0.0) + pltpu.roll(jnp.where(clear, 0.0, a), 1 << level, 1)
            return jnp.where(clear, a, b) + pltpu.roll(jnp.where(clear, b, a), 1 << level, 1)

        def tree(make, first, count_log, level0):
            if count_log == 0:
                return make(first)
            step = 1 << (count_log - 1)
            return combine(
                tree(make, first, count_log - 1, level0),
                tree(make, first + step, count_log - 1, level0),
                level0 + count_log - 1,
            )

        def slot(r):
            p = [msg_ref[pl.ds(block * (8 * STRIDE) + x * CAP + r, 8, stride=STRIDE), :] for x in range(3)]
            tile = [got_ref[pl.ds(r * ND + at, 8), x * LANES : (x + 1) * LANES] for x in range(6)]
            counts = p[0] < 0.5 * FAR
            p[0] = jnp.where(counts, p[0], 0.0)
            n = tile[3:]
            res = n[0] * (p[0] - tile[0]) + n[1] * (p[1] - tile[1]) + n[2] * (p[2] - tile[2])
            w = jnp.where(counts, 1.0 / (1.0 + res * res), 0.0)
            jac = [
                p[1] * n[2] - p[2] * n[1],
                p[2] * n[0] - p[0] * n[2],
                p[0] * n[1] - p[1] * n[0],
                n[0],
                n[1],
                n[2],
            ]
            wj = [w * j for j in jac]

            def make(k):
                if k < 21:
                    i, j = PAIRS[k]
                    return wj[i] * jac[j]
                if k < SUMS:
                    return wj[k - 21] * res
                return None

            return tree(make, 0, 5, 0)

        total = tree(slot, 0, 2, 5)
        codes = msg_ref[pl.ds(block * (8 * STRIDE) + 12, 8, stride=STRIDE), :]
        sums_ref[pl.ds(at, 8), :] = jnp.where(lax.bitwise_and(lane, 31) < SUMS, total, codes)


def sums_kernel(pc_ref, sm_ref, msg_ref, sums_ref, rows_ref, table_ref, got_ref):
    tile_table(pc_ref, sm_ref, rows_ref, table_ref, lax.axis_index("grp"))
    fetch_tiles(msg_ref, table_ref, got_ref)
    tile_sums(msg_ref, got_ref, sums_ref)


def row_sums(out_rows, in_rows):
    lane = iota((LOC, LANES), 1)
    total = jnp.zeros((LOC, LANES), F32)
    for rows, place, sign in ((out_rows, L_SRC, 1.0), (in_rows, L_DST, -1.0)):
        turned = jnp.transpose(rows)
        hot = jnp.concatenate(
            [
                onehot(jnp.broadcast_to(turned[r * 32 + place : r * 32 + place + 1, :], (LOC, ND)) == iota((LOC, ND), 0).astype(F32))
                for r in range(CAP)
            ],
            axis=0,
        )
        each = sum(dot(hot, term) for term in parts_of(rows, 3))
        part = jnp.zeros((LOC, LANES), F32)
        for r in range(CAP):
            part = jnp.where(lane // 32 == r, each[r * LOC : (r + 1) * LOC], part)
        total = total + jnp.where(lax.bitwise_and(lane, 31) < 21, part, sign * part)
    return total


def return_kernel(sums_ref, out_ref, in_ref, part_ref, send_a, recv_a, send_b, recv_b, send_c, recv_c, own_sem):
    row = lax.axis_index("scan")
    col = lax.axis_index("grp")
    barrier = pltpu.get_barrier_semaphore()
    home = row // 8
    lone = home == col

    @pl.loop(0, 32)
    def _(n):
        src_row = 8 * col + n // NG
        src_col = n % NG

        @pl.when(jnp.logical_or(src_row != row, src_col != col))
        def _():
            pl.semaphore_signal(barrier, inc=1, device_id=(src_row, src_col), device_id_type=MESH)

    for step in range(1, NG):
        pl.semaphore_signal(barrier, inc=1, device_id=(row, (col + step) % NG), device_id_type=MESH)
    pl.semaphore_wait(barrier, 32 + 3 - jnp.where(lone, 1, 0))

    def copy_a(to_row, slot):
        return pltpu.make_async_remote_copy(
            src_ref=sums_ref.at[to_row],
            dst_ref=out_ref.at[slot],
            send_sem=send_a.at[to_row],
            recv_sem=recv_a.at[slot],
            device_id=(to_row, home),
            device_id_type=MESH,
        )

    def copy_b(to_col, slot):
        return pltpu.make_async_remote_copy(
            src_ref=sums_ref.at[pl.ds(to_col * 8, 8)],
            dst_ref=in_ref.at[slot],
            send_sem=send_b.at[to_col],
            recv_sem=recv_b.at[slot],
            device_id=(row, to_col),
            device_id_type=MESH,
        )

    def copy_c(to_col, slot):
        return pltpu.make_async_remote_copy(
            src_ref=part_ref.at[col],
            dst_ref=part_ref.at[slot],
            send_sem=send_c.at[to_col],
            recv_sem=recv_c.at[slot],
            device_id=(row, to_col),
            device_id_type=MESH,
        )

    my_slot = (row % 8) * NG + col
    own_a = pltpu.make_async_copy(sums_ref.at[row], out_ref.at[my_slot], own_sem.at[0])
    own_b = pltpu.make_async_copy(sums_ref.at[pl.ds(col * 8, 8)], in_ref.at[col], own_sem.at[1])
    own_b.start()

    @pl.when(lone)
    def _():
        own_a.start()

    @pl.when(jnp.logical_not(lone))
    def _():
        copy_a(row, my_slot).start()

    @pl.loop(1, NS)
    def _(step):
        copy_a((row + step) % NS, my_slot).start()

    for step in range(1, NG):
        copy_b((col + step) % NG, col).start()

    @pl.loop(0, 32)
    def _(n):
        src_row = 8 * col + n // NG
        src_col = n % NG

        @pl.when(jnp.logical_or(src_row != row, src_col != col))
        def _():
            copy_a(row, n).wait_recv()

    @pl.when(lone)
    def _():
        own_a.wait()

    for step in range(1, NG):
        copy_b(col, (col + step) % NG).wait_recv()
    own_b.wait()

    part_ref[col] = row_sums(out_ref[...].reshape(ND, LANES), in_ref[...].reshape(ND, LANES))
    for step in range(1, NG):
        copy_c((col + step) % NG, col).start()

    @pl.when(jnp.logical_not(lone))
    def _():
        copy_a(row, my_slot).wait_send()

    @pl.loop(1, NS)
    def _(step):
        copy_a((row + step) % NS, my_slot).wait_send()

    for step in range(1, NG):
        copy_b((col + step) % NG, col).wait_send()
        copy_c((col + step) % NG, col).wait_send()
        copy_c(col, (col + step) % NG).wait_recv()


def build_kernel(out_ref, in_ref, part_ref, hess_ref, grad_ref, lhs_ref, rhs_ref):
    row = lax.axis_index("scan")
    col = lax.axis_index("grp")
    rows = [out_ref[...], in_ref[...], part_ref[...].reshape(NG * LOC, LANES)]
    rows[2] = jnp.concatenate([rows[2], jnp.zeros((ND - NG * LOC, LANES), F32)], axis=0)
    wide = jnp.concatenate([jnp.transpose(r) for r in rows], axis=1)
    items = 3 * ND
    out_row = iota((CAP * 48, LANES), 0)
    i_of = (out_row % 48) // 8
    j_of = jnp.minimum(out_row % 8, 5)
    low = jnp.minimum(i_of, j_of)
    high = jnp.maximum(i_of, j_of)
    lane_of = low * 6 - (low * (low - 1)) // 2 + (high - low) + 32 * (out_row // 48)
    spread = onehot(lane_of == iota((CAP * 48, LANES), 1))
    values = [dot(spread, term).astype(BF16) for term in parts_of(wide, 2)]
    lane1 = iota((1, ND), 1)
    for r in range(CAP):
        s_at = r * 32 + L_SRC
        b_at = r * 32 + L_DST
        owner = jnp.concatenate(
            [wide[s_at : s_at + 1, :ND], wide[b_at : b_at + 1, ND : 2 * ND], (lane1 % LOC).astype(F32)], axis=1
        )
        for a in range(LOC):
            mine = onehot(owner == float(a))
            for n in range(2):
                lhs_ref[a * 48 : (a + 1) * 48, (n * CAP + r) * items : (n * CAP + r + 1) * items] = (
                    values[n][r * 48 : (r + 1) * 48] * mine
                )
        item = iota((ND, LANES), 0)
        lane = iota((ND, LANES), 1)
        c_out = jnp.broadcast_to(rows[0][:, b_at : b_at + 1], (ND, LANES)) + (16 * (item // 16)).astype(F32)
        c_in = jnp.broadcast_to(rows[1][:, s_at : s_at + 1], (ND, LANES)) + (16 * ((item % 32) // 4)).astype(F32)
        lane_f = lane.astype(F32)
        diag = (lane == item % LOC + LOC * (row % 8)) & (row // 8 == col) & (item < NG * LOC)
        columns = jnp.concatenate(
            [
                jnp.where(c_out == lane_f, -1.0, 0.0),
                jnp.where(c_in == lane_f, -1.0, 0.0),
                jnp.where(diag, 1.0, 0.0),
            ],
            axis=0,
        ).astype(BF16)
        for n in range(2):
            rhs_ref[(n * CAP + r) * items : (n * CAP + r + 1) * items, :] = columns
    block = dot(lhs_ref[...], rhs_ref[...])
    for a in range(LOC):
        for i in range(6):
            at = (a * 6 + i) * 8
            hess_ref[a, i] = block[at : at + 6, :]
    mine = sum(part_ref[n, pl.ds(col * 4, 4), :] for n in range(NG))
    flat = sum(mine[:, r * 32 : (r + 1) * 32] for r in range(CAP))
    grad_ref[...] = flat[:, 21:27]


def vmem(count):
    return [pl.BlockSpec(memory_space=pltpu.VMEM)] * count


def local(samples, point_count, corr_scan, corr_tile, corr_src):
    smem = [pl.BlockSpec(memory_space=pltpu.SMEM)]
    msg = pl.pallas_call(
        pack_kernel,
        out_shape=jax.ShapeDtypeStruct((ND * STRIDE, LANES), F32),
        in_specs=smem + vmem(4),
        out_specs=pl.BlockSpec(memory_space=pltpu.VMEM),
        scratch_shapes=[pltpu.VMEM((3 * REQ, 3 * LANES), BF16)],
        name="pack",
    )(point_count, corr_scan, corr_tile, corr_src, samples)
    recv = pl.pallas_call(
        exchange_kernel,
        out_shape=jax.ShapeDtypeStruct((ND * STRIDE, LANES), F32),
        in_specs=vmem(1),
        out_specs=pl.BlockSpec(memory_space=pltpu.VMEM),
        scratch_shapes=[
            pltpu.SemaphoreType.DMA((ND,)),
            pltpu.SemaphoreType.DMA((ND,)),
            pltpu.SemaphoreType.DMA,
        ],
        compiler_params=pltpu.CompilerParams(collective_id=0, has_side_effects=True),
        name="exchange",
    )(msg)
    sums = pl.pallas_call(
        sums_kernel,
        out_shape=jax.ShapeDtypeStruct((ND, LANES), F32),
        in_specs=smem + vmem(2),
        out_specs=pl.BlockSpec(memory_space=pltpu.VMEM),
        scratch_shapes=[
            pltpu.VMEM((LOC * TL * 8, LANES), F32),
            pltpu.VMEM((3 * LOC * TL, 6 * LANES), BF16),
            pltpu.VMEM((CAP * ND, 6 * LANES), F32),
        ],
        name="sums",
    )(point_count, samples, recv)
    dma = pltpu.SemaphoreType.DMA
    out_rows, in_rows, parts = pl.pallas_call(
        return_kernel,
        out_shape=(
            jax.ShapeDtypeStruct((32, NG, LANES), F32),
            jax.ShapeDtypeStruct((NG, 8, NG, LANES), F32),
            jax.ShapeDtypeStruct((NG, LOC, LANES), F32),
        ),
        in_specs=vmem(1),
        out_specs=tuple(vmem(3)),
        scratch_shapes=[
            dma((NS,)),
            dma((32,)),
            dma((NG,)),
            dma((NG,)),
            dma((NG,)),
            dma((NG,)),
            dma((2,)),
        ],
        compiler_params=pltpu.CompilerParams(collective_id=1, has_side_effects=True),
        name="give_back",
    )(sums.reshape(NS, NG, LANES))
    hessian, gradient = pl.pallas_call(
        build_kernel,
        out_shape=(
            jax.ShapeDtypeStruct((LOC, 6, 6, LANES), F32),
            jax.ShapeDtypeStruct((4, 6), F32),
        ),
        in_specs=vmem(3),
        out_specs=tuple(vmem(2)),
        scratch_shapes=[
            pltpu.VMEM((LOC * 48, 2 * CAP * 3 * ND), BF16),
            pltpu.VMEM((2 * CAP * 3 * ND, LANES), BF16),
        ],
        name="build",
    )(out_rows.reshape(ND, LANES), in_rows.reshape(ND, LANES), parts)
    return hessian, gradient


def solution(mesh):
    placed = (
        P("scan", "grp", None, None),
        P("scan"),
        P("scan", "grp"),
        P("scan", "grp"),
        P("scan", "grp", None),
    )
    return jax.shard_map(
        local,
        mesh=mesh,
        in_specs=placed,
        out_specs=(P("scan", None, None, "grp"), P(("scan", "grp"), None)),
        check_vma=False,
    )
```

```python
import functools

import jax
import jax.numpy as jnp
from jax import lax
from jax.experimental import pallas as pl
from jax.experimental.pallas import tpu as pltpu
from jax.sharding import PartitionSpec as P

F32 = jnp.float32
BF16 = jnp.bfloat16
I32 = jnp.int32
MESH = pl.DeviceIdType.MESH

NS = 32
NG = 4
ND = NS * NG
LOC = 16
TL = 16
CT = 16
REQ = LOC * CT
CAP = 4
ROWS = 13
FAR = 1000.0
LANES = 128
PAIRS = [(i, j) for i in range(6) for j in range(i, 6)]
UNITS = 16
GROUPS = 8
ITEMS = GROUPS * LANES


def iota(shape, dim):
    return lax.broadcasted_iota(I32, shape, dim)


def dot(a, b):
    return lax.dot_general(a, b, (((1,), (0,)), ((), ())), preferred_element_type=F32)


def dot_t(a, b):
    return lax.dot_general(a, b, (((1,), (1,)), ((), ())), preferred_element_type=F32)


def parts_of(x, count):
    terms = []
    for _ in range(count):
        term = x.astype(BF16)
        terms.append(term)
        x = x - term.astype(F32)
    return terms


def onehot(cond):
    return jnp.where(cond, 1.0, 0.0).astype(BF16)


def pick_points(pc_ref, src_ref, sm_ref, pay_ref, group):
    first = group * (TL * LANES)

    @pl.loop(0, LOC)
    def _(s):
        picks = src_ref[s]
        tile = lax.shift_right_logical(picks, 7)
        lane = lax.bitwise_and(picks, 127)
        acc = [jnp.zeros((CT, LANES), F32) for _ in range(3)]
        for t in range(TL):
            here = tile == t
            for x in range(3):
                row = jnp.broadcast_to(sm_ref[s, x, pl.ds(t, 1), :], (CT, LANES))
                got = jnp.take_along_axis(row, lane, axis=1, mode="promise_in_bounds")
                acc[x] = jnp.where(here, got, acc[x])
        acc[0] = jnp.where(first + picks < pc_ref[s], acc[0], FAR)
        at = pl.multiple_of(s * CT, CT)
        for x in range(3):
            for n, term in enumerate(parts_of(acc[x], 3)):
                pay_ref[pl.ds(n * REQ + at, CT), x * LANES : (x + 1) * LANES] = term


def pack(cs_ref, ct_ref, pay_ref, msg_ref, group):
    cs = cs_ref[...]
    ct = ct_ref[...]
    dest = (lax.shift_right_logical(cs, 4) * NG + lax.shift_right_logical(ct, 4)).astype(F32)
    code = (lax.bitwise_and(cs, 15) * TL + lax.bitwise_and(ct, 15) + 1).astype(F32)
    wide = dot(dest.astype(BF16), onehot(iota((CT, REQ), 1) % CT == iota((CT, REQ), 0)))
    wide = jnp.where(iota((LOC, REQ), 1) // CT == iota((LOC, REQ), 0), wide, 0.0)
    dest_t = dot(jnp.ones((ND, LOC), BF16), wide.astype(BF16))
    to_me = dest_t == iota((ND, REQ), 0).astype(F32)
    rank = dot(onehot(to_me), onehot(iota((REQ, REQ), 0) < iota((REQ, REQ), 1)))
    takes = [onehot(to_me & (rank == float(r))) for r in range(CAP)]
    tall = dot(onehot(iota((REQ, LOC), 0) // CT == iota((REQ, LOC), 1)), code.astype(BF16))
    tall = jnp.where(iota((REQ, CT), 0) % CT == iota((REQ, CT), 1), tall, 0.0)
    code_b = dot(tall.astype(BF16), jnp.ones((CT, LANES), BF16))
    target = lax.shift_right_logical(code_b.astype(I32) - 1, 4).astype(F32)
    source = (iota((REQ, LANES), 0) // CT).astype(F32)
    lane = iota((REQ, LANES), 1)
    codes = jnp.where(lane < 32, source, jnp.where(lane < 64, target, code_b)).astype(BF16)
    lane = iota((ND, LANES), 1)
    row = jnp.zeros((ND, LANES), F32)
    for r in range(CAP):
        at = r * 8 + group
        here = (lane == at) | (lane == 32 + at) | (lane == 100 + r * 8)
        row = jnp.where(here, dot(takes[r], codes), row)
    msg_ref[pl.ds(12, ND, stride=ROWS), :] = row
    got = dot(
        jnp.concatenate([jnp.concatenate([take] * 3, axis=1) for take in takes], axis=0), pay_ref[...]
    )
    for r in range(CAP):
        for x in range(3):
            msg_ref[pl.ds(x * CAP + r, ND, stride=ROWS), :] = got[r * ND : (r + 1) * ND, x * LANES : (x + 1) * LANES]


def tile_table(pc_ref, sm_ref, table_ref, group):
    point = (group * TL + iota((TL, LANES), 0)) * LANES + iota((TL, LANES), 1)

    @pl.loop(0, LOC)
    def _(s):
        valid = point < pc_ref[s]
        at = pl.multiple_of(s * TL, TL)
        for x in range(6):
            value = sm_ref[s, x]
            if x >= 3:
                value = jnp.where(valid, value, 0.0)
            for n, term in enumerate(parts_of(value, 3)):
                table_ref[pl.ds(n * LOC * TL + at, TL), x * LANES : (x + 1) * LANES] = term


def unit_sums(at, msg_ref, table_ref, left_ref, right_ref):
    lane = iota((8, LANES), 1)
    sub = iota((8, LANES), 0)
    codes = msg_ref[pl.ds(at + 12, 8, stride=ROWS), :]
    tile_at = (iota((8, LOC * TL), 1) + 1).astype(F32)
    take = jnp.concatenate(
        [
            jnp.where(jnp.broadcast_to(codes[:, 100 + r * 8 : 101 + r * 8], (8, LOC * TL)) == tile_at, 1.0, 0.0)
            for r in range(CAP)
        ],
        axis=0,
    ).astype(BF16)
    tile = dot(jnp.concatenate([take] * 3, axis=1), table_ref[...])
    p = [
        jnp.concatenate([msg_ref[pl.ds(at + x * CAP + r, 8, stride=ROWS), :] for r in range(CAP)], axis=0)
        for x in range(3)
    ]
    q = [tile[:, x * LANES : (x + 1) * LANES] for x in range(3)]
    n = [tile[:, x * LANES : (x + 1) * LANES] for x in range(3, 6)]
    counts = p[0] < 0.5 * FAR
    p[0] = jnp.where(counts, p[0], 0.0)
    res = n[0] * (p[0] - q[0]) + n[1] * (p[1] - q[1]) + n[2] * (p[2] - q[2])
    w = jnp.where(counts, 1.0 / (1.0 + res * res), 0.0)
    jac = [
        p[1] * n[2] - p[2] * n[1],
        p[2] * n[0] - p[0] * n[2],
        p[0] * n[1] - p[1] * n[0],
        n[0],
        n[1],
        n[2],
    ]
    for i in range(6):
        high, low = parts_of(w * jac[i], 2)
        left_ref[i * 32 : (i + 1) * 32, :] = jnp.concatenate([high, high, low], axis=1)
    for j, value in enumerate(jac + [res, jnp.zeros_like(res)]):
        high, low = parts_of(value, 2)
        right_ref[j * 32 : (j + 1) * 32, :] = jnp.concatenate([high, low, high], axis=1)
    every = dot_t(left_ref[...], right_ref[...])
    halves = []
    for half in range(2):
        arrays = []
        for i in range(6):
            kept = jnp.zeros((8, LANES), F32)
            for r in range(CAP):
                block = every[i * 32 + r * 8 : i * 32 + r * 8 + 8, half * LANES : (half + 1) * LANES]
                kept = jnp.where(lane % 32 == r * 8 + sub, block, kept)
            arrays.append(kept)
        arrays += [None, None]
        for level in range(3):
            clear = (sub // (1 << level)) % 2 == 0
            arrays = [fold(arrays[n], arrays[n + 1], clear, 1 << level) for n in range(0, len(arrays), 2)]
        halves.append(arrays[0])
    low, high = halves
    first = (lane // 4) % 2 == 0
    blocks = []
    for c in range(2):
        if c == 0:
            block = jnp.where(first, low, pltpu.roll(high, 4, 1))
        else:
            block = jnp.where(first, pltpu.roll(low, LANES - 4, 1), high)
        code = jnp.sum(jnp.where(sub // 4 == c, codes, 0.0), axis=0, keepdims=True)
        blocks.append(jnp.where(sub == 7, jnp.broadcast_to(code, (8, LANES)), block))
    return blocks


def fold(a, b, clear, shift):
    if a is None:
        return None
    if b is None:
        return jnp.where(clear, a, 0.0) + pltpu.roll(jnp.where(clear, 0.0, a), shift, 0)
    return jnp.where(clear, a, b) + pltpu.roll(jnp.where(clear, b, a), shift, 0)


def turn_groups(load, owner_ref, sums_ref, column_ref):
    lane = iota((8, LANES), 1)
    lane1 = iota((1, LANES), 1)
    which = ((lane1 // 4) % 2) * 4 + ((lane1 // 64) % 2) * 2 + (lane1 // 32) % 2
    for q in range(GROUPS):
        blocks = [load(q, m) for m in range(8)]
        for bit, shift in ((1, 64), (0, 32), (2, 4)):
            clear = (lane // shift) % 2 == 0
            for m in range(8):
                if (m >> bit) % 2 == 0:
                    a, b = blocks[m], blocks[m + (1 << bit)]
                    blocks[m] = jnp.where(clear, a, pltpu.roll(b, shift, 1))
                    blocks[m + (1 << bit)] = jnp.where(clear, pltpu.roll(a, LANES - shift, 1), b)
        source = blocks[0][7:8, :]
        target = blocks[1][7:8, :]
        at = q * LANES
        if q < GROUPS // 2:
            owner = source
            column = target + (16 * (2 * q + which // 4)).astype(F32)
        else:
            owner = target
            column = source + (16 * which).astype(F32)
            blocks[6] = -blocks[6]
        mine = jnp.where(jnp.broadcast_to(owner, (LOC, LANES)) == iota((LOC, LANES), 0).astype(F32), 1.0, 0.0)
        there = jnp.where(jnp.broadcast_to(column, (LANES, LANES)) == iota((LANES, LANES), 0).astype(F32), -1.0, 0.0)
        stack = jnp.concatenate(blocks, axis=0)
        for n, term in enumerate(parts_of(stack, 2)):
            owner_ref[:, n * ITEMS + at : n * ITEMS + at + LANES] = mine.astype(BF16)
            column_ref[:, n * ITEMS + at : n * ITEMS + at + LANES] = there.astype(BF16)
            sums_ref[:, n * ITEMS + at : n * ITEMS + at + LANES] = term


def matrix(owner_ref, sums_ref, column_ref, lhs_ref, block_ref):
    for k, (i, j) in enumerate(PAIRS):
        row = sums_ref[j * 8 + i : j * 8 + i + 1, :]
        lhs_ref[k * LOC : (k + 1) * LOC, :] = jnp.broadcast_to(row, (LOC, 2 * ITEMS)) * owner_ref[...]
    block_ref[...] = dot_t(lhs_ref[...], column_ref[...])


def order(p):
    return 2 * (1 - p % 2) + (p % 2 + p // 2) % 2


def step_kernel(
    pc_ref, cs_ref, ct_ref, src_ref, sm_ref, block_ref, part_ref,
    pay_ref, msg_ref, recv_ref, table_ref, left_ref, right_ref, back_ref, out_ref, in_ref,
    owner_ref, sums_ref, column_ref, lhs_ref,
    send_p, recv_p, send_a, recv_a, send_b, recv_b, send_c, recv_c,
):
    row = lax.axis_index("scan")
    col = lax.axis_index("grp")
    z, y, core = row // 8, (row // 2) % 4, row % 2
    me = row * NG + col
    barrier = pltpu.get_barrier_semaphore()

    @pl.loop(1, ND)
    def _(step):
        other = (me + step) % ND
        pl.semaphore_signal(barrier, inc=1, device_id=(other // NG, other % NG), device_id_type=MESH)

    pick_points(pc_ref, src_ref, sm_ref, pay_ref, col)
    pack(cs_ref, ct_ref, pay_ref, msg_ref, col)
    pl.semaphore_wait(barrier, ND - 1)

    def points(to_row, to_col, at):
        to = to_row * NG + to_col
        return pltpu.make_async_remote_copy(
            src_ref=msg_ref.at[pl.ds(to * ROWS, ROWS)],
            dst_ref=recv_ref.at[pl.ds(at * ROWS, ROWS)],
            send_sem=send_p.at[to],
            recv_sem=recv_p.at[at],
            device_id=(to_row, to_col),
            device_id_type=MESH,
        )

    def each_of_unit(u, sign, act):
        uz = (z + sign * order(u // 4) + 4) % 4
        uy = (y + sign * order(u % 4) + 4) % 4
        for dc in range(2):
            for dx in range(NG):
                there = ((uz * 4 + uy) * 2 + (core + dc) % 2, (col + dx) % NG)
                if dc == 0 and dx == 0:

                    @pl.when(u < UNITS - 1)
                    def _():
                        act(*there)

                else:
                    act(*there)
        return uz * 4 + uy

    own = pltpu.make_async_copy(
        msg_ref.at[pl.ds(me * ROWS, ROWS)], recv_ref.at[pl.ds(me * ROWS, ROWS)], recv_p.at[me]
    )
    own.start()

    @pl.loop(0, UNITS)
    def _(u):
        each_of_unit(u, 1, lambda r, c: points(r, c, me).start())

    tile_table(pc_ref, sm_ref, table_ref, col)

    home = row // 8
    slot = (row % 8) * NG + col

    def give(to_row, at):
        return pltpu.make_async_remote_copy(
            src_ref=back_ref.at[to_row],
            dst_ref=out_ref.at[at],
            send_sem=send_a.at[to_row],
            recv_sem=recv_a.at[at],
            device_id=(to_row, home),
            device_id_type=MESH,
        )

    def share(unit, from_col, at):
        return pltpu.make_async_remote_copy(
            src_ref=back_ref.at[pl.ds(2 * unit, 2)],
            dst_ref=in_ref.at[from_col, pl.ds(2 * at, 2)],
            send_sem=send_b.at[unit],
            recv_sem=recv_b.at[from_col * 4 + at],
            device_id=(row, unit // 4),
            device_id_type=MESH,
        )

    @pl.loop(0, UNITS)
    def _(u):
        unit = each_of_unit(u, -1, lambda r, c: points(r, c, r * NG + c).wait_recv())

        @pl.when(u == UNITS - 1)
        def _():
            own.wait()

        first, second = unit_sums(unit * (8 * ROWS), recv_ref, table_ref, left_ref, right_ref)
        back_ref[2 * unit] = first
        back_ref[2 * unit + 1] = second
        for c in range(2):
            to_row = 2 * unit + c
            lone = jnp.logical_and(to_row == row, home == col)

            @pl.when(jnp.logical_not(lone))
            def _():
                give(to_row, slot).start()

            @pl.when(lone)
            def _():
                pltpu.make_async_copy(back_ref.at[to_row], out_ref.at[slot], recv_a.at[slot]).start()

        @pl.when(unit // 4 != col)
        def _():
            share(unit, col, unit % 4).start()

        @pl.when(unit // 4 == col)
        def _():
            pltpu.make_async_copy(
                back_ref.at[pl.ds(2 * unit, 2)], in_ref.at[col, pl.ds(2 * (unit % 4), 2)], recv_b.at[col * 4 + unit % 4]
            ).start()

    @pl.loop(0, 32)
    def _(n):
        give(row, n).wait_recv()

    @pl.loop(0, UNITS)
    def _(n):
        share(0, n // 4, n % 4).wait_recv()

    def load(q, m):
        return out_ref[q * 8 + m] if q < GROUPS // 2 else in_ref[q - GROUPS // 2, m]

    turn_groups(load, owner_ref, sums_ref, column_ref)
    part = dot_t(owner_ref[...], sums_ref[...])
    part_ref[col] = jnp.concatenate([part, jnp.zeros((LOC, LANES - 64), F32)], axis=1)

    def spread(to_col, at):
        return pltpu.make_async_remote_copy(
            src_ref=part_ref.at[col],
            dst_ref=part_ref.at[at],
            send_sem=send_c.at[to_col],
            recv_sem=recv_c.at[at],
            device_id=(row, to_col),
            device_id_type=MESH,
        )

    for step in range(1, NG):
        spread((col + step) % NG, col).start()

    matrix(owner_ref, sums_ref, column_ref, lhs_ref, block_ref)

    @pl.loop(1, ND)
    def _(step):
        other = (me + step) % ND
        points(other // NG, other % NG, me).wait_send()

    @pl.loop(0, NS)
    def _(n):
        @pl.when(jnp.logical_not(jnp.logical_and(n == row, home == col)))
        def _():
            give(n, slot).wait_send()

    @pl.loop(0, UNITS)
    def _(n):
        @pl.when(n // 4 != col)
        def _():
            share(n, col, n % 4).wait_send()

    for step in range(1, NG):
        other = (col + step) % NG
        spread(other, col).wait_send()
        spread(other, other).wait_recv()


def finish_kernel(block_ref, part_ref, hess_ref, grad_ref):
    row = lax.axis_index("scan")
    col = lax.axis_index("grp")
    total = part_ref[0] + part_ref[1] + part_ref[2] + part_ref[3]
    lane = iota((LOC, LANES), 1)
    diag = (lane == iota((LOC, LANES), 0) + LOC * (row % 8)) & (row // 8 == col)
    for k, (i, j) in enumerate(PAIRS):
        at = j * 8 + i
        value = block_ref[k * LOC : (k + 1) * LOC, :] + jnp.where(
            diag, jnp.broadcast_to(total[:, at : at + 1], (LOC, LANES)), 0.0
        )
        hess_ref[i, j] = value
        if i != j:
            hess_ref[j, i] = value
    some = jnp.zeros((4, LANES), F32)
    for n in range(NG):
        some = jnp.where(col == n, total[n * 4 : (n + 1) * 4, :], some)
    grad_ref[...] = some[:, 48:54]


def vmem(count):
    return [pl.BlockSpec(memory_space=pltpu.VMEM)] * count


def local(samples, point_count, corr_scan, corr_tile, corr_src):
    dma = pltpu.SemaphoreType.DMA
    block, parts = pl.pallas_call(
        step_kernel,
        out_shape=(
            jax.ShapeDtypeStruct((len(PAIRS) * LOC, LANES), F32),
            jax.ShapeDtypeStruct((NG, LOC, LANES), F32),
        ),
        in_specs=[pl.BlockSpec(memory_space=pltpu.SMEM)] + vmem(4),
        out_specs=tuple(vmem(2)),
        scratch_shapes=[
            pltpu.VMEM((3 * REQ, 3 * LANES), BF16),
            pltpu.VMEM((ND * ROWS, LANES), F32),
            pltpu.VMEM((ND * ROWS, LANES), F32),
            pltpu.VMEM((3 * LOC * TL, 6 * LANES), BF16),
            pltpu.VMEM((6 * 32, 3 * LANES), BF16),
            pltpu.VMEM((8 * 32, 3 * LANES), BF16),
            pltpu.VMEM((NS, 8, LANES), F32),
            pltpu.VMEM((32, 8, LANES), F32),
            pltpu.VMEM((NG, 8, 8, LANES), F32),
            pltpu.VMEM((LOC, 2 * ITEMS), BF16),
            pltpu.VMEM((64, 2 * ITEMS), BF16),
            pltpu.VMEM((LANES, 2 * ITEMS), BF16),
            pltpu.VMEM((len(PAIRS) * LOC, 2 * ITEMS), BF16),
            dma((ND,)),
            dma((ND,)),
            dma((NS,)),
            dma((32,)),
            dma((UNITS,)),
            dma((UNITS,)),
            dma((NG,)),
            dma((NG,)),
        ],
        compiler_params=pltpu.CompilerParams(collective_id=0, has_side_effects=True),
        name="step",
    )(point_count, corr_scan, corr_tile, corr_src, samples.transpose(0, 2, 1, 3))
    hessian, gradient = pl.pallas_call(
        finish_kernel,
        out_shape=(
            jax.ShapeDtypeStruct((6, 6, LOC, LANES), F32),
            jax.ShapeDtypeStruct((4, 6), F32),
        ),
        in_specs=vmem(2),
        out_specs=tuple(vmem(2)),
        name="finish",
    )(block, parts)
    return hessian.transpose(2, 0, 1, 3), gradient


def solution(mesh):
    placed = (
        P("scan", "grp", None, None),
        P("scan"),
        P("scan", "grp"),
        P("scan", "grp"),
        P("scan", "grp", None),
    )
    return jax.shard_map(
        local,
        mesh=mesh,
        in_specs=placed,
        out_specs=(P("scan", None, None, "grp"), P(("scan", "grp"), None)),
        check_vma=False,
    )
```

```python
import functools

import jax
import jax.numpy as jnp
from jax import lax
from jax.experimental import pallas as pl
from jax.experimental.pallas import tpu as pltpu
from jax.sharding import PartitionSpec as P

F32 = jnp.float32
BF16 = jnp.bfloat16
I32 = jnp.int32
MESH = pl.DeviceIdType.MESH

NS = 32
NG = 4
ND = NS * NG
LOC = 16
TL = 16
CT = 16
REQ = LOC * CT
CAP = 4
ROWS = 13
FAR = 1000.0
LANES = 128
PAIRS = [(i, j) for i in range(6) for j in range(i, 6)]
UNITS = 16
GROUPS = 8
ITEMS = GROUPS * LANES


def iota(shape, dim):
    return lax.broadcasted_iota(I32, shape, dim)


def dot(a, b):
    return lax.dot_general(a, b, (((1,), (0,)), ((), ())), preferred_element_type=F32)


def dot_t(a, b):
    return lax.dot_general(a, b, (((1,), (1,)), ((), ())), preferred_element_type=F32)


def parts_of(x, count):
    terms = []
    for _ in range(count):
        term = x.astype(BF16)
        terms.append(term)
        x = x - term.astype(F32)
    return terms


def onehot(cond):
    return jnp.where(cond, 1.0, 0.0).astype(BF16)


def pick_points(pc_ref, src_ref, sm_ref, pay_ref, group):
    first = group * (TL * LANES)

    @pl.loop(0, LOC)
    def _(s):
        picks = src_ref[s]
        tile = lax.shift_right_logical(picks, 7)
        lane = lax.bitwise_and(picks, 127)
        acc = [jnp.zeros((CT, LANES), F32) for _ in range(3)]
        for t in range(TL):
            here = tile == t
            for x in range(3):
                row = jnp.broadcast_to(sm_ref[s, x, pl.ds(t, 1), :], (CT, LANES))
                got = jnp.take_along_axis(row, lane, axis=1, mode="promise_in_bounds")
                acc[x] = jnp.where(here, got, acc[x])
        acc[0] = jnp.where(first + picks < pc_ref[s], acc[0], FAR)
        at = pl.multiple_of(s * CT, CT)
        for x in range(3):
            for n, term in enumerate(parts_of(acc[x], 3)):
                pay_ref[pl.ds(n * REQ + at, CT), x * LANES : (x + 1) * LANES] = term


def pack(cs_ref, ct_ref, pay_ref, msg_ref, group):
    cs = cs_ref[...]
    ct = ct_ref[...]
    dest = (lax.shift_right_logical(cs, 4) * NG + lax.shift_right_logical(ct, 4)).astype(F32)
    code = (lax.bitwise_and(cs, 15) * TL + lax.bitwise_and(ct, 15) + 1).astype(F32)
    wide = dot(dest.astype(BF16), onehot(iota((CT, REQ), 1) % CT == iota((CT, REQ), 0)))
    wide = jnp.where(iota((LOC, REQ), 1) // CT == iota((LOC, REQ), 0), wide, 0.0)
    dest_t = dot(jnp.ones((ND, LOC), BF16), wide.astype(BF16))
    to_me = dest_t == iota((ND, REQ), 0).astype(F32)
    rank = dot(onehot(to_me), onehot(iota((REQ, REQ), 0) < iota((REQ, REQ), 1)))
    takes = [onehot(to_me & (rank == float(r))) for r in range(CAP)]
    tall = dot(onehot(iota((REQ, LOC), 0) // CT == iota((REQ, LOC), 1)), code.astype(BF16))
    tall = jnp.where(iota((REQ, CT), 0) % CT == iota((REQ, CT), 1), tall, 0.0)
    code_b = dot(tall.astype(BF16), jnp.ones((CT, LANES), BF16))
    target = lax.shift_right_logical(code_b.astype(I32) - 1, 4).astype(F32)
    source = (iota((REQ, LANES), 0) // CT).astype(F32)
    lane = iota((REQ, LANES), 1)
    codes = jnp.where(lane < 32, source, jnp.where(lane < 64, target, code_b)).astype(BF16)
    lane = iota((ND, LANES), 1)
    row = jnp.zeros((ND, LANES), F32)
    for r in range(CAP):
        at = r * 8 + group
        here = (lane == at) | (lane == 32 + at) | (lane == 100 + r * 8)
        row = jnp.where(here, dot(takes[r], codes), row)
    msg_ref[pl.ds(12, ND, stride=ROWS), :] = row
    got = dot(
        jnp.concatenate([jnp.concatenate([take] * 3, axis=1) for take in takes], axis=0), pay_ref[...]
    )
    for r in range(CAP):
        for x in range(3):
            msg_ref[pl.ds(x * CAP + r, ND, stride=ROWS), :] = got[r * ND : (r + 1) * ND, x * LANES : (x + 1) * LANES]


def tile_table(pc_ref, sm_ref, table_ref, group):
    point = (group * TL + iota((TL, LANES), 0)) * LANES + iota((TL, LANES), 1)

    @pl.loop(0, LOC)
    def _(s):
        valid = point < pc_ref[s]
        at = pl.multiple_of(s * TL, TL)
        for x in range(6):
            value = sm_ref[s, x]
            if x >= 3:
                value = jnp.where(valid, value, 0.0)
            for n, term in enumerate(parts_of(value, 3)):
                table_ref[pl.ds(n * LOC * TL + at, TL), x * LANES : (x + 1) * LANES] = term


def unit_sums(at, msg_ref, table_ref, left_ref, right_ref):
    lane = iota((8, LANES), 1)
    sub = iota((8, LANES), 0)
    codes = msg_ref[pl.ds(at + 12, 8, stride=ROWS), :]
    tile_at = (iota((8, LOC * TL), 1) + 1).astype(F32)
    take = jnp.concatenate(
        [
            jnp.where(jnp.broadcast_to(codes[:, 100 + r * 8 : 101 + r * 8], (8, LOC * TL)) == tile_at, 1.0, 0.0)
            for r in range(CAP)
        ],
        axis=0,
    ).astype(BF16)
    tile = dot(jnp.concatenate([take] * 3, axis=1), table_ref[...])
    p = [
        jnp.concatenate([msg_ref[pl.ds(at + x * CAP + r, 8, stride=ROWS), :] for r in range(CAP)], axis=0)
        for x in range(3)
    ]
    q = [tile[:, x * LANES : (x + 1) * LANES] for x in range(3)]
    n = [tile[:, x * LANES : (x + 1) * LANES] for x in range(3, 6)]
    counts = p[0] < 0.5 * FAR
    p[0] = jnp.where(counts, p[0], 0.0)
    res = n[0] * (p[0] - q[0]) + n[1] * (p[1] - q[1]) + n[2] * (p[2] - q[2])
    w = jnp.where(counts, 1.0 / (1.0 + res * res), 0.0)
    jac = [
        p[1] * n[2] - p[2] * n[1],
        p[2] * n[0] - p[0] * n[2],
        p[0] * n[1] - p[1] * n[0],
        n[0],
        n[1],
        n[2],
    ]
    for i in range(6):
        high, low = parts_of(w * jac[i], 2)
        left_ref[i * 32 : (i + 1) * 32, :] = jnp.concatenate([high, high, low], axis=1)
    for j, value in enumerate(jac + [res, jnp.zeros_like(res)]):
        high, low = parts_of(value, 2)
        right_ref[j * 32 : (j + 1) * 32, :] = jnp.concatenate([high, low, high], axis=1)
    every = dot_t(left_ref[...], right_ref[...])
    halves = []
    for half in range(2):
        arrays = []
        for i in range(6):
            kept = jnp.zeros((8, LANES), F32)
            for r in range(CAP):
                block = every[i * 32 + r * 8 : i * 32 + r * 8 + 8, half * LANES : (half + 1) * LANES]
                kept = jnp.where(lane % 32 == r * 8 + sub, block, kept)
            arrays.append(kept)
        arrays += [None, None]
        for level in range(3):
            clear = (sub // (1 << level)) % 2 == 0
            arrays = [fold(arrays[n], arrays[n + 1], clear, 1 << level) for n in range(0, len(arrays), 2)]
        halves.append(arrays[0])
    low, high = halves
    first = (lane // 4) % 2 == 0
    blocks = []
    for c in range(2):
        if c == 0:
            block = jnp.where(first, low, pltpu.roll(high, 4, 1))
        else:
            block = jnp.where(first, pltpu.roll(low, LANES - 4, 1), high)
        code = jnp.sum(jnp.where(sub // 4 == c, codes, 0.0), axis=0, keepdims=True)
        blocks.append(jnp.where(sub == 7, jnp.broadcast_to(code, (8, LANES)), block))
    return blocks


def fold(a, b, clear, shift):
    if a is None:
        return None
    if b is None:
        return jnp.where(clear, a, 0.0) + pltpu.roll(jnp.where(clear, 0.0, a), shift, 0)
    return jnp.where(clear, a, b) + pltpu.roll(jnp.where(clear, b, a), shift, 0)


def turn_groups(load, owner_ref, sums_ref, column_ref):
    lane = iota((8, LANES), 1)
    lane1 = iota((1, LANES), 1)
    which = ((lane1 // 4) % 2) * 4 + ((lane1 // 64) % 2) * 2 + (lane1 // 32) % 2
    for q in range(GROUPS):
        blocks = [load(q, m) for m in range(8)]
        for bit, shift in ((1, 64), (0, 32), (2, 4)):
            clear = (lane // shift) % 2 == 0
            for m in range(8):
                if (m >> bit) % 2 == 0:
                    a, b = blocks[m], blocks[m + (1 << bit)]
                    blocks[m] = jnp.where(clear, a, pltpu.roll(b, shift, 1))
                    blocks[m + (1 << bit)] = jnp.where(clear, pltpu.roll(a, LANES - shift, 1), b)
        source = blocks[0][7:8, :]
        target = blocks[1][7:8, :]
        at = q * LANES
        if q < GROUPS // 2:
            owner = source
            column = target + (16 * (2 * q + which // 4)).astype(F32)
        else:
            owner = target
            column = source + (16 * which).astype(F32)
            blocks[6] = -blocks[6]
        mine = jnp.where(jnp.broadcast_to(owner, (LOC, LANES)) == iota((LOC, LANES), 0).astype(F32), 1.0, 0.0)
        there = jnp.where(jnp.broadcast_to(column, (LANES, LANES)) == iota((LANES, LANES), 0).astype(F32), -1.0, 0.0)
        stack = jnp.concatenate(blocks, axis=0)
        for n, term in enumerate(parts_of(stack, 2)):
            owner_ref[:, n * ITEMS + at : n * ITEMS + at + LANES] = mine.astype(BF16)
            column_ref[:, n * ITEMS + at : n * ITEMS + at + LANES] = there.astype(BF16)
            sums_ref[:, n * ITEMS + at : n * ITEMS + at + LANES] = term


def matrix(owner_ref, sums_ref, column_ref, lhs_ref, block_ref):
    for k, (i, j) in enumerate(PAIRS):
        row = sums_ref[j * 8 + i : j * 8 + i + 1, :]
        lhs_ref[k * LOC : (k + 1) * LOC, :] = jnp.broadcast_to(row, (LOC, 2 * ITEMS)) * owner_ref[...]
    block_ref[...] = dot_t(lhs_ref[...], column_ref[...])


def low(x, bits):
    return lax.bitwise_and(x, (1 << bits) - 1)


def high(x, bits):
    return lax.shift_right_logical(x, bits)


def order(p):
    return 2 * (1 - low(p, 1)) + low(p + high(p, 1), 1)


def step_kernel(
    pc_ref, cs_ref, ct_ref, src_ref, sm_ref, block_ref, part_ref,
    pay_ref, msg_ref, recv_ref, table_ref, left_ref, right_ref, back_ref, out_ref, in_ref,
    owner_ref, sums_ref, column_ref, lhs_ref,
    send_p, recv_p, send_a, recv_a, send_b, recv_b, send_c, recv_c,
):
    row = lax.axis_index("scan")
    col = lax.axis_index("grp")
    z, y, core = high(row, 3), low(high(row, 1), 2), low(row, 1)
    me = row * NG + col
    barrier = pltpu.get_barrier_semaphore()

    @pl.loop(1, ND)
    def _(step):
        other = low(me + step, 7)
        pl.semaphore_signal(barrier, inc=1, device_id=(high(other, 2), low(other, 2)), device_id_type=MESH)

    pick_points(pc_ref, src_ref, sm_ref, pay_ref, col)
    pack(cs_ref, ct_ref, pay_ref, msg_ref, col)
    pl.semaphore_wait(barrier, ND - 1)

    def points(to_row, to_col, at):
        to = to_row * NG + to_col
        return pltpu.make_async_remote_copy(
            src_ref=msg_ref.at[pl.ds(to * ROWS, ROWS)],
            dst_ref=recv_ref.at[pl.ds(at * ROWS, ROWS)],
            send_sem=send_p.at[to],
            recv_sem=recv_p.at[at],
            device_id=(to_row, to_col),
            device_id_type=MESH,
        )

    def each_of_unit(u, sign, act):
        uz = low(z + sign * order(high(u, 2)) + 4, 2)
        uy = low(y + sign * order(low(u, 2)) + 4, 2)
        for dc in range(2):
            for dx in range(NG):
                there = ((uz * 4 + uy) * 2 + low(core + dc, 1), low(col + dx, 2))
                if dc == 0 and dx == 0:

                    @pl.when(u < UNITS - 1)
                    def _():
                        act(*there)

                else:
                    act(*there)
        return uz * 4 + uy

    own = pltpu.make_async_copy(
        msg_ref.at[pl.ds(me * ROWS, ROWS)], recv_ref.at[pl.ds(me * ROWS, ROWS)], recv_p.at[me]
    )
    own.start()

    @pl.loop(0, UNITS)
    def _(u):
        each_of_unit(u, 1, lambda r, c: points(r, c, me).start())

    tile_table(pc_ref, sm_ref, table_ref, col)

    home = high(row, 3)
    slot = low(row, 3) * NG + col

    def give(to_row, at):
        return pltpu.make_async_remote_copy(
            src_ref=back_ref.at[to_row],
            dst_ref=out_ref.at[at],
            send_sem=send_a.at[to_row],
            recv_sem=recv_a.at[at],
            device_id=(to_row, home),
            device_id_type=MESH,
        )

    def share(unit, from_col, at):
        return pltpu.make_async_remote_copy(
            src_ref=back_ref.at[pl.ds(2 * unit, 2)],
            dst_ref=in_ref.at[from_col, pl.ds(2 * at, 2)],
            send_sem=send_b.at[unit],
            recv_sem=recv_b.at[from_col * 4 + at],
            device_id=(row, high(unit, 2)),
            device_id_type=MESH,
        )

    @pl.loop(0, UNITS)
    def _(u):
        unit = each_of_unit(u, -1, lambda r, c: points(r, c, r * NG + c).wait_recv())

        @pl.when(u == UNITS - 1)
        def _():
            own.wait()

        first, second = unit_sums(unit * (8 * ROWS), recv_ref, table_ref, left_ref, right_ref)
        back_ref[2 * unit] = first
        back_ref[2 * unit + 1] = second
        for c in range(2):
            to_row = 2 * unit + c
            lone = jnp.logical_and(to_row == row, home == col)

            @pl.when(jnp.logical_not(lone))
            def _():
                give(to_row, slot).start()

            @pl.when(lone)
            def _():
                pltpu.make_async_copy(back_ref.at[to_row], out_ref.at[slot], recv_a.at[slot]).start()

        @pl.when(high(unit, 2) != col)
        def _():
            share(unit, col, low(unit, 2)).start()

        @pl.when(high(unit, 2) == col)
        def _():
            pltpu.make_async_copy(
                back_ref.at[pl.ds(2 * unit, 2)], in_ref.at[col, pl.ds(2 * low(unit, 2), 2)], recv_b.at[col * 4 + low(unit, 2)]
            ).start()

    @pl.loop(0, 32)
    def _(n):
        give(row, n).wait_recv()

    @pl.loop(0, UNITS)
    def _(n):
        share(0, high(n, 2), low(n, 2)).wait_recv()

    def load(q, m):
        return out_ref[q * 8 + m] if q < GROUPS // 2 else in_ref[q - GROUPS // 2, m]

    turn_groups(load, owner_ref, sums_ref, column_ref)
    part = dot_t(owner_ref[...], sums_ref[...])
    part_ref[col] = jnp.concatenate([part, jnp.zeros((LOC, LANES - 64), F32)], axis=1)

    def spread(to_col, at):
        return pltpu.make_async_remote_copy(
            src_ref=part_ref.at[col],
            dst_ref=part_ref.at[at],
            send_sem=send_c.at[to_col],
            recv_sem=recv_c.at[at],
            device_id=(row, to_col),
            device_id_type=MESH,
        )

    for step in range(1, NG):
        spread(low(col + step, 2), col).start()

    matrix(owner_ref, sums_ref, column_ref, lhs_ref, block_ref)

    @pl.loop(1, ND)
    def _(step):
        other = low(me + step, 7)
        points(high(other, 2), low(other, 2), me).wait_send()

    @pl.loop(0, NS)
    def _(n):
        @pl.when(jnp.logical_not(jnp.logical_and(n == row, home == col)))
        def _():
            give(n, slot).wait_send()

    @pl.loop(0, UNITS)
    def _(n):
        @pl.when(high(n, 2) != col)
        def _():
            share(n, col, low(n, 2)).wait_send()

    for step in range(1, NG):
        other = low(col + step, 2)
        spread(other, col).wait_send()
        spread(other, other).wait_recv()


def finish_kernel(block_ref, part_ref, hess_ref, grad_ref):
    row = lax.axis_index("scan")
    col = lax.axis_index("grp")
    total = part_ref[0] + part_ref[1] + part_ref[2] + part_ref[3]
    lane = iota((LOC, LANES), 1)
    diag = (lane == iota((LOC, LANES), 0) + LOC * (row % 8)) & (row // 8 == col)
    for k, (i, j) in enumerate(PAIRS):
        at = j * 8 + i
        value = block_ref[k * LOC : (k + 1) * LOC, :] + jnp.where(
            diag, jnp.broadcast_to(total[:, at : at + 1], (LOC, LANES)), 0.0
        )
        hess_ref[i, j] = value
        if i != j:
            hess_ref[j, i] = value
    some = jnp.zeros((4, LANES), F32)
    for n in range(NG):
        some = jnp.where(col == n, total[n * 4 : (n + 1) * 4, :], some)
    grad_ref[...] = some[:, 48:54]


def vmem(count):
    return [pl.BlockSpec(memory_space=pltpu.VMEM)] * count


def local(samples, point_count, corr_scan, corr_tile, corr_src):
    dma = pltpu.SemaphoreType.DMA
    block, parts = pl.pallas_call(
        step_kernel,
        out_shape=(
            jax.ShapeDtypeStruct((len(PAIRS) * LOC, LANES), F32),
            jax.ShapeDtypeStruct((NG, LOC, LANES), F32),
        ),
        in_specs=[pl.BlockSpec(memory_space=pltpu.SMEM)] + vmem(4),
        out_specs=tuple(vmem(2)),
        scratch_shapes=[
            pltpu.VMEM((3 * REQ, 3 * LANES), BF16),
            pltpu.VMEM((ND * ROWS, LANES), F32),
            pltpu.VMEM((ND * ROWS, LANES), F32),
            pltpu.VMEM((3 * LOC * TL, 6 * LANES), BF16),
            pltpu.VMEM((6 * 32, 3 * LANES), BF16),
            pltpu.VMEM((8 * 32, 3 * LANES), BF16),
            pltpu.VMEM((NS, 8, LANES), F32),
            pltpu.VMEM((32, 8, LANES), F32),
            pltpu.VMEM((NG, 8, 8, LANES), F32),
            pltpu.VMEM((LOC, 2 * ITEMS), BF16),
            pltpu.VMEM((64, 2 * ITEMS), BF16),
            pltpu.VMEM((LANES, 2 * ITEMS), BF16),
            pltpu.VMEM((len(PAIRS) * LOC, 2 * ITEMS), BF16),
            dma((ND,)),
            dma((ND,)),
            dma((NS,)),
            dma((32,)),
            dma((UNITS,)),
            dma((UNITS,)),
            dma((NG,)),
            dma((NG,)),
        ],
        compiler_params=pltpu.CompilerParams(collective_id=0, has_side_effects=True),
        name="step",
    )(point_count, corr_scan, corr_tile, corr_src, samples.transpose(0, 2, 1, 3))
    hessian, gradient = pl.pallas_call(
        finish_kernel,
        out_shape=(
            jax.ShapeDtypeStruct((6, 6, LOC, LANES), F32),
            jax.ShapeDtypeStruct((4, 6), F32),
        ),
        in_specs=vmem(2),
        out_specs=tuple(vmem(2)),
        name="finish",
    )(block, parts)
    return hessian.transpose(2, 0, 1, 3), gradient


def solution(mesh):
    placed = (
        P("scan", "grp", None, None),
        P("scan"),
        P("scan", "grp"),
        P("scan", "grp"),
        P("scan", "grp", None),
    )
    return jax.shard_map(
        local,
        mesh=mesh,
        in_specs=placed,
        out_specs=(P("scan", None, None, "grp"), P(("scan", "grp"), None)),
        check_vma=False,
    )
```

```python
import functools

import jax
import jax.numpy as jnp
from jax import lax
from jax.experimental import pallas as pl
from jax.experimental.pallas import tpu as pltpu
from jax.sharding import PartitionSpec as P

F32 = jnp.float32
BF16 = jnp.bfloat16
I32 = jnp.int32
MESH = pl.DeviceIdType.MESH

NS = 32
NG = 4
ND = NS * NG
LOC = 16
TL = 16
CT = 16
REQ = LOC * CT
CAP = 4
FAR = 1000.0
LANES = 128
PAIRS = [(i, j) for i in range(6) for j in range(i, 6)]
PLANES = 4
SLOTS = ND * CAP
HALF = PLANES * LANES
SPOT = {(i, j): (i, j) for i in range(4) for j in range(i, 7)}
SPOT |= {(5, 5): (1, 0), (5, 6): (1, 7), (4, 4): (2, 1), (4, 5): (2, 0), (4, 6): (2, 7)}


def iota(shape, dim):
    return lax.broadcasted_iota(I32, shape, dim)


def dot(a, b):
    return lax.dot_general(a, b, (((1,), (0,)), ((), ())), preferred_element_type=F32)


def dot_t(a, b):
    return lax.dot_general(a, b, (((1,), (1,)), ((), ())), preferred_element_type=F32)


def parts_of(x, count):
    terms = []
    for _ in range(count):
        term = x.astype(BF16)
        terms.append(term)
        x = x - term.astype(F32)
    return terms


def onehot(cond):
    return jnp.where(cond, 1.0, 0.0).astype(BF16)


def low(x, bits):
    return lax.bitwise_and(x, (1 << bits) - 1)


def high(x, bits):
    return lax.shift_right_logical(x, bits)


def pick_points(x, pc_ref, src_ref, sm_ref, pay_ref, group):
    first = group * (TL * LANES)

    @pl.loop(0, LOC)
    def _(s):
        picks = src_ref[s]
        tile = high(picks, 7)
        lane = low(picks, 7)
        acc = jnp.zeros((CT, LANES), F32)
        for t in range(TL):
            row = jnp.broadcast_to(sm_ref[s, x, pl.ds(t, 1), :], (CT, LANES))
            got = jnp.take_along_axis(row, lane, axis=1, mode="promise_in_bounds")
            acc = jnp.where(tile == t, got, acc)
        if x == 0:
            acc = jnp.where(first + picks < pc_ref[s], acc, FAR)
        at = pl.multiple_of(s * CT, CT)
        for n, term in enumerate(parts_of(acc, 3)):
            pay_ref[pl.ds(n * REQ + at, CT), :] = term


def route(cs_ref, ct_ref, take_ref, code_ref, group):
    cs = cs_ref[...]
    ct = ct_ref[...]
    dest = (high(cs, 4) * NG + high(ct, 4)).astype(F32)
    code = (low(cs, 4) * TL + low(ct, 4) + 1).astype(F32)
    wide = dot(dest.astype(BF16), onehot(iota((CT, REQ), 1) % CT == iota((CT, REQ), 0)))
    wide = jnp.where(iota((LOC, REQ), 1) // CT == iota((LOC, REQ), 0), wide, 0.0)
    dest_t = dot(jnp.ones((ND, LOC), BF16), wide.astype(BF16))
    to_me = dest_t == iota((ND, REQ), 0).astype(F32)
    rank = dot(onehot(to_me), onehot(iota((REQ, REQ), 0) < iota((REQ, REQ), 1)))
    takes = [onehot(to_me & (rank == float(r))) for r in range(CAP)]
    for r in range(CAP):
        for n in range(3):
            take_ref[r * ND : (r + 1) * ND, n * REQ : (n + 1) * REQ] = takes[r]
    tall = dot(onehot(iota((REQ, LOC), 0) // CT == iota((REQ, LOC), 1)), code.astype(BF16))
    tall = jnp.where(iota((REQ, CT), 0) % CT == iota((REQ, CT), 1), tall, 0.0)
    code_b = dot(tall.astype(BF16), jnp.ones((CT, LANES), BF16))
    target = high(code_b.astype(I32) - 1, 4).astype(F32)
    source = (iota((REQ, LANES), 0) // CT).astype(F32)
    lane = iota((REQ, LANES), 1)
    codes = jnp.where(lane < 16, source, jnp.where(lane < 32, target, code_b)).astype(BF16)
    lane = iota((ND, LANES), 1)
    row = jnp.zeros((ND, LANES), F32)
    for r in range(CAP):
        at = group * CAP + r
        here = (lane == at) | (lane == 16 + at) | (lane == 32 + r)
        row = jnp.where(here, dot(takes[r], codes), row)
    code_ref[...] = row


def pack(x, take_ref, pay_ref, msg_ref):
    got = dot(take_ref[...], pay_ref[...])
    for r in range(CAP):
        msg_ref[x, pl.ds(r, ND, stride=CAP), :] = got[r * ND : (r + 1) * ND]


def tile_table(pc_ref, sm_ref, table_ref, group):
    point = (group * TL + iota((TL, LANES), 0)) * LANES + iota((TL, LANES), 1)

    @pl.loop(0, LOC)
    def _(s):
        valid = point < pc_ref[s]
        at = pl.multiple_of(s * TL, TL)
        for x in range(6):
            value = sm_ref[s, x]
            if x >= 3:
                value = jnp.where(valid, value, 0.0)
            for n, term in enumerate(parts_of(value, 3)):
                table_ref[pl.ds(n * LOC * TL + at, TL), x * LANES : (x + 1) * LANES] = term


def fetch_tiles(code_ref, table_ref, tile_ref, note_ref):
    codes = code_ref[...].astype(BF16)
    spread = dot(onehot(iota((SLOTS, ND), 0) // CAP == iota((SLOTS, ND), 1)), codes)
    spread = jnp.where(iota((SLOTS, LANES), 1) == 32 + iota((SLOTS, LANES), 0) % CAP, spread, 0.0)
    wanted = dot(spread.astype(BF16), jnp.ones((LANES, LOC * TL), BF16))
    take = onehot(wanted == (iota((SLOTS, LOC * TL), 1) + 1).astype(F32))
    tile_ref[...] = dot(jnp.concatenate([take] * 3, axis=1), table_ref[...])
    here = iota((ND, ND), 0)
    note_ref[...] = dot(onehot((here // 4 == iota((ND, ND), 1) // 4) & (here % 4 == 3)), codes)


def fold(a, b, clear, shift):
    return jnp.where(clear, a, b) + pltpu.roll(jnp.where(clear, b, a), shift, 0)


def plane_sums(plane, recv_ref, tile_ref, note_ref, left_ref, right_ref, back_ref):
    at = pl.multiple_of(plane * LANES, LANES)
    p = [recv_ref[x, pl.ds(at, LANES), :] for x in range(3)]
    tile = [tile_ref[pl.ds(at, LANES), x * LANES : (x + 1) * LANES] for x in range(6)]
    q, n = tile[:3], tile[3:]
    counts = p[0] < 0.5 * FAR
    p[0] = jnp.where(counts, p[0], 0.0)
    res = n[0] * (p[0] - q[0]) + n[1] * (p[1] - q[1]) + n[2] * (p[2] - q[2])
    w = jnp.where(counts, 1.0 / (1.0 + res * res), 0.0)
    jac = [
        p[1] * n[2] - p[2] * n[1],
        p[2] * n[0] - p[0] * n[2],
        p[0] * n[1] - p[1] * n[0],
        n[0],
        n[1],
        n[2],
    ]
    for i in range(6):
        big, small = parts_of(w * jac[i], 2)
        for r in range(8):
            for k, term in enumerate((big, big, small)):
                left_ref[r, i * 16 : (i + 1) * 16, k * LANES : (k + 1) * LANES] = term[r * 16 : (r + 1) * 16]
    for j, value in enumerate(jac + [res]):
        big, small = parts_of(value, 2)
        spots = [j] + {4: [9], 5: [8], 6: [15]}.get(j, [])
        for r in range(8):
            for k, term in enumerate((big, small, big)):
                for spot in spots:
                    right_ref[r, spot * 16 : (spot + 1) * 16, k * LANES : (k + 1) * LANES] = term[r * 16 : (r + 1) * 16]
    lane = iota((8, LANES), 1)
    sub = iota((8, LANES), 0)
    spot = lane // 16
    first = [spot < 8, (spot >= 1) & (spot <= 6), (spot >= 2) & (spot <= 6), spot < 8]
    other = [None, 5, 4, None]
    for chip in range(4):
        arrays = []
        for c in range(2):
            r = chip * 2 + c
            every = dot_t(left_ref[r], right_ref[r])
            for i in range(4):
                kept = jnp.zeros((8, LANES), F32)
                for h in range(2):
                    value = every[i * 16 + h * 8 : i * 16 + h * 8 + 8, :LANES]
                    if other[i] is not None:
                        o = other[i] * 16 + h * 8
                        value = jnp.where(first[i], value, every[o : o + 8, LANES:])
                    kept = jnp.where(lane % 16 == h * 8 + sub, value, kept)
                arrays.append(kept)
        for level in range(3):
            clear = (sub // (1 << level)) % 2 == 0
            arrays = [fold(arrays[n], arrays[n + 1], clear, 1 << level) for n in range(0, len(arrays), 2)]
        note = note_ref[pl.ds(plane * 32 + chip * 8, 8), :]
        back_ref[plane * 4 + chip] = jnp.where((sub % 4 == 3) & (spot < 3), note, arrays[0])


def turn(plane, mid_ref, back_ref, turn_ref):
    lane = iota((8, LANES), 1)
    blocks = [mid_ref[plane * 4 + m] for m in range(4)] + [back_ref[plane * 4 + m] for m in range(4)]
    for bit in range(3):
        shift = 16 << bit
        clear = (lane // shift) % 2 == 0
        for m in range(8):
            if (m >> bit) % 2 == 0:
                a, b = blocks[m], blocks[m + (1 << bit)]
                blocks[m] = jnp.where(clear, a, pltpu.roll(b, shift, 1))
                blocks[m + (1 << bit)] = jnp.where(clear, pltpu.roll(a, LANES - shift, 1), b)
    for n in range(8):
        turn_ref[plane, n] = jnp.where(lane < 64, blocks[n], -blocks[n]) if n >= 6 else blocks[n]


def arrange(turn_ref, owner_ref, sums_ref, column_ref):
    lane = iota((1, LANES), 1)
    y = (lane // 16) % 4
    for t in range(PLANES):
        source = turn_ref[t, 0]
        target = turn_ref[t, 1]
        for c in range(2):
            s = source[c * 4 + 3 : c * 4 + 4, :]
            b = target[c * 4 + 3 : c * 4 + 4, :]
            owner = jnp.broadcast_to(jnp.where(lane < 64, s, b), (LOC, LANES))
            at = c * HALF + t * LANES
            owner_ref[:, at : at + LANES] = onehot(owner == iota((LOC, LANES), 0).astype(F32))
            if column_ref is not None:
                column = jnp.where(lane < 64, b, s) + (16 * (2 * y + c)).astype(F32)
                there = jnp.broadcast_to(column, (LANES, LANES)) == iota((LANES, LANES), 0).astype(F32)
                there = jnp.where(there, -1.0, 0.0).astype(BF16)
                for n in range(2):
                    column_ref[:, n * 2 * HALF + at : n * 2 * HALF + at + LANES] = there
        for p in range(0, 8, 2):
            pair = jnp.concatenate([turn_ref[t, p], turn_ref[t, p + 1]], axis=0)
            for n, term in enumerate(parts_of(pair, 2)):
                sums_ref[p * 8 : p * 8 + 16, n * HALF + t * LANES : n * HALF + (t + 1) * LANES] = term


def scan_sums(owner_ref, sums_ref):
    owners = [jnp.concatenate([owner_ref[:, c * HALF : (c + 1) * HALF]] * 2, axis=1) for c in range(2)]
    both = dot_t(jnp.concatenate(owners, axis=0), sums_ref[...])
    lane = iota((LOC, 64), 1)
    part = jnp.where((lane // 4) % 2 == 0, both[:LOC], both[LOC:])
    return jnp.concatenate([part, jnp.zeros((LOC, LANES - 64), F32)], axis=1)


def matrix(owner_ref, sums_ref, column_ref, lhs_ref, block_ref):
    for k, pair in enumerate(PAIRS):
        i, p = SPOT[pair]
        for c in range(2):
            at = p * 8 + c * 4 + i
            mine = owner_ref[:, c * HALF : (c + 1) * HALF]
            for n in range(2):
                row = sums_ref[at : at + 1, n * HALF : (n + 1) * HALF]
                lhs_ref[k * LOC : (k + 1) * LOC, (2 * n + c) * HALF : (2 * n + c + 1) * HALF] = (
                    jnp.broadcast_to(row, (LOC, HALF)) * mine
                )
    block_ref[...] = dot_t(lhs_ref[...], column_ref[...])


def order(p):
    return 2 * (1 - low(p, 1)) + low(p + high(p, 1), 1)


def step_kernel(
    pc_ref, cs_any, ct_any, src_any, sm_any, block_ref, part_ref,
    cs_ref, ct_ref, src_ref, sm_ref, take_ref, pay_ref, code_ref, msg_ref, codes_ref, recv_ref, table_ref, tile_ref, note_ref,
    left_ref, right_ref, back_ref, mid_ref, turn_ref, got_ref, owner_ref, sums_ref, column_ref, lhs_ref,
    load_sem, send_p, recv_n, recv_p, send_a, recv_a, send_b, recv_b, send_c, recv_c,
):
    row = lax.axis_index("scan")
    col = lax.axis_index("grp")
    z, y, core = high(row, 3), low(high(row, 1), 2), low(row, 1)
    me = row * NG + col
    barrier = pltpu.get_barrier_semaphore()

    @pl.loop(1, ND)
    def _(step):
        other = low(me + step, 7)
        pl.semaphore_signal(barrier, inc=1, device_id=(high(other, 2), low(other, 2)), device_id_type=MESH)

    loads = [
        pltpu.make_async_copy(a, b, load_sem.at[n])
        for n, (a, b) in enumerate(
            [(cs_any, cs_ref), (ct_any, ct_ref), (src_any, src_ref)]
            + [(sm_any.at[:, x], sm_ref.at[:, x]) for x in range(3)]
            + [(sm_any.at[:, pl.ds(3, 3)], sm_ref.at[:, pl.ds(3, 3)])]
        )
    ]
    for load in loads:
        load.start()

    def to_all(act):
        @pl.loop(0, 16)
        def _(u):
            uz = low(z + order(high(u, 2)), 2)
            uy = low(y + order(low(u, 2)), 2)
            for dc in range(2):
                for dx in range(NG):
                    there = ((uz * 4 + uy) * 2 + low(core + dc, 1), low(col + dx, 2))
                    if dc == 0 and dx == 0:

                        @pl.when(u < 15)
                        def _():
                            act(*there)

                    else:
                        act(*there)

    def send_codes(r, c):
        pltpu.make_async_remote_copy(
            src_ref=code_ref.at[pl.ds(r * NG + c, 1)],
            dst_ref=codes_ref.at[pl.ds(me, 1)],
            send_sem=send_p.at[3],
            recv_sem=recv_n,
            device_id=(r, c),
            device_id_type=MESH,
        ).start()

    def send_points(x, r, c):
        pltpu.make_async_remote_copy(
            src_ref=msg_ref.at[x, pl.ds((r * NG + c) * CAP, CAP)],
            dst_ref=recv_ref.at[x, pl.ds(me * CAP, CAP)],
            send_sem=send_p.at[x],
            recv_sem=recv_p.at[z],
            device_id=(r, c),
            device_id_type=MESH,
        ).start()

    loads[0].wait()
    loads[1].wait()
    route(cs_ref, ct_ref, take_ref, code_ref, col)
    loads[2].wait()
    for x in range(3):
        loads[3 + x].wait()
        pick_points(x, pc_ref, src_ref, sm_ref, pay_ref.at[x], col)
        pack(x, take_ref, pay_ref.at[x], msg_ref)
        if x == 0:
            pl.semaphore_wait(barrier, ND - 1)
            pltpu.make_async_copy(code_ref.at[pl.ds(me, 1)], codes_ref.at[pl.ds(me, 1)], recv_n).start()
            to_all(send_codes)
        to_all(functools.partial(send_points, x))
    pltpu.make_async_copy(
        msg_ref.at[:, pl.ds(me * CAP, CAP)], recv_ref.at[:, pl.ds(me * CAP, CAP)], recv_p.at[z]
    ).start()

    loads[6].wait()
    tile_table(pc_ref, sm_ref, table_ref, col)
    for spot in (7, 10, 11, 12, 13, 14):
        right_ref[:, spot * 16 : (spot + 1) * 16, :] = jnp.zeros((8, 16, 3 * LANES), BF16)
    pltpu.make_async_copy(codes_ref, codes_ref, recv_n).wait()
    fetch_tiles(codes_ref, table_ref, tile_ref, note_ref)

    @pl.loop(0, PLANES)
    def _(u):
        plane = low(z + order(u), 2)
        arrived = recv_ref.at[:, pl.ds(plane * LANES, LANES)]
        pltpu.make_async_copy(arrived, arrived, recv_p.at[plane]).wait()
        plane_sums(plane, recv_ref, tile_ref, note_ref, left_ref, right_ref, back_ref)
        for n in range(8):
            to_row = plane * 8 + n
            src = back_ref.at[plane * 4 + n // 2, pl.ds(n % 2 * 4, 4)]
            dst = mid_ref.at[high(row, 1), pl.ds(core * 4, 4)]

            @pl.when(to_row != row)
            def _():
                pltpu.make_async_remote_copy(
                    src_ref=src,
                    dst_ref=dst,
                    send_sem=send_a,
                    recv_sem=recv_a,
                    device_id=(to_row, col),
                    device_id_type=MESH,
                ).start()

            @pl.when(to_row == row)
            def _():
                pltpu.make_async_copy(src, dst, recv_a).start()

    pltpu.make_async_copy(mid_ref, mid_ref, recv_a).wait()

    def give(to_col, at):
        return pltpu.make_async_remote_copy(
            src_ref=turn_ref.at[to_col],
            dst_ref=got_ref.at[at],
            send_sem=send_b.at[to_col],
            recv_sem=recv_b.at[at],
            device_id=(row, to_col),
            device_id_type=MESH,
        )

    def spread(to_col, at):
        return pltpu.make_async_remote_copy(
            src_ref=part_ref.at[col],
            dst_ref=part_ref.at[at],
            send_sem=send_c.at[to_col],
            recv_sem=recv_c.at[at],
            device_id=(row, to_col),
            device_id_type=MESH,
        )

    for plane in range(PLANES):
        turn(plane, mid_ref, back_ref, turn_ref)
    for step in (2, 1, 3):
        give(low(col + step, 2), col).start()
    own = pltpu.make_async_copy(turn_ref.at[col], got_ref.at[col], recv_b.at[col])
    own.start()
    arrange(turn_ref, owner_ref, sums_ref, None)
    part_ref[col] = scan_sums(owner_ref, sums_ref)
    for step in (2, 1, 3):
        spread(low(col + step, 2), col).start()

    for x in range(3):
        left = msg_ref.at[x, pl.ds(0, (ND - 1) * CAP)]
        pltpu.make_async_copy(left, left, send_p.at[x]).wait()
    left = code_ref.at[pl.ds(0, ND - 1)]
    pltpu.make_async_copy(left, left, send_p.at[3]).wait()
    for left in (back_ref.at[pl.ds(0, 15)], back_ref.at[15, pl.ds(0, 4)]):
        pltpu.make_async_copy(left, left, send_a).wait()

    own.wait()
    for step in range(1, NG):
        other = low(col + step, 2)
        give(other, other).wait_recv()
    arrange(got_ref, owner_ref, sums_ref, column_ref)
    matrix(owner_ref, sums_ref, column_ref, lhs_ref, block_ref)
    for step in range(1, NG):
        other = low(col + step, 2)
        give(other, col).wait_send()
        spread(other, col).wait_send()
        spread(other, other).wait_recv()


def finish_kernel(block_ref, part_ref, hess_ref, grad_ref):
    row = lax.axis_index("scan")
    col = lax.axis_index("grp")
    total = part_ref[0] + part_ref[1] + part_ref[2] + part_ref[3]
    total = total + pltpu.roll(total, LANES - 4, 1)
    lane = iota((LOC, LANES), 1)
    diag = (lane == iota((LOC, LANES), 0) + LOC * (row % 8)) & (row // 8 == col)
    for k, (i, j) in enumerate(PAIRS):
        at = SPOT[i, j][1] * 8 + SPOT[i, j][0]
        value = block_ref[k * LOC : (k + 1) * LOC, :] + jnp.where(
            diag, jnp.broadcast_to(total[:, at : at + 1], (LOC, LANES)), 0.0
        )
        hess_ref[i, j] = value
        if i != j:
            hess_ref[j, i] = value
    some = jnp.zeros((4, LANES), F32)
    for n in range(NG):
        some = jnp.where(col == n, total[n * 4 : (n + 1) * 4, :], some)
    at = [SPOT[i, 6][1] * 8 + SPOT[i, 6][0] for i in range(6)]
    grad_ref[...] = jnp.concatenate([some[:, a : a + 1] for a in at], axis=1)


def vmem(count):
    return [pl.BlockSpec(memory_space=pltpu.VMEM)] * count


def local(samples, point_count, corr_scan, corr_tile, corr_src):
    dma = pltpu.SemaphoreType.DMA
    block, parts = pl.pallas_call(
        step_kernel,
        out_shape=(
            jax.ShapeDtypeStruct((len(PAIRS) * LOC, LANES), F32),
            jax.ShapeDtypeStruct((NG, LOC, LANES), F32),
        ),
        in_specs=[pl.BlockSpec(memory_space=pltpu.SMEM)] + [pl.BlockSpec(memory_space=pl.ANY)] * 4,
        out_specs=tuple(vmem(2)),
        scratch_shapes=[
            pltpu.VMEM((LOC, CT), I32),
            pltpu.VMEM((LOC, CT), I32),
            pltpu.VMEM((LOC, CT, LANES), I32),
            pltpu.VMEM((LOC, 6, TL, LANES), F32),
            pltpu.VMEM((SLOTS, 3 * REQ), BF16),
            pltpu.VMEM((3, 3 * REQ, LANES), BF16),
            pltpu.VMEM((ND, LANES), F32),
            pltpu.VMEM((3, SLOTS, LANES), F32),
            pltpu.VMEM((ND, LANES), F32),
            pltpu.VMEM((3, SLOTS, LANES), F32),
            pltpu.VMEM((3 * LOC * TL, 6 * LANES), BF16),
            pltpu.VMEM((SLOTS, 6 * LANES), F32),
            pltpu.VMEM((ND, LANES), F32),
            pltpu.VMEM((8, 6 * 16, 3 * LANES), BF16),
            pltpu.VMEM((8, 16 * 16, 3 * LANES), BF16),
            pltpu.VMEM((16, 8, LANES), F32),
            pltpu.VMEM((16, 8, LANES), F32),
            pltpu.VMEM((PLANES, 8, 8, LANES), F32),
            pltpu.VMEM((NG, 8, 8, LANES), F32),
            pltpu.VMEM((LOC, 2 * HALF), BF16),
            pltpu.VMEM((64, 2 * HALF), BF16),
            pltpu.VMEM((LANES, 4 * HALF), BF16),
            pltpu.VMEM((len(PAIRS) * LOC, 4 * HALF), BF16),
            dma((7,)),
            dma((4,)),
            dma,
            dma((PLANES,)),
            dma,
            dma,
            dma((NG,)),
            dma((NG,)),
            dma((NG,)),
            dma((NG,)),
        ],
        compiler_params=pltpu.CompilerParams(collective_id=0, has_side_effects=True),
        name="step",
    )(point_count, corr_scan, corr_tile, corr_src, samples.transpose(0, 2, 1, 3))
    hessian, gradient = pl.pallas_call(
        finish_kernel,
        out_shape=(
            jax.ShapeDtypeStruct((6, 6, LOC, LANES), F32),
            jax.ShapeDtypeStruct((4, 6), F32),
        ),
        in_specs=vmem(2),
        out_specs=tuple(vmem(2)),
        name="finish",
    )(block, parts)
    return hessian.transpose(2, 0, 1, 3), gradient


def solution(mesh):
    placed = (
        P("scan", "grp", None, None),
        P("scan"),
        P("scan", "grp"),
        P("scan", "grp"),
        P("scan", "grp", None),
    )
    return jax.shard_map(
        local,
        mesh=mesh,
        in_specs=placed,
        out_specs=(P("scan", None, None, "grp"), P(("scan", "grp"), None)),
        check_vma=False,
    )
```

```python
import functools

import jax
import jax.numpy as jnp
from jax import lax
from jax.experimental import pallas as pl
from jax.experimental.pallas import tpu as pltpu
from jax.sharding import PartitionSpec as P

F32 = jnp.float32
BF16 = jnp.bfloat16
I32 = jnp.int32
MESH = pl.DeviceIdType.MESH

NS = 32
NG = 4
ND = NS * NG
LOC = 16
TL = 16
CT = 16
REQ = LOC * CT
CAP = 4
FAR = 1000.0
LANES = 128
PAIRS = [(i, j) for i in range(6) for j in range(i, 6)]
PLANES = 4
SLOTS = ND * CAP
FIRST = CAP + 1
HALF = PLANES * LANES
SPOT = {(i, j): (i, j) for i in range(4) for j in range(i, 7)}
SPOT |= {(5, 5): (1, 0), (5, 6): (1, 7), (4, 4): (2, 1), (4, 5): (2, 0), (4, 6): (2, 7)}


def iota(shape, dim):
    return lax.broadcasted_iota(I32, shape, dim)


def dot(a, b):
    return lax.dot_general(a, b, (((1,), (0,)), ((), ())), preferred_element_type=F32)


def dot_t(a, b):
    return lax.dot_general(a, b, (((1,), (1,)), ((), ())), preferred_element_type=F32)


def parts_of(x, count):
    terms = []
    for _ in range(count):
        term = x.astype(BF16)
        terms.append(term)
        x = x - term.astype(F32)
    return terms


def onehot(cond):
    return jnp.where(cond, 1.0, 0.0).astype(BF16)


def low(x, bits):
    return lax.bitwise_and(x, (1 << bits) - 1)


def high(x, bits):
    return lax.shift_right_logical(x, bits)


def pick_points(x, pc_ref, src_ref, sm_ref, pay_ref, group):
    first = group * (TL * LANES)

    @pl.loop(0, LOC)
    def _(s):
        picks = src_ref[s]
        tile = high(picks, 7)
        lane = low(picks, 7)
        acc = jnp.zeros((CT, LANES), F32)
        for t in range(TL):
            row = jnp.broadcast_to(sm_ref[s, x, pl.ds(t, 1), :], (CT, LANES))
            got = jnp.take_along_axis(row, lane, axis=1, mode="promise_in_bounds")
            acc = jnp.where(tile == t, got, acc)
        if x == 0:
            acc = jnp.where(first + picks < pc_ref[s], acc, FAR)
        at = pl.multiple_of(s * CT, CT)
        for n, term in enumerate(parts_of(acc, 3)):
            pay_ref[pl.ds(n * REQ + at, CT), :] = term


def route(cs_ref, ct_ref, take_ref, first_ref, group):
    cs = cs_ref[...]
    ct = ct_ref[...]
    dest = (high(cs, 4) * NG + high(ct, 4)).astype(F32)
    code = (low(cs, 4) * TL + low(ct, 4) + 1).astype(F32)
    wide = dot(dest.astype(BF16), onehot(iota((CT, REQ), 1) % CT == iota((CT, REQ), 0)))
    wide = jnp.where(iota((LOC, REQ), 1) // CT == iota((LOC, REQ), 0), wide, 0.0)
    dest_t = dot(jnp.ones((ND, LOC), BF16), wide.astype(BF16))
    to_me = dest_t == iota((ND, REQ), 0).astype(F32)
    rank = dot(onehot(to_me), onehot(iota((REQ, REQ), 0) < iota((REQ, REQ), 1)))
    takes = [onehot(to_me & (rank == float(r))) for r in range(CAP)]
    for r in range(CAP):
        for n in range(3):
            take_ref[r * ND : (r + 1) * ND, n * REQ : (n + 1) * REQ] = takes[r]
    tall = dot(onehot(iota((REQ, LOC), 0) // CT == iota((REQ, LOC), 1)), code.astype(BF16))
    tall = jnp.where(iota((REQ, CT), 0) % CT == iota((REQ, CT), 1), tall, 0.0)
    code_b = dot(tall.astype(BF16), jnp.ones((CT, LANES), BF16))
    target = high(code_b.astype(I32) - 1, 4).astype(F32)
    source = (iota((REQ, LANES), 0) // CT).astype(F32)
    lane = iota((REQ, LANES), 1)
    codes = jnp.where(lane < 16, source, jnp.where(lane < 32, target, code_b)).astype(BF16)
    lane = iota((ND, LANES), 1)
    row = jnp.zeros((ND, LANES), F32)
    for r in range(CAP):
        at = group * CAP + r
        here = (lane == at) | (lane == 16 + at) | (lane == 32 + r)
        row = jnp.where(here, dot(takes[r], codes), row)
    first_ref[pl.ds(CAP, ND, stride=FIRST), :] = row


def pack(take_ref, pay_ref, msg_ref, rows):
    got = dot(take_ref[...], pay_ref[...])
    for r in range(CAP):
        msg_ref[pl.ds(r, ND, stride=rows), :] = got[r * ND : (r + 1) * ND]


def tile_table(pc_ref, sm_ref, table_ref, group):
    point = (group * TL + iota((TL, LANES), 0)) * LANES + iota((TL, LANES), 1)

    @pl.loop(0, LOC)
    def _(s):
        valid = point < pc_ref[s]
        at = pl.multiple_of(s * TL, TL)
        for x in range(6):
            value = sm_ref[s, x]
            if x >= 3:
                value = jnp.where(valid, value, 0.0)
            for n, term in enumerate(parts_of(value, 3)):
                table_ref[pl.ds(n * LOC * TL + at, TL), x * LANES : (x + 1) * LANES] = term


def fetch_tiles(first_ref, plane, table_ref, tile_ref, note_ref, x_ref):
    src = plane * (32 * FIRST)
    at = pl.multiple_of(plane * LANES, LANES)
    codes = first_ref[pl.ds(src + CAP, 32, stride=FIRST), :].astype(BF16)
    for r in range(CAP):
        x_ref[pl.ds(r, 32, stride=CAP), :] = first_ref[pl.ds(src + r, 32, stride=FIRST), :]
    spread = dot(onehot(iota((LANES, 32), 0) // CAP == iota((LANES, 32), 1)), codes)
    spread = jnp.where(iota((LANES, LANES), 1) == 32 + iota((LANES, LANES), 0) % CAP, spread, 0.0)
    wanted = dot(spread.astype(BF16), jnp.ones((LANES, LOC * TL), BF16))
    take = onehot(wanted == (iota((LANES, LOC * TL), 1) + 1).astype(F32))
    tile_ref[...] = dot(jnp.concatenate([take] * 3, axis=1), table_ref[...])
    here = iota((32, 32), 0)
    note_ref[...] = dot(onehot((here // 4 == iota((32, 32), 1) // 4) & (here % 4 == 3)), codes)


def fold(a, b, clear, shift):
    return jnp.where(clear, a, b) + pltpu.roll(jnp.where(clear, b, a), shift, 0)


def plane_sums(plane, x_ref, recv_ref, tile_ref, note_ref, left_ref, right_ref, back_ref):
    at = pl.multiple_of(plane * LANES, LANES)
    p = [x_ref[...]] + [recv_ref[x, pl.ds(at, LANES), :] for x in range(2)]
    tile = [tile_ref[:, x * LANES : (x + 1) * LANES] for x in range(6)]
    q, n = tile[:3], tile[3:]
    counts = p[0] < 0.5 * FAR
    p[0] = jnp.where(counts, p[0], 0.0)
    res = n[0] * (p[0] - q[0]) + n[1] * (p[1] - q[1]) + n[2] * (p[2] - q[2])
    w = jnp.where(counts, 1.0 / (1.0 + res * res), 0.0)
    jac = [
        p[1] * n[2] - p[2] * n[1],
        p[2] * n[0] - p[0] * n[2],
        p[0] * n[1] - p[1] * n[0],
        n[0],
        n[1],
        n[2],
    ]
    for i in range(6):
        big, small = parts_of(w * jac[i], 2)
        for r in range(8):
            for k, term in enumerate((big, big, small)):
                left_ref[r, i * 16 : (i + 1) * 16, k * LANES : (k + 1) * LANES] = term[r * 16 : (r + 1) * 16]
    for j, value in enumerate(jac + [res]):
        big, small = parts_of(value, 2)
        spots = [j] + {4: [9], 5: [8], 6: [15]}.get(j, [])
        for r in range(8):
            for k, term in enumerate((big, small, big)):
                for spot in spots:
                    right_ref[r, spot * 16 : (spot + 1) * 16, k * LANES : (k + 1) * LANES] = term[r * 16 : (r + 1) * 16]
    lane = iota((8, LANES), 1)
    sub = iota((8, LANES), 0)
    spot = lane // 16
    first = [spot < 8, (spot >= 1) & (spot <= 6), (spot >= 2) & (spot <= 6), spot < 8]
    other = [None, 5, 4, None]
    for chip in range(4):
        arrays = []
        for c in range(2):
            r = chip * 2 + c
            every = dot_t(left_ref[r], right_ref[r])
            for i in range(4):
                kept = jnp.zeros((8, LANES), F32)
                for h in range(2):
                    value = every[i * 16 + h * 8 : i * 16 + h * 8 + 8, :LANES]
                    if other[i] is not None:
                        o = other[i] * 16 + h * 8
                        value = jnp.where(first[i], value, every[o : o + 8, LANES:])
                    kept = jnp.where(lane % 16 == h * 8 + sub, value, kept)
                arrays.append(kept)
        for level in range(3):
            clear = (sub // (1 << level)) % 2 == 0
            arrays = [fold(arrays[n], arrays[n + 1], clear, 1 << level) for n in range(0, len(arrays), 2)]
        note = note_ref[chip * 8 : chip * 8 + 8, :]
        back_ref[plane * 4 + chip] = jnp.where((sub % 4 == 3) & (spot < 3), note, arrays[0])


def turn(plane, partner_ref, source_ref, turn_ref):
    lane = iota((8, LANES), 1)
    blocks = [ref[plane * 4 + m] for ref in (partner_ref, source_ref) for m in range(4)]
    for bit in range(3):
        shift = 16 << bit
        clear = (lane // shift) % 2 == 0
        for m in range(8):
            if (m >> bit) % 2 == 0:
                a, b = blocks[m], blocks[m + (1 << bit)]
                blocks[m] = jnp.where(clear, a, pltpu.roll(b, shift, 1))
                blocks[m + (1 << bit)] = jnp.where(clear, pltpu.roll(a, LANES - shift, 1), b)
    for n in range(8):
        turn_ref[plane, n] = jnp.where(lane < 64, blocks[n], -blocks[n]) if n >= 6 else blocks[n]


def arrange(turn_ref, owner_ref, sums_ref, column_ref):
    lane = iota((1, LANES), 1)
    y = (lane // 16) % 4
    for t in range(PLANES):
        source = turn_ref[t, 0]
        target = turn_ref[t, 1]
        for c in range(2):
            s = source[c * 4 + 3 : c * 4 + 4, :]
            b = target[c * 4 + 3 : c * 4 + 4, :]
            owner = jnp.broadcast_to(jnp.where(lane < 64, s, b), (LOC, LANES))
            at = c * HALF + t * LANES
            owner_ref[:, at : at + LANES] = onehot(owner == iota((LOC, LANES), 0).astype(F32))
            if column_ref is not None:
                column = jnp.where(lane < 64, b, s) + (16 * (2 * y + c)).astype(F32)
                there = jnp.broadcast_to(column, (LANES, LANES)) == iota((LANES, LANES), 0).astype(F32)
                there = jnp.where(there, -1.0, 0.0).astype(BF16)
                for n in range(2):
                    column_ref[:, n * 2 * HALF + at : n * 2 * HALF + at + LANES] = there
        for p in range(0, 8, 2):
            pair = jnp.concatenate([turn_ref[t, p], turn_ref[t, p + 1]], axis=0)
            for n, term in enumerate(parts_of(pair, 2)):
                sums_ref[p * 8 : p * 8 + 16, n * HALF + t * LANES : n * HALF + (t + 1) * LANES] = term


def scan_sums(owner_ref, sums_ref):
    owners = [jnp.concatenate([owner_ref[:, c * HALF : (c + 1) * HALF]] * 2, axis=1) for c in range(2)]
    both = dot_t(jnp.concatenate(owners, axis=0), sums_ref[...])
    lane = iota((LOC, 64), 1)
    part = jnp.where((lane // 4) % 2 == 0, both[:LOC], both[LOC:])
    return jnp.concatenate([part, jnp.zeros((LOC, LANES - 64), F32)], axis=1)


def matrix(owner_ref, sums_ref, column_ref, lhs_ref, block_ref):
    for k, pair in enumerate(PAIRS):
        i, p = SPOT[pair]
        for c in range(2):
            at = p * 8 + c * 4 + i
            mine = owner_ref[:, c * HALF : (c + 1) * HALF]
            for n in range(2):
                row = sums_ref[at : at + 1, n * HALF : (n + 1) * HALF]
                lhs_ref[k * LOC : (k + 1) * LOC, (2 * n + c) * HALF : (2 * n + c + 1) * HALF] = (
                    jnp.broadcast_to(row, (LOC, HALF)) * mine
                )
    block_ref[...] = dot_t(lhs_ref[...], column_ref[...])


def order(p):
    return 2 * (1 - low(p, 1)) + low(p + high(p, 1), 1)


def step_kernel(
    pc_ref, cs_any, ct_any, src_any, sm_any, block_ref, part_ref,
    cs_ref, ct_ref, src_ref, sm_ref, take_ref, pay_ref, first_ref, msg_ref, firsts_ref, recv_ref, table_ref, tile_ref, note_ref,
    x_ref, left_ref, right_ref, back_ref, mid_ref, out_ref, in_ref, turn_ref, owner_ref, sums_ref, column_ref, lhs_ref,
    load_sem, send_p, recv_f, recv_p, send_a, recv_a, send_b, recv_b, send_c, recv_c,
):
    row = lax.axis_index("scan")
    col = lax.axis_index("grp")
    z, y, core = high(row, 3), low(high(row, 1), 2), low(row, 1)
    me = row * NG + col
    chip = high(row, 1)
    barrier = pltpu.get_barrier_semaphore()
    loads = [
        pltpu.make_async_copy(a, b, load_sem.at[n])
        for n, (a, b) in enumerate(
            [(cs_any, cs_ref), (ct_any, ct_ref), (src_any, src_ref)]
            + [(sm_any.at[:, x], sm_ref.at[:, x]) for x in range(3)]
            + [(sm_any.at[:, pl.ds(3, 3)], sm_ref.at[:, pl.ds(3, 3)])]
        )
    ]
    for load in loads:
        load.start()

    def to_all(act):
        @pl.loop(0, 16)
        def _(u):
            uz = low(z + order(high(u, 2)), 2)
            uy = low(y + order(low(u, 2)), 2)
            for dx in (2, 1, 3, 0):
                for dc in (1, 0):
                    there = ((uz * 4 + uy) * 2 + low(core + dc, 1), low(col + dx, 2))
                    if dc == 0 and dx == 0:

                        @pl.when(u < 15)
                        def _():
                            act(*there)

                    else:
                        act(*there)

    to_all(lambda r, c: pl.semaphore_signal(barrier, inc=1, device_id=(r, c), device_id_type=MESH))

    def send(src, dst, sem, recv, r, c, rows):
        pltpu.make_async_remote_copy(
            src_ref=src.at[pl.ds((r * NG + c) * rows, rows)],
            dst_ref=dst.at[pl.ds(me * rows, rows)],
            send_sem=sem,
            recv_sem=recv.at[z],
            device_id=(r, c),
            device_id_type=MESH,
        ).start()

    loads[0].wait()
    loads[1].wait()
    route(cs_ref, ct_ref, take_ref, first_ref, col)
    loads[2].wait()
    for x in range(3):
        loads[3 + x].wait()
        pick_points(x, pc_ref, src_ref, sm_ref, pay_ref.at[x], col)
        if x == 0:
            pack(take_ref, pay_ref.at[x], first_ref, FIRST)
            pl.semaphore_wait(barrier, ND - 1)
            to_all(lambda r, c: send(first_ref, firsts_ref, send_p.at[0], recv_f, r, c, FIRST))
        else:
            msg, got = msg_ref.at[x - 1], recv_ref.at[x - 1]
            pack(take_ref, pay_ref.at[x], msg, CAP)
            to_all(lambda r, c: send(msg, got, send_p.at[x], recv_p, r, c, CAP))
    pltpu.make_async_copy(
        first_ref.at[pl.ds(me * FIRST, FIRST)], firsts_ref.at[pl.ds(me * FIRST, FIRST)], recv_f.at[z]
    ).start()
    pltpu.make_async_copy(
        msg_ref.at[:, pl.ds(me * CAP, CAP)], recv_ref.at[:, pl.ds(me * CAP, CAP)], recv_p.at[z]
    ).start()

    loads[6].wait()
    tile_table(pc_ref, sm_ref, table_ref, col)
    for spot in (7, 10, 11, 12, 13, 14):
        right_ref[:, spot * 16 : (spot + 1) * 16, :] = jnp.zeros((8, 16, 3 * LANES), BF16)

    def cross(ref, plane, got, kind, at):
        return pltpu.make_async_remote_copy(
            src_ref=ref.at[pl.ds(plane * 4, 4)],
            dst_ref=got.at[pl.ds(at * 4, 4)],
            send_sem=send_b.at[kind, plane],
            recv_sem=recv_b.at[kind, at],
            device_id=(row, plane),
            device_id_type=MESH,
        )

    def keep(ref, got, kind):
        return pltpu.make_async_copy(
            ref.at[pl.ds(col * 4, 4)], got.at[pl.ds(col * 4, 4)], recv_b.at[kind, col]
        )

    @pl.loop(0, PLANES)
    def _(u):
        plane = low(z + order(u), 2)
        arrived = firsts_ref.at[pl.ds(plane * (32 * FIRST), 32 * FIRST)]
        pltpu.make_async_copy(arrived, arrived, recv_f.at[plane]).wait()
        fetch_tiles(firsts_ref, plane, table_ref, tile_ref, note_ref, x_ref)
        arrived = recv_ref.at[:, pl.ds(plane * LANES, LANES)]
        pltpu.make_async_copy(arrived, arrived, recv_p.at[plane]).wait()
        plane_sums(plane, x_ref, recv_ref, tile_ref, note_ref, left_ref, right_ref, back_ref)
        for n in (4, 5, 2, 3, 6, 7, 0, 1):
            to_chip = plane * 4 + low(y + n // 2, 2)
            to_row = to_chip * 2 + n % 2
            src = back_ref.at[to_chip, pl.ds(n % 2 * 4, 4)]
            dst = mid_ref.at[chip, pl.ds(core * 4, 4)]

            @pl.when(to_row != row)
            def _():
                pltpu.make_async_remote_copy(
                    src_ref=src,
                    dst_ref=dst,
                    send_sem=send_a,
                    recv_sem=recv_a.at[z],
                    device_id=(to_row, col),
                    device_id_type=MESH,
                ).start()

            @pl.when(to_row == row)
            def _():
                pltpu.make_async_copy(src, dst, recv_a.at[z]).start()

        @pl.when(plane != col)
        def _():
            cross(back_ref, plane, in_ref, 0, col).start()

        @pl.when(plane == col)
        def _():
            keep(back_ref, in_ref, 0).start()

    @pl.loop(0, PLANES)
    def _(u):
        plane = low(z - order(u) + 4, 2)
        arrived = mid_ref.at[pl.ds(plane * 4, 4)]
        pltpu.make_async_copy(arrived, arrived, recv_a.at[plane]).wait()

        @pl.when(plane != col)
        def _():
            cross(mid_ref, plane, out_ref, 1, col).start()

        @pl.when(plane == col)
        def _():
            keep(mid_ref, out_ref, 1).start()

    def spread(to_col, at):
        return pltpu.make_async_remote_copy(
            src_ref=part_ref.at[col],
            dst_ref=part_ref.at[at],
            send_sem=send_c.at[to_col],
            recv_sem=recv_c.at[at],
            device_id=(row, to_col),
            device_id_type=MESH,
        )

    for plane in range(PLANES):
        turn(plane, mid_ref, back_ref, turn_ref)
    arrange(turn_ref, owner_ref, sums_ref, None)
    part_ref[col] = scan_sums(owner_ref, sums_ref)
    for step in (2, 1, 3):
        spread(low(col + step, 2), col).start()

    left = first_ref.at[pl.ds(0, (ND - 1) * FIRST)]
    pltpu.make_async_copy(left, left, send_p.at[0]).wait()
    for x in range(2):
        left = msg_ref.at[x, pl.ds(0, (ND - 1) * CAP)]
        pltpu.make_async_copy(left, left, send_p.at[1 + x]).wait()
    for left in (back_ref.at[pl.ds(0, 15)], back_ref.at[15, pl.ds(0, 4)]):
        pltpu.make_async_copy(left, left, send_a).wait()

    for kind, got in enumerate((in_ref, out_ref)):
        keep(got, got, kind).wait()
        for step in range(1, NG):
            cross(got, 0, got, kind, low(col + step, 2)).wait_recv()
    for plane in range(PLANES):
        turn(plane, out_ref, in_ref, turn_ref)
    arrange(turn_ref, owner_ref, sums_ref, column_ref)
    matrix(owner_ref, sums_ref, column_ref, lhs_ref, block_ref)
    for step in range(1, NG):
        other = low(col + step, 2)
        cross(back_ref, other, in_ref, 0, col).wait_send()
        cross(mid_ref, other, out_ref, 1, col).wait_send()
        spread(other, col).wait_send()
        spread(other, other).wait_recv()


def finish_kernel(block_ref, part_ref, hess_ref, grad_ref):
    row = lax.axis_index("scan")
    col = lax.axis_index("grp")
    total = part_ref[0] + part_ref[1] + part_ref[2] + part_ref[3]
    total = total + pltpu.roll(total, LANES - 4, 1)
    lane = iota((LOC, LANES), 1)
    diag = (lane == iota((LOC, LANES), 0) + LOC * (row % 8)) & (row // 8 == col)
    for k, (i, j) in enumerate(PAIRS):
        at = SPOT[i, j][1] * 8 + SPOT[i, j][0]
        value = block_ref[k * LOC : (k + 1) * LOC, :] + jnp.where(
            diag, jnp.broadcast_to(total[:, at : at + 1], (LOC, LANES)), 0.0
        )
        hess_ref[i, j] = value
        if i != j:
            hess_ref[j, i] = value
    some = jnp.zeros((4, LANES), F32)
    for n in range(NG):
        some = jnp.where(col == n, total[n * 4 : (n + 1) * 4, :], some)
    at = [SPOT[i, 6][1] * 8 + SPOT[i, 6][0] for i in range(6)]
    grad_ref[...] = jnp.concatenate([some[:, a : a + 1] for a in at], axis=1)


def vmem(count):
    return [pl.BlockSpec(memory_space=pltpu.VMEM)] * count


def local(samples, point_count, corr_scan, corr_tile, corr_src):
    dma = pltpu.SemaphoreType.DMA
    block, parts = pl.pallas_call(
        step_kernel,
        out_shape=(
            jax.ShapeDtypeStruct((len(PAIRS) * LOC, LANES), F32),
            jax.ShapeDtypeStruct((NG, LOC, LANES), F32),
        ),
        in_specs=[pl.BlockSpec(memory_space=pltpu.SMEM)] + [pl.BlockSpec(memory_space=pl.ANY)] * 4,
        out_specs=tuple(vmem(2)),
        scratch_shapes=[
            pltpu.VMEM((LOC, CT), I32),
            pltpu.VMEM((LOC, CT), I32),
            pltpu.VMEM((LOC, CT, LANES), I32),
            pltpu.VMEM((LOC, 6, TL, LANES), F32),
            pltpu.VMEM((SLOTS, 3 * REQ), BF16),
            pltpu.VMEM((3, 3 * REQ, LANES), BF16),
            pltpu.VMEM((ND * FIRST, LANES), F32),
            pltpu.VMEM((2, SLOTS, LANES), F32),
            pltpu.VMEM((ND * FIRST, LANES), F32),
            pltpu.VMEM((2, SLOTS, LANES), F32),
            pltpu.VMEM((3 * LOC * TL, 6 * LANES), BF16),
            pltpu.VMEM((LANES, 6 * LANES), F32),
            pltpu.VMEM((32, LANES), F32),
            pltpu.VMEM((LANES, LANES), F32),
            pltpu.VMEM((8, 6 * 16, 3 * LANES), BF16),
            pltpu.VMEM((8, 16 * 16, 3 * LANES), BF16),
            pltpu.VMEM((16, 8, LANES), F32),
            pltpu.VMEM((16, 8, LANES), F32),
            pltpu.VMEM((16, 8, LANES), F32),
            pltpu.VMEM((16, 8, LANES), F32),
            pltpu.VMEM((PLANES, 8, 8, LANES), F32),
            pltpu.VMEM((LOC, 2 * HALF), BF16),
            pltpu.VMEM((64, 2 * HALF), BF16),
            pltpu.VMEM((LANES, 4 * HALF), BF16),
            pltpu.VMEM((len(PAIRS) * LOC, 4 * HALF), BF16),
            dma((7,)),
            dma((3,)),
            dma((PLANES,)),
            dma((PLANES,)),
            dma,
            dma((PLANES,)),
            dma((2, NG)),
            dma((2, NG)),
            dma((NG,)),
            dma((NG,)),
        ],
        compiler_params=pltpu.CompilerParams(collective_id=0, has_side_effects=True),
        name="step",
    )(point_count, corr_scan, corr_tile, corr_src, samples.transpose(0, 2, 1, 3))
    hessian, gradient = pl.pallas_call(
        finish_kernel,
        out_shape=(
            jax.ShapeDtypeStruct((6, 6, LOC, LANES), F32),
            jax.ShapeDtypeStruct((4, 6), F32),
        ),
        in_specs=vmem(2),
        out_specs=tuple(vmem(2)),
        name="finish",
    )(block, parts)
    return hessian.transpose(2, 0, 1, 3), gradient


def solution(mesh):
    placed = (
        P("scan", "grp", None, None),
        P("scan"),
        P("scan", "grp"),
        P("scan", "grp"),
        P("scan", "grp", None),
    )
    return jax.shard_map(
        local,
        mesh=mesh,
        in_specs=placed,
        out_specs=(P("scan", None, None, "grp"), P(("scan", "grp"), None)),
        check_vma=False,
    )
```

```python
import functools

import jax
import jax.numpy as jnp
from jax import lax
from jax.experimental import pallas as pl
from jax.experimental.pallas import tpu as pltpu
from jax.sharding import PartitionSpec as P

F32 = jnp.float32
BF16 = jnp.bfloat16
I32 = jnp.int32
MESH = pl.DeviceIdType.MESH

NS = 32
NG = 4
ND = NS * NG
LOC = 16
TL = 16
CT = 16
REQ = LOC * CT
CAP = 4
FAR = 1000.0
LANES = 128
PAIRS = [(i, j) for i in range(6) for j in range(i, 6)]
PLANES = 4
SLOTS = ND * CAP
HALF = PLANES * LANES
SPOT = {(i, j): (i, j) for i in range(4) for j in range(i, 7)}
SPOT |= {(5, 5): (1, 0), (5, 6): (1, 7), (4, 4): (2, 1), (4, 5): (2, 0), (4, 6): (2, 7)}


def iota(shape, dim):
    return lax.broadcasted_iota(I32, shape, dim)


def dot(a, b):
    return lax.dot_general(a, b, (((1,), (0,)), ((), ())), preferred_element_type=F32)


def dot_t(a, b):
    return lax.dot_general(a, b, (((1,), (1,)), ((), ())), preferred_element_type=F32)


def parts_of(x, count):
    terms = []
    for _ in range(count):
        term = x.astype(BF16)
        terms.append(term)
        x = x - term.astype(F32)
    return terms


def onehot(cond):
    return jnp.where(cond, 1.0, 0.0).astype(BF16)


def low(x, bits):
    return lax.bitwise_and(x, (1 << bits) - 1)


def high(x, bits):
    return lax.shift_right_logical(x, bits)


def pick_points(pc_ref, src_ref, sm_ref, pay_ref, group):
    first = group * (TL * LANES)
    for s in range(LOC):
        picks = src_ref[s]
        halves = []
        for h in range(2):
            part = picks[h * 8 : h * 8 + 8]
            tile = high(part, 7)
            lane = low(part, 7)
            acc = [jnp.zeros((8, LANES), F32) for _ in range(3)]
            for t in range(TL):
                here = tile == t
                for x in range(3):
                    row = jnp.broadcast_to(sm_ref[s, x, t : t + 1, :], (8, LANES))
                    got = jnp.take_along_axis(row, lane, axis=1, mode="promise_in_bounds")
                    acc[x] = jnp.where(here, got, acc[x])
            acc[0] = jnp.where(first + part < pc_ref[s], acc[0], FAR)
            halves.append(acc)
        for x in range(3):
            both = jnp.concatenate([halves[0][x], halves[1][x]], axis=0)
            for n, term in enumerate(parts_of(both, 3)):
                pay_ref[n * REQ + s * CT : n * REQ + (s + 1) * CT, x * LANES : (x + 1) * LANES] = term


def route(cs_ref, ct_ref, take_ref, code_ref, group):
    cs = cs_ref[...]
    ct = ct_ref[...]
    dest = (high(cs, 4) * NG + high(ct, 4)).astype(F32)
    code = (low(cs, 4) * TL + low(ct, 4) + 1).astype(F32)
    wide = dot(dest.astype(BF16), onehot(iota((CT, REQ), 1) % CT == iota((CT, REQ), 0)))
    wide = jnp.where(iota((LOC, REQ), 1) // CT == iota((LOC, REQ), 0), wide, 0.0)
    dest_t = dot(jnp.ones((ND, LOC), BF16), wide.astype(BF16))
    to_me = dest_t == iota((ND, REQ), 0).astype(F32)
    rank = dot(onehot(to_me), onehot(iota((REQ, REQ), 0) < iota((REQ, REQ), 1)))
    takes = [onehot(to_me & (rank == float(r))) for r in range(CAP)]
    for r in range(CAP):
        for n in range(3):
            take_ref[r * ND : (r + 1) * ND, n * REQ : (n + 1) * REQ] = takes[r]
    tall = dot(onehot(iota((REQ, LOC), 0) // CT == iota((REQ, LOC), 1)), code.astype(BF16))
    tall = jnp.where(iota((REQ, CT), 0) % CT == iota((REQ, CT), 1), tall, 0.0)
    code_b = dot(tall.astype(BF16), jnp.ones((CT, LANES), BF16))
    target = high(code_b.astype(I32) - 1, 4).astype(F32)
    source = (iota((REQ, LANES), 0) // CT).astype(F32)
    lane = iota((REQ, LANES), 1)
    codes = jnp.where(lane < 16, source, jnp.where(lane < 32, target, code_b)).astype(BF16)
    lane = iota((ND, LANES), 1)
    row = jnp.zeros((ND, LANES), F32)
    for r in range(CAP):
        at = group * CAP + r
        here = (lane == at) | (lane == 16 + at) | (lane == 32 + r)
        row = jnp.where(here, dot(takes[r], codes), row)
    code_ref[...] = row


def pack(take_ref, pay_ref, msg_ref):
    got = dot(take_ref[...], pay_ref[...])
    for r in range(CAP):
        for x in range(3):
            msg_ref[x, pl.ds(r, ND, stride=CAP), :] = got[r * ND : (r + 1) * ND, x * LANES : (x + 1) * LANES]


def tile_table(pc_ref, sm_ref, table_ref, group):
    point = (group * TL + iota((TL, LANES), 0)) * LANES + iota((TL, LANES), 1)

    @pl.loop(0, LOC)
    def _(s):
        valid = point < pc_ref[s]
        at = pl.multiple_of(s * TL, TL)
        for x in range(6):
            value = sm_ref[s, x]
            if x >= 3:
                value = jnp.where(valid, value, 0.0)
            for n, term in enumerate(parts_of(value, 3)):
                table_ref[pl.ds(n * LOC * TL + at, TL), x * LANES : (x + 1) * LANES] = term


def fetch_tiles(code_ref, table_ref, tile_ref, note_ref):
    codes = code_ref[...].astype(BF16)
    spread = dot(onehot(iota((SLOTS, ND), 0) // CAP == iota((SLOTS, ND), 1)), codes)
    spread = jnp.where(iota((SLOTS, LANES), 1) == 32 + iota((SLOTS, LANES), 0) % CAP, spread, 0.0)
    wanted = dot(spread.astype(BF16), jnp.ones((LANES, LOC * TL), BF16))
    take = onehot(wanted == (iota((SLOTS, LOC * TL), 1) + 1).astype(F32))
    tile_ref[...] = dot(jnp.concatenate([take] * 3, axis=1), table_ref[...])
    here = iota((ND, ND), 0)
    note_ref[...] = dot(onehot((here // 4 == iota((ND, ND), 1) // 4) & (here % 4 == 3)), codes)


def fold(a, b, clear, shift):
    return jnp.where(clear, a, b) + pltpu.roll(jnp.where(clear, b, a), shift, 0)


def group_sums(group, recv_ref, tile_ref, note_ref, left_ref, right_ref, back_ref):
    at = pl.multiple_of(group * LANES, LANES)
    p = [recv_ref[x, pl.ds(at, LANES), :] for x in range(3)]
    tile = [tile_ref[pl.ds(at, LANES), x * LANES : (x + 1) * LANES] for x in range(6)]
    q, n = tile[:3], tile[3:]
    counts = p[0] < 0.5 * FAR
    p[0] = jnp.where(counts, p[0], 0.0)
    res = n[0] * (p[0] - q[0]) + n[1] * (p[1] - q[1]) + n[2] * (p[2] - q[2])
    w = jnp.where(counts, 1.0 / (1.0 + res * res), 0.0)
    jac = [
        p[1] * n[2] - p[2] * n[1],
        p[2] * n[0] - p[0] * n[2],
        p[0] * n[1] - p[1] * n[0],
        n[0],
        n[1],
        n[2],
    ]
    for i in range(6):
        big, small = parts_of(w * jac[i], 2)
        for r in range(8):
            for k, term in enumerate((big, big, small)):
                left_ref[r, i * 16 : (i + 1) * 16, k * LANES : (k + 1) * LANES] = term[r * 16 : (r + 1) * 16]
    for j, value in enumerate(jac + [res]):
        big, small = parts_of(value, 2)
        spots = [j] + {4: [9], 5: [8], 6: [15]}.get(j, [])
        for r in range(8):
            for k, term in enumerate((big, small, big)):
                for spot in spots:
                    right_ref[r, spot * 16 : (spot + 1) * 16, k * LANES : (k + 1) * LANES] = term[r * 16 : (r + 1) * 16]
    lane = iota((8, LANES), 1)
    sub = iota((8, LANES), 0)
    spot = lane // 16
    first = [spot < 8, (spot >= 1) & (spot <= 6), (spot >= 2) & (spot <= 6), spot < 8]
    other = [None, 5, 4, None]
    for chip in range(4):
        arrays = []
        for c in range(2):
            r = chip * 2 + c
            every = dot_t(left_ref[r], right_ref[r])
            for i in range(4):
                kept = jnp.zeros((8, LANES), F32)
                for h in range(2):
                    value = every[i * 16 + h * 8 : i * 16 + h * 8 + 8, :LANES]
                    if other[i] is not None:
                        o = other[i] * 16 + h * 8
                        value = jnp.where(first[i], value, every[o : o + 8, LANES:])
                    kept = jnp.where(lane % 16 == h * 8 + sub, value, kept)
                arrays.append(kept)
        for level in range(3):
            clear = (sub // (1 << level)) % 2 == 0
            arrays = [fold(arrays[n], arrays[n + 1], clear, 1 << level) for n in range(0, len(arrays), 2)]
        note = note_ref[pl.ds(group * 32 + chip * 8, 8), :]
        back_ref[chip * 4 + low(group - chip + 4, 2)] = jnp.where((sub % 4 == 3) & (spot < 3), note, arrays[0])


def turn(plane, partner_ref, source_ref, turn_ref):
    lane = iota((8, LANES), 1)
    blocks = [ref[plane * 4 + m] for ref in (partner_ref, source_ref) for m in range(4)]
    for bit in range(3):
        shift = 16 << bit
        clear = (lane // shift) % 2 == 0
        for m in range(8):
            if (m >> bit) % 2 == 0:
                a, b = blocks[m], blocks[m + (1 << bit)]
                blocks[m] = jnp.where(clear, a, pltpu.roll(b, shift, 1))
                blocks[m + (1 << bit)] = jnp.where(clear, pltpu.roll(a, LANES - shift, 1), b)
    for n in range(8):
        turn_ref[plane, n] = jnp.where(lane < 64, blocks[n], -blocks[n]) if n >= 6 else blocks[n]


def arrange(turn_ref, owner_ref, sums_ref, column_ref):
    lane = iota((1, LANES), 1)
    y = (lane // 16) % 4
    for t in range(PLANES):
        source = turn_ref[t, 0]
        target = turn_ref[t, 1]
        for c in range(2):
            s = source[c * 4 + 3 : c * 4 + 4, :]
            b = target[c * 4 + 3 : c * 4 + 4, :]
            owner = jnp.broadcast_to(jnp.where(lane < 64, s, b), (LOC, LANES))
            at = c * HALF + t * LANES
            owner_ref[:, at : at + LANES] = onehot(owner == iota((LOC, LANES), 0).astype(F32))
            if column_ref is not None:
                column = jnp.where(lane < 64, b, s) + (16 * (2 * y + c)).astype(F32)
                there = jnp.broadcast_to(column, (LANES, LANES)) == iota((LANES, LANES), 0).astype(F32)
                there = jnp.where(there, -1.0, 0.0).astype(BF16)
                for n in range(2):
                    column_ref[:, n * 2 * HALF + at : n * 2 * HALF + at + LANES] = there
        for p in range(0, 8, 2):
            pair = jnp.concatenate([turn_ref[t, p], turn_ref[t, p + 1]], axis=0)
            for n, term in enumerate(parts_of(pair, 2)):
                sums_ref[p * 8 : p * 8 + 16, n * HALF + t * LANES : n * HALF + (t + 1) * LANES] = term


def scan_sums(owner_ref, sums_ref):
    owners = [jnp.concatenate([owner_ref[:, c * HALF : (c + 1) * HALF]] * 2, axis=1) for c in range(2)]
    both = dot_t(jnp.concatenate(owners, axis=0), sums_ref[...])
    lane = iota((LOC, 64), 1)
    part = jnp.where((lane // 4) % 2 == 0, both[:LOC], both[LOC:])
    return jnp.concatenate([part, jnp.zeros((LOC, LANES - 64), F32)], axis=1)


def matrix(owner_ref, sums_ref, column_ref, lhs_ref, block_ref):
    for k, pair in enumerate(PAIRS):
        i, p = SPOT[pair]
        for c in range(2):
            at = p * 8 + c * 4 + i
            mine = owner_ref[:, c * HALF : (c + 1) * HALF]
            for n in range(2):
                row = sums_ref[at : at + 1, n * HALF : (n + 1) * HALF]
                lhs_ref[k * LOC : (k + 1) * LOC, (2 * n + c) * HALF : (2 * n + c + 1) * HALF] = (
                    jnp.broadcast_to(row, (LOC, HALF)) * mine
                )
    block_ref[...] = dot_t(lhs_ref[...], column_ref[...])


def order(p):
    return 2 * high(p, 1) + low(p + high(p, 1), 1)


def step_kernel(
    pc_any, cs_any, ct_any, src_any, sm_any, block_ref, part_ref,
    pc_ref, cs_ref, ct_ref, src_ref, sm_ref, take_ref, pay_ref, code_ref, msg_ref, codes_ref, recv_ref, table_ref, tile_ref,
    note_ref, left_ref, right_ref, back_ref, mid_ref, out_ref, in_ref, turn_ref, owner_ref, sums_ref, column_ref, lhs_ref,
    load_sem, send_n, send_p, recv_n, recv_p, send_a, recv_a, send_b, recv_b, send_c, recv_c,
):
    row = lax.axis_index("scan")
    col = lax.axis_index("grp")
    z, y, core = high(row, 3), low(high(row, 1), 2), low(row, 1)
    me = row * NG + col
    chip = high(row, 1)
    group = low(y + z, 2)
    place = group * 32 + z * 8 + core * NG + col
    barrier = pltpu.get_barrier_semaphore()
    loads = [
        pltpu.make_async_copy(a, b, load_sem.at[n])
        for n, (a, b) in enumerate(
            [
                (cs_any, cs_ref),
                (ct_any, ct_ref),
                (src_any, src_ref),
                (pc_any, pc_ref),
                (sm_any.at[:, pl.ds(0, 3)], sm_ref.at[:, pl.ds(0, 3)]),
                (sm_any.at[:, pl.ds(3, 3)], sm_ref.at[:, pl.ds(3, 3)]),
            ]
        )
    ]
    for load in loads:
        load.start()

    def to_all(act):
        @pl.loop(0, 16)
        def _(u):
            dz = low(u + 2, 2)
            uz = low(z + dz, 2)
            uy = low(y + order(high(u, 2)) - dz + 4, 2)
            for dx in (2, 1, 3, 0):
                for dc in (1, 0):
                    there = ((uz * 4 + uy) * 2 + low(core + dc, 1), low(col + dx, 2))
                    if dc == 0 and dx == 0:

                        @pl.when(u != 2)
                        def _():
                            act(*there)

                    else:
                        act(*there)

    to_all(lambda r, c: pl.semaphore_signal(barrier, inc=1, device_id=(r, c), device_id_type=MESH))

    def send_codes(r, c):
        pltpu.make_async_remote_copy(
            src_ref=code_ref.at[pl.ds(r * NG + c, 1)],
            dst_ref=codes_ref.at[pl.ds(place, 1)],
            send_sem=send_n,
            recv_sem=recv_n,
            device_id=(r, c),
            device_id_type=MESH,
        ).start()

    def send_points(r, c):
        for x in range(3):
            pltpu.make_async_remote_copy(
                src_ref=msg_ref.at[x, pl.ds((r * NG + c) * CAP, CAP)],
                dst_ref=recv_ref.at[x, pl.ds(place * CAP, CAP)],
                send_sem=send_p,
                recv_sem=recv_p.at[group],
                device_id=(r, c),
                device_id_type=MESH,
            ).start()

    for n in range(5):
        loads[n].wait()
    route(cs_ref, ct_ref, take_ref, code_ref, col)
    pick_points(pc_ref, src_ref, sm_ref, pay_ref, col)
    pack(take_ref, pay_ref, msg_ref)
    pl.semaphore_wait(barrier, ND - 1)
    to_all(send_codes)
    to_all(send_points)
    pltpu.make_async_copy(code_ref.at[pl.ds(me, 1)], codes_ref.at[pl.ds(place, 1)], recv_n).start()
    pltpu.make_async_copy(
        msg_ref.at[:, pl.ds(me * CAP, CAP)], recv_ref.at[:, pl.ds(place * CAP, CAP)], recv_p.at[group]
    ).start()

    loads[5].wait()
    tile_table(pc_ref, sm_ref, table_ref, col)
    for spot in (7, 10, 11, 12, 13, 14):
        right_ref[:, spot * 16 : (spot + 1) * 16, :] = jnp.zeros((8, 16, 3 * LANES), BF16)
    pltpu.make_async_copy(codes_ref, codes_ref, recv_n).wait()
    fetch_tiles(codes_ref, table_ref, tile_ref, note_ref)

    def cross_all(block_of, which, got, kind):
        for plane in range(PLANES):
            at = low(which - plane + 4, 2)
            src = block_of(plane, at)

            @pl.when(plane != col)
            def _():
                pltpu.make_async_remote_copy(
                    src_ref=src,
                    dst_ref=got.at[col * 4 + at],
                    send_sem=send_b.at[kind, plane],
                    recv_sem=recv_b.at[kind, col],
                    device_id=(row, plane),
                    device_id_type=MESH,
                ).start()

            @pl.when(plane == col)
            def _():
                pltpu.make_async_copy(src, got.at[plane * 4 + at], recv_b.at[kind, plane]).start()

    @pl.loop(0, PLANES)
    def _(u):
        which = low(group - order(u) + 4, 2)
        arrived = recv_ref.at[:, pl.ds(which * LANES, LANES)]
        pltpu.make_async_copy(arrived, arrived, recv_p.at[which]).wait()
        group_sums(which, recv_ref, tile_ref, note_ref, left_ref, right_ref, back_ref)
        for n in range(8):
            to_z = n // 2
            to_chip = to_z * 4 + low(which - to_z + 4, 2)
            to_row = to_chip * 2 + n % 2
            src = back_ref.at[to_chip, pl.ds(n % 2 * 4, 4)]
            dst = mid_ref.at[group * 4 + z, pl.ds(core * 4, 4)]

            @pl.when(to_row != row)
            def _():
                pltpu.make_async_remote_copy(
                    src_ref=src,
                    dst_ref=dst,
                    send_sem=send_a,
                    recv_sem=recv_a.at[group],
                    device_id=(to_row, col),
                    device_id_type=MESH,
                ).start()

            @pl.when(to_row == row)
            def _():
                pltpu.make_async_copy(src, dst, recv_a.at[group]).start()

        cross_all(lambda plane, at: back_ref.at[plane * 4 + at], which, in_ref, 0)

    @pl.loop(0, PLANES)
    def _(u):
        which = low(group + order(u), 2)
        arrived = mid_ref.at[pl.ds(which * 4, 4)]
        pltpu.make_async_copy(arrived, arrived, recv_a.at[which]).wait()
        cross_all(lambda plane, at: mid_ref.at[which * 4 + plane], which, out_ref, 1)

    def spread(to_col, at):
        return pltpu.make_async_remote_copy(
            src_ref=part_ref.at[col],
            dst_ref=part_ref.at[at],
            send_sem=send_c.at[to_col],
            recv_sem=recv_c.at[at],
            device_id=(row, to_col),
            device_id_type=MESH,
        )

    for plane in range(PLANES):
        turn(plane, mid_ref, back_ref, turn_ref)
    arrange(turn_ref, owner_ref, sums_ref, None)
    part_ref[col] = scan_sums(owner_ref, sums_ref)
    for step in (2, 1, 3):
        spread(low(col + step, 2), col).start()

    left = code_ref.at[pl.ds(0, ND - 1)]
    pltpu.make_async_copy(left, left, send_n).wait()
    left = msg_ref.at[:, pl.ds(0, (ND - 1) * CAP)]
    pltpu.make_async_copy(left, left, send_p).wait()
    for left in (back_ref.at[pl.ds(0, 15)], back_ref.at[15, pl.ds(0, 4)]):
        pltpu.make_async_copy(left, left, send_a).wait()

    for kind, got in enumerate((in_ref, out_ref)):
        for source in range(NG):
            arrived = got.at[pl.ds(source * 4, 4)]
            pltpu.make_async_copy(arrived, arrived, recv_b.at[kind, source]).wait()
    for plane in range(PLANES):
        turn(plane, out_ref, in_ref, turn_ref)
    arrange(turn_ref, owner_ref, sums_ref, column_ref)
    matrix(owner_ref, sums_ref, column_ref, lhs_ref, block_ref)
    for step in range(1, NG):
        other = low(col + step, 2)
        for kind in range(2):
            left = back_ref.at[pl.ds(0, 4)]
            pltpu.make_async_copy(left, left, send_b.at[kind, other]).wait()
        spread(other, col).wait_send()
        spread(other, other).wait_recv()


def finish_kernel(block_ref, part_ref, hess_ref, grad_ref):
    row = lax.axis_index("scan")
    col = lax.axis_index("grp")
    total = part_ref[0] + part_ref[1] + part_ref[2] + part_ref[3]
    total = total + pltpu.roll(total, LANES - 4, 1)
    lane = iota((LOC, LANES), 1)
    diag = (lane == iota((LOC, LANES), 0) + LOC * (row % 8)) & (row // 8 == col)
    for k, (i, j) in enumerate(PAIRS):
        at = SPOT[i, j][1] * 8 + SPOT[i, j][0]
        value = block_ref[k * LOC : (k + 1) * LOC, :] + jnp.where(
            diag, jnp.broadcast_to(total[:, at : at + 1], (LOC, LANES)), 0.0
        )
        hess_ref[i, j] = value
        if i != j:
            hess_ref[j, i] = value
    some = jnp.zeros((4, LANES), F32)
    for n in range(NG):
        some = jnp.where(col == n, total[n * 4 : (n + 1) * 4, :], some)
    at = [SPOT[i, 6][1] * 8 + SPOT[i, 6][0] for i in range(6)]
    grad_ref[...] = jnp.concatenate([some[:, a : a + 1] for a in at], axis=1)


def vmem(count):
    return [pl.BlockSpec(memory_space=pltpu.VMEM)] * count


def local(samples, point_count, corr_scan, corr_tile, corr_src):
    dma = pltpu.SemaphoreType.DMA
    block, parts = pl.pallas_call(
        step_kernel,
        out_shape=(
            jax.ShapeDtypeStruct((len(PAIRS) * LOC, LANES), F32),
            jax.ShapeDtypeStruct((NG, LOC, LANES), F32),
        ),
        in_specs=[pl.BlockSpec(memory_space=pl.ANY)] * 5,
        out_specs=tuple(vmem(2)),
        scratch_shapes=[
            pltpu.SMEM((LOC,), I32),
            pltpu.VMEM((LOC, CT), I32),
            pltpu.VMEM((LOC, CT), I32),
            pltpu.VMEM((LOC, CT, LANES), I32),
            pltpu.VMEM((LOC, 6, TL, LANES), F32),
            pltpu.VMEM((SLOTS, 3 * REQ), BF16),
            pltpu.VMEM((3 * REQ, 3 * LANES), BF16),
            pltpu.VMEM((ND, LANES), F32),
            pltpu.VMEM((3, SLOTS, LANES), F32),
            pltpu.VMEM((ND, LANES), F32),
            pltpu.VMEM((3, SLOTS, LANES), F32),
            pltpu.VMEM((3 * LOC * TL, 6 * LANES), BF16),
            pltpu.VMEM((SLOTS, 6 * LANES), F32),
            pltpu.VMEM((ND, LANES), F32),
            pltpu.VMEM((8, 6 * 16, 3 * LANES), BF16),
            pltpu.VMEM((8, 16 * 16, 3 * LANES), BF16),
            pltpu.VMEM((16, 8, LANES), F32),
            pltpu.VMEM((16, 8, LANES), F32),
            pltpu.VMEM((16, 8, LANES), F32),
            pltpu.VMEM((16, 8, LANES), F32),
            pltpu.VMEM((PLANES, 8, 8, LANES), F32),
            pltpu.VMEM((LOC, 2 * HALF), BF16),
            pltpu.VMEM((64, 2 * HALF), BF16),
            pltpu.VMEM((LANES, 4 * HALF), BF16),
            pltpu.VMEM((len(PAIRS) * LOC, 4 * HALF), BF16),
            dma((6,)),
            dma,
            dma,
            dma,
            dma((PLANES,)),
            dma,
            dma((PLANES,)),
            dma((2, NG)),
            dma((2, NG)),
            dma((NG,)),
            dma((NG,)),
        ],
        compiler_params=pltpu.CompilerParams(collective_id=0, has_side_effects=True),
        name="step",
    )(point_count, corr_scan, corr_tile, corr_src, samples.transpose(0, 2, 1, 3))
    hessian, gradient = pl.pallas_call(
        finish_kernel,
        out_shape=(
            jax.ShapeDtypeStruct((6, 6, LOC, LANES), F32),
            jax.ShapeDtypeStruct((4, 6), F32),
        ),
        in_specs=vmem(2),
        out_specs=tuple(vmem(2)),
        name="finish",
    )(block, parts)
    return hessian.transpose(2, 0, 1, 3), gradient


def solution(mesh):
    placed = (
        P("scan", "grp", None, None),
        P("scan"),
        P("scan", "grp"),
        P("scan", "grp"),
        P("scan", "grp", None),
    )
    return jax.shard_map(
        local,
        mesh=mesh,
        in_specs=placed,
        out_specs=(P("scan", None, None, "grp"), P(("scan", "grp"), None)),
        check_vma=False,
    )
```

```python
import functools

import jax
import jax.numpy as jnp
from jax import lax
from jax.experimental import pallas as pl
from jax.experimental.pallas import tpu as pltpu
from jax.sharding import PartitionSpec as P

F32 = jnp.float32
BF16 = jnp.bfloat16
I32 = jnp.int32
MESH = pl.DeviceIdType.MESH

NS = 32
NG = 4
ND = NS * NG
LOC = 16
TL = 16
CT = 16
REQ = LOC * CT
CAP = 4
FAR = 1000.0
LANES = 128
PAIRS = [(i, j) for i in range(6) for j in range(i, 6)]
PLANES = 4
SLOTS = ND * CAP
HALF = PLANES * LANES
SPOT = {(i, j): (i, j) for i in range(4) for j in range(i, 7)}
SPOT |= {(5, 5): (1, 0), (5, 6): (1, 7), (4, 4): (2, 1), (4, 5): (2, 0), (4, 6): (2, 7)}


def iota(shape, dim):
    return lax.broadcasted_iota(I32, shape, dim)


def dot(a, b):
    return lax.dot_general(a, b, (((1,), (0,)), ((), ())), preferred_element_type=F32)


def dot_t(a, b):
    return lax.dot_general(a, b, (((1,), (1,)), ((), ())), preferred_element_type=F32)


def parts_of(x, count):
    terms = []
    for _ in range(count):
        term = x.astype(BF16)
        terms.append(term)
        x = x - term.astype(F32)
    return terms


def onehot(cond):
    return jnp.where(cond, 1.0, 0.0).astype(BF16)


def low(x, bits):
    return lax.bitwise_and(x, (1 << bits) - 1)


def high(x, bits):
    return lax.shift_right_logical(x, bits)


def pick_points(pc_ref, src_ref, sm_ref, pay_ref, group):
    first = group * (TL * LANES)
    for s in range(LOC):
        picks = src_ref[s]
        halves = []
        for h in range(2):
            part = picks[h * 8 : h * 8 + 8]
            tile = high(part, 7)
            lane = low(part, 7)
            acc = [jnp.zeros((8, LANES), F32) for _ in range(3)]
            for t in range(TL):
                here = tile == t
                for x in range(3):
                    row = jnp.broadcast_to(sm_ref[s, x, t : t + 1, :], (8, LANES))
                    got = jnp.take_along_axis(row, lane, axis=1, mode="promise_in_bounds")
                    acc[x] = jnp.where(here, got, acc[x])
            acc[0] = jnp.where(first + part < pc_ref[s], acc[0], FAR)
            halves.append(acc)
        for x in range(3):
            both = jnp.concatenate([halves[0][x], halves[1][x]], axis=0)
            for n, term in enumerate(parts_of(both, 3)):
                pay_ref[n * REQ + s * CT : n * REQ + (s + 1) * CT, x * LANES : (x + 1) * LANES] = term


def route(cs_ref, ct_ref, take_ref, code_ref, group):
    cs = cs_ref[...]
    ct = ct_ref[...]
    dest = (high(cs, 4) * NG + high(ct, 4)).astype(F32)
    code = (low(cs, 4) * TL + low(ct, 4) + 1).astype(F32)
    wide = dot(dest.astype(BF16), onehot(iota((CT, REQ), 1) % CT == iota((CT, REQ), 0)))
    wide = jnp.where(iota((LOC, REQ), 1) // CT == iota((LOC, REQ), 0), wide, 0.0)
    dest_t = dot(jnp.ones((ND, LOC), BF16), wide.astype(BF16))
    to_me = dest_t == iota((ND, REQ), 0).astype(F32)
    rank = dot(onehot(to_me), onehot(iota((REQ, REQ), 0) < iota((REQ, REQ), 1)))
    takes = [onehot(to_me & (rank == float(r))) for r in range(CAP)]
    for r in range(CAP):
        for n in range(3):
            take_ref[r * ND : (r + 1) * ND, n * REQ : (n + 1) * REQ] = takes[r]
    tall = dot(onehot(iota((REQ, LOC), 0) // CT == iota((REQ, LOC), 1)), code.astype(BF16))
    tall = jnp.where(iota((REQ, CT), 0) % CT == iota((REQ, CT), 1), tall, 0.0)
    code_b = dot(tall.astype(BF16), jnp.ones((CT, LANES), BF16))
    target = high(code_b.astype(I32) - 1, 4).astype(F32)
    source = (iota((REQ, LANES), 0) // CT).astype(F32)
    lane = iota((REQ, LANES), 1)
    codes = jnp.where(lane < 16, source, jnp.where(lane < 32, target, code_b)).astype(BF16)
    lane = iota((ND, LANES), 1)
    row = jnp.zeros((ND, LANES), F32)
    for r in range(CAP):
        at = group * CAP + r
        here = (lane == at) | (lane == 16 + at) | (lane == 32 + r)
        row = jnp.where(here, dot(takes[r], codes), row)
    code_ref[...] = row


def pack(take_ref, pay_ref, msg_ref):
    got = dot(take_ref[...], pay_ref[...])
    for r in range(CAP):
        for x in range(3):
            msg_ref[x, pl.ds(r, ND, stride=CAP), :] = got[r * ND : (r + 1) * ND, x * LANES : (x + 1) * LANES]


def tile_table(pc_ref, sm_ref, table_ref, group):
    point = (group * TL + iota((TL, LANES), 0)) * LANES + iota((TL, LANES), 1)

    @pl.loop(0, LOC)
    def _(s):
        valid = point < pc_ref[s]
        at = pl.multiple_of(s * TL, TL)
        for x in range(6):
            value = sm_ref[s, x]
            if x >= 3:
                value = jnp.where(valid, value, 0.0)
            for n, term in enumerate(parts_of(value, 3)):
                table_ref[pl.ds(n * LOC * TL + at, TL), x * LANES : (x + 1) * LANES] = term


def fetch_tiles(code_ref, table_ref, tile_ref, note_ref):
    codes = code_ref[...].astype(BF16)
    spread = dot(onehot(iota((SLOTS, ND), 0) // CAP == iota((SLOTS, ND), 1)), codes)
    spread = jnp.where(iota((SLOTS, LANES), 1) == 32 + iota((SLOTS, LANES), 0) % CAP, spread, 0.0)
    wanted = dot(spread.astype(BF16), jnp.ones((LANES, LOC * TL), BF16))
    take = onehot(wanted == (iota((SLOTS, LOC * TL), 1) + 1).astype(F32))
    tile_ref[...] = dot(jnp.concatenate([take] * 3, axis=1), table_ref[...])
    here = iota((ND, ND), 0)
    note_ref[...] = dot(onehot((here // 4 == iota((ND, ND), 1) // 4) & (here % 4 == 3)), codes)


def fold(a, b, clear, shift):
    return jnp.where(clear, a, b) + pltpu.roll(jnp.where(clear, b, a), shift, 0)


def group_sums(group, recv_ref, tile_ref, note_ref, left_ref, right_ref, back_ref):
    at = pl.multiple_of(group * LANES, LANES)
    p = [recv_ref[x, pl.ds(at, LANES), :] for x in range(3)]
    tile = [tile_ref[pl.ds(at, LANES), x * LANES : (x + 1) * LANES] for x in range(6)]
    q, n = tile[:3], tile[3:]
    counts = p[0] < 0.5 * FAR
    p[0] = jnp.where(counts, p[0], 0.0)
    res = n[0] * (p[0] - q[0]) + n[1] * (p[1] - q[1]) + n[2] * (p[2] - q[2])
    w = jnp.where(counts, 1.0 / (1.0 + res * res), 0.0)
    jac = [
        p[1] * n[2] - p[2] * n[1],
        p[2] * n[0] - p[0] * n[2],
        p[0] * n[1] - p[1] * n[0],
        n[0],
        n[1],
        n[2],
    ]
    for i in range(6):
        big, small = parts_of(w * jac[i], 2)
        for r in range(8):
            for k, term in enumerate((big, big, small)):
                left_ref[r, i * 16 : (i + 1) * 16, k * LANES : (k + 1) * LANES] = term[r * 16 : (r + 1) * 16]
    for j, value in enumerate(jac + [res]):
        big, small = parts_of(value, 2)
        spots = [j] + {4: [9], 5: [8], 6: [15]}.get(j, [])
        for r in range(8):
            for k, term in enumerate((big, small, big)):
                for spot in spots:
                    right_ref[r, spot * 16 : (spot + 1) * 16, k * LANES : (k + 1) * LANES] = term[r * 16 : (r + 1) * 16]
    lane = iota((8, LANES), 1)
    sub = iota((8, LANES), 0)
    spot = lane // 16
    first = [spot < 8, (spot >= 1) & (spot <= 6), (spot >= 2) & (spot <= 6), spot < 8]
    other = [None, 5, 4, None]
    for chip in range(4):
        arrays = []
        for c in range(2):
            r = chip * 2 + c
            every = dot_t(left_ref[r], right_ref[r])
            for i in range(4):
                kept = jnp.zeros((8, LANES), F32)
                for h in range(2):
                    value = every[i * 16 + h * 8 : i * 16 + h * 8 + 8, :LANES]
                    if other[i] is not None:
                        o = other[i] * 16 + h * 8
                        value = jnp.where(first[i], value, every[o : o + 8, LANES:])
                    kept = jnp.where(lane % 16 == h * 8 + sub, value, kept)
                arrays.append(kept)
        for level in range(3):
            clear = (sub // (1 << level)) % 2 == 0
            arrays = [fold(arrays[n], arrays[n + 1], clear, 1 << level) for n in range(0, len(arrays), 2)]
        note = note_ref[pl.ds(group * 32 + chip * 8, 8), :]
        back_ref[chip * 4 + low(group - chip + 4, 2)] = jnp.where((sub % 4 == 3) & (spot < 3), note, arrays[0])


def turn(blocks, signs, turn_ref, at):
    lane = iota((8, LANES), 1)
    for bit in range(3):
        shift = 16 << bit
        clear = (lane // shift) % 2 == 0
        for m in range(8):
            if (m >> bit) % 2 == 0:
                a, b = blocks[m], blocks[m + (1 << bit)]
                blocks[m] = jnp.where(clear, a, pltpu.roll(b, shift, 1))
                blocks[m + (1 << bit)] = jnp.where(clear, pltpu.roll(a, LANES - shift, 1), b)
    for n in range(8):
        turn_ref[at, n] = jnp.where(lane < 64, blocks[n], -blocks[n]) if signs and n >= 6 else blocks[n]


def arrange(turn_ref, count, signs, owner_ref, sums_ref, column_ref):
    lane = iota((1, LANES), 1)
    y = (lane // 16) % 4
    half = count * LANES
    for t in range(count):
        source = turn_ref[t, 0]
        target = turn_ref[t, 1]
        for c in range(2):
            s = source[c * 4 + 3 : c * 4 + 4, :]
            b = target[c * 4 + 3 : c * 4 + 4, :]
            owner = jnp.broadcast_to(jnp.where(lane < 64, s, b) if signs else s, (LOC, LANES))
            at = c * half + t * LANES
            owner_ref[:, at : at + LANES] = onehot(owner == iota((LOC, LANES), 0).astype(F32))
            if column_ref is not None:
                column = jnp.where(lane < 64, b, s) + (16 * (2 * y + c)).astype(F32)
                there = jnp.broadcast_to(column, (LANES, LANES)) == iota((LANES, LANES), 0).astype(F32)
                there = jnp.where(there, -1.0, 0.0).astype(BF16)
                for n in range(2):
                    column_ref[:, n * 2 * half + at : n * 2 * half + at + LANES] = there
        for p in range(0, 8, 2):
            pair = jnp.concatenate([turn_ref[t, p], turn_ref[t, p + 1]], axis=0)
            for n, term in enumerate(parts_of(pair, 2)):
                sums_ref[p * 8 : p * 8 + 16, n * half + t * LANES : n * half + (t + 1) * LANES] = term


def scan_sums(count, owner_ref, sums_ref):
    half = count * LANES
    owners = [jnp.concatenate([owner_ref[:, c * half : (c + 1) * half]] * 2, axis=1) for c in range(2)]
    both = dot_t(jnp.concatenate(owners, axis=0), sums_ref[:, : 2 * half])
    lane = iota((LOC, 64), 1)
    part = jnp.where((lane // 4) % 2 == 0, both[:LOC], both[LOC:])
    return jnp.concatenate([part, jnp.zeros((LOC, LANES - 64), F32)], axis=1)


def matrix(owner_ref, sums_ref, column_ref, lhs_ref, block_ref):
    for k, pair in enumerate(PAIRS):
        i, p = SPOT[pair]
        for c in range(2):
            at = p * 8 + c * 4 + i
            mine = owner_ref[:, c * HALF : (c + 1) * HALF]
            for n in range(2):
                row = sums_ref[at : at + 1, n * HALF : (n + 1) * HALF]
                lhs_ref[k * LOC : (k + 1) * LOC, (2 * n + c) * HALF : (2 * n + c + 1) * HALF] = (
                    jnp.broadcast_to(row, (LOC, HALF)) * mine
                )
    block_ref[...] = dot_t(lhs_ref[...], column_ref[...])


def far(p):
    return 2 * (1 - low(p, 1)) + low(p + high(p, 1), 1)


def order(p):
    return 2 * high(p, 1) + low(p + high(p, 1), 1)


def step_kernel(
    pc_any, cs_any, ct_any, src_any, sm_any, block_ref, part_ref,
    pc_ref, cs_ref, ct_ref, src_ref, sm_ref, take_ref, pay_ref, code_ref, msg_ref, codes_ref, recv_ref, table_ref, tile_ref,
    note_ref, left_ref, right_ref, back_ref, mid_ref, out_ref, in_ref, last_ref, turn_ref, owner_ref, sums_ref, column_ref, lhs_ref,
    load_sem, send_n, send_p, recv_n, recv_p, send_a, recv_a, send_l, recv_l, send_b, recv_b, send_c, recv_c,
):
    row = lax.axis_index("scan")
    col = lax.axis_index("grp")
    z, y, core = high(row, 3), low(high(row, 1), 2), low(row, 1)
    me = row * NG + col
    chip = high(row, 1)
    group = low(y + z, 2)
    place = group * 32 + z * 8 + core * NG + col
    barrier = pltpu.get_barrier_semaphore()
    loads = [
        pltpu.make_async_copy(a, b, load_sem.at[n])
        for n, (a, b) in enumerate(
            [
                (cs_any, cs_ref),
                (ct_any, ct_ref),
                (src_any, src_ref),
                (pc_any, pc_ref),
                (sm_any.at[:, pl.ds(0, 3)], sm_ref.at[:, pl.ds(0, 3)]),
                (sm_any.at[:, pl.ds(3, 3)], sm_ref.at[:, pl.ds(3, 3)]),
            ]
        )
    ]
    for load in loads:
        load.start()

    def to_some(first, last, act):
        @pl.loop(first, last)
        def _(u):
            dz = low(u + 2, 2)
            uz = low(z + dz, 2)
            uy = low(y + order(high(u, 2)) - dz + 4, 2)
            for dx in (2, 1, 3, 0):
                for dc in (1, 0):
                    there = ((uz * 4 + uy) * 2 + low(core + dc, 1), low(col + dx, 2))
                    if dc == 0 and dx == 0:

                        @pl.when(u != 2)
                        def _():
                            act(*there)

                    else:
                        act(*there)

    @pl.loop(0, 16)
    def _(u):
        far_z = low(z + far(high(u, 2)), 2)
        far_y = low(y + far(low(u, 2)), 2)
        for dx in (2, 1, 3, 0):
            for dc in (1, 0):

                def greet():
                    there = ((far_z * 4 + far_y) * 2 + low(core + dc, 1), low(col + dx, 2))
                    pl.semaphore_signal(barrier, inc=1, device_id=there, device_id_type=MESH)

                if dc == 0 and dx == 0:
                    pl.when(u < 15)(greet)
                else:
                    greet()


    def send_codes(r, c):
        pltpu.make_async_remote_copy(
            src_ref=code_ref.at[pl.ds(r * NG + c, 1)],
            dst_ref=codes_ref.at[pl.ds(place, 1)],
            send_sem=send_n,
            recv_sem=recv_n,
            device_id=(r, c),
            device_id_type=MESH,
        ).start()

    def send_points(r, c):
        for x in range(3):
            pltpu.make_async_remote_copy(
                src_ref=msg_ref.at[x, pl.ds((r * NG + c) * CAP, CAP)],
                dst_ref=recv_ref.at[x, pl.ds(place * CAP, CAP)],
                send_sem=send_p,
                recv_sem=recv_p.at[group],
                device_id=(r, c),
                device_id_type=MESH,
            ).start()

    for n in range(5):
        loads[n].wait()
    route(cs_ref, ct_ref, take_ref, code_ref, col)
    pick_points(pc_ref, src_ref, sm_ref, pay_ref, col)
    pack(take_ref, pay_ref, msg_ref)
    pl.semaphore_wait(barrier, ND - 1)
    to_some(0, 4, send_points)
    to_some(0, 16, send_codes)
    to_some(4, 16, send_points)
    pltpu.make_async_copy(code_ref.at[pl.ds(me, 1)], codes_ref.at[pl.ds(place, 1)], recv_n).start()
    pltpu.make_async_copy(
        msg_ref.at[:, pl.ds(me * CAP, CAP)], recv_ref.at[:, pl.ds(place * CAP, CAP)], recv_p.at[group]
    ).start()

    loads[5].wait()
    tile_table(pc_ref, sm_ref, table_ref, col)
    for spot in (7, 10, 11, 12, 13, 14):
        right_ref[:, spot * 16 : (spot + 1) * 16, :] = jnp.zeros((8, 16, 3 * LANES), BF16)
    pltpu.make_async_copy(codes_ref, codes_ref, recv_n).wait()
    fetch_tiles(codes_ref, table_ref, tile_ref, note_ref)

    def cross_all(block_of, which, got, kind):
        for plane in range(PLANES):
            at = low(which - plane + 4, 2)
            src = block_of(plane, at)

            @pl.when(plane != col)
            def _():
                pltpu.make_async_remote_copy(
                    src_ref=src,
                    dst_ref=got.at[col * 4 + at],
                    send_sem=send_b.at[kind, plane],
                    recv_sem=recv_b.at[kind, col],
                    device_id=(row, plane),
                    device_id_type=MESH,
                ).start()

            @pl.when(plane == col)
            def _():
                pltpu.make_async_copy(src, got.at[plane * 4 + at], recv_b.at[kind, plane]).start()

    def serve(u):
        which = low(group - order(u) + 4, 2)
        arrived = recv_ref.at[:, pl.ds(which * LANES, LANES)]
        pltpu.make_async_copy(arrived, arrived, recv_p.at[which]).wait()
        group_sums(which, recv_ref, tile_ref, note_ref, left_ref, right_ref, back_ref)
        return which

    @pl.loop(0, PLANES - 1)
    def _(u):
        which = serve(u)
        for n in range(8):
            to_z = n // 2
            to_chip = to_z * 4 + low(which - to_z + 4, 2)
            to_row = to_chip * 2 + n % 2
            src = back_ref.at[to_chip, pl.ds(n % 2 * 4, 4)]
            dst = mid_ref.at[group * 4 + z, pl.ds(core * 4, 4)]

            @pl.when(to_row != row)
            def _():
                pltpu.make_async_remote_copy(
                    src_ref=src,
                    dst_ref=dst,
                    send_sem=send_a,
                    recv_sem=recv_a.at[group],
                    device_id=(to_row, col),
                    device_id_type=MESH,
                ).start()

            @pl.when(to_row == row)
            def _():
                pltpu.make_async_copy(src, dst, recv_a.at[group]).start()

        cross_all(lambda plane, at: back_ref.at[plane * 4 + at], which, in_ref, 0)

    which = serve(PLANES - 1)
    for n in range(8):
        to_z = n // 2
        to_chip = to_z * 4 + low(which - to_z + 4, 2)
        for step in (2, 1, 3, 0):
            pltpu.make_async_remote_copy(
                src_ref=back_ref.at[to_chip, pl.ds(n % 2 * 4, 4)],
                dst_ref=last_ref.at[col * 4 + z, pl.ds(core * 4, 4)],
                send_sem=send_l,
                recv_sem=recv_l,
                device_id=(to_chip * 2 + n % 2, low(col + step, 2)),
                device_id_type=MESH,
            ).start()
    cross_all(lambda plane, at: back_ref.at[plane * 4 + at], which, in_ref, 0)

    @pl.loop(0, PLANES - 1)
    def _(u):
        which = low(group + order(u), 2)
        arrived = mid_ref.at[pl.ds(which * 4, 4)]
        pltpu.make_async_copy(arrived, arrived, recv_a.at[which]).wait()
        cross_all(lambda plane, at: mid_ref.at[which * 4 + plane], which, out_ref, 1)

    def spread(to_col, at):
        return pltpu.make_async_remote_copy(
            src_ref=part_ref.at[col],
            dst_ref=part_ref.at[at],
            send_sem=send_c.at[to_col],
            recv_sem=recv_c.at[at],
            device_id=(row, to_col),
            device_id_type=MESH,
        )

    late = low(group + order(PLANES - 1), 2)
    for m in range(4):
        mid_ref[late * 4 + m] = jnp.zeros((8, LANES), F32)
    for t in range(PLANES):
        turn([ref[t * 4 + m] for ref in (mid_ref, back_ref) for m in range(4)], True, turn_ref, t)
    arrange(turn_ref, PLANES, True, owner_ref, sums_ref, None)
    part_ref[col] = scan_sums(PLANES, owner_ref, sums_ref)
    for step in (2, 1, 3):
        spread(low(col + step, 2), col).start()

    left = code_ref.at[pl.ds(0, ND - 1)]
    pltpu.make_async_copy(left, left, send_n).wait()
    left = msg_ref.at[:, pl.ds(0, (ND - 1) * CAP)]
    pltpu.make_async_copy(left, left, send_p).wait()
    for left in (back_ref.at[pl.ds(0, 11)], back_ref.at[11, pl.ds(0, 4)]):
        pltpu.make_async_copy(left, left, send_a).wait()
    pltpu.make_async_copy(last_ref, last_ref, send_l).wait()

    for source in range(NG):
        arrived = in_ref.at[pl.ds(source * 4, 4)]
        pltpu.make_async_copy(arrived, arrived, recv_b.at[0, source]).wait()
        arrived = out_ref.at[pl.ds(source * 4, 3)]
        pltpu.make_async_copy(arrived, arrived, recv_b.at[1, source]).wait()
    pltpu.make_async_copy(last_ref, last_ref, recv_l).wait()
    for t in range(PLANES):
        out_ref[t * 4 + low(late - col + 4, 2)] = last_ref[t * 4 + col]
    for t in range(2):
        turn([last_ref[t * 8 + m] for m in range(8)], False, turn_ref, t)
    arrange(turn_ref, 2, False, owner_ref, sums_ref, None)
    part_ref[NG] = scan_sums(2, owner_ref, sums_ref)
    for t in range(PLANES):
        turn([ref[t * 4 + m] for ref in (out_ref, in_ref) for m in range(4)], True, turn_ref, t)
    arrange(turn_ref, PLANES, True, owner_ref, sums_ref, column_ref)
    matrix(owner_ref, sums_ref, column_ref, lhs_ref, block_ref)
    for step in range(1, NG):
        other = low(col + step, 2)
        for kind in range(2):
            left = back_ref.at[pl.ds(0, 4 - kind)]
            pltpu.make_async_copy(left, left, send_b.at[kind, other]).wait()
        spread(other, col).wait_send()
        spread(other, other).wait_recv()


def finish_kernel(block_ref, part_ref, hess_ref, grad_ref):
    row = lax.axis_index("scan")
    col = lax.axis_index("grp")
    total = part_ref[0] + part_ref[1] + part_ref[2] + part_ref[3] + part_ref[4]
    total = total + pltpu.roll(total, LANES - 4, 1)
    lane = iota((LOC, LANES), 1)
    diag = (lane == iota((LOC, LANES), 0) + LOC * (row % 8)) & (row // 8 == col)
    for k, (i, j) in enumerate(PAIRS):
        at = SPOT[i, j][1] * 8 + SPOT[i, j][0]
        value = block_ref[k * LOC : (k + 1) * LOC, :] + jnp.where(
            diag, jnp.broadcast_to(total[:, at : at + 1], (LOC, LANES)), 0.0
        )
        hess_ref[i, j] = value
        if i != j:
            hess_ref[j, i] = value
    some = jnp.zeros((4, LANES), F32)
    for n in range(NG):
        some = jnp.where(col == n, total[n * 4 : (n + 1) * 4, :], some)
    at = [SPOT[i, 6][1] * 8 + SPOT[i, 6][0] for i in range(6)]
    grad_ref[...] = jnp.concatenate([some[:, a : a + 1] for a in at], axis=1)


def vmem(count):
    return [pl.BlockSpec(memory_space=pltpu.VMEM)] * count


def local(samples, point_count, corr_scan, corr_tile, corr_src):
    dma = pltpu.SemaphoreType.DMA
    block, parts = pl.pallas_call(
        step_kernel,
        out_shape=(
            pltpu.VMEM((len(PAIRS) * LOC, LANES), F32),
            pltpu.VMEM((NG + 1, LOC, LANES), F32),
        ),
        in_specs=[pl.BlockSpec(memory_space=pl.ANY)] * 5,
        out_specs=tuple(vmem(2)),
        scratch_shapes=[
            pltpu.SMEM((LOC,), I32),
            pltpu.VMEM((LOC, CT), I32),
            pltpu.VMEM((LOC, CT), I32),
            pltpu.VMEM((LOC, CT, LANES), I32),
            pltpu.VMEM((LOC, 6, TL, LANES), F32),
            pltpu.VMEM((SLOTS, 3 * REQ), BF16),
            pltpu.VMEM((3 * REQ, 3 * LANES), BF16),
            pltpu.VMEM((ND, LANES), F32),
            pltpu.VMEM((3, SLOTS, LANES), F32),
            pltpu.VMEM((ND, LANES), F32),
            pltpu.VMEM((3, SLOTS, LANES), F32),
            pltpu.VMEM((3 * LOC * TL, 6 * LANES), BF16),
            pltpu.VMEM((SLOTS, 6 * LANES), F32),
            pltpu.VMEM((ND, LANES), F32),
            pltpu.VMEM((8, 6 * 16, 3 * LANES), BF16),
            pltpu.VMEM((8, 16 * 16, 3 * LANES), BF16),
            pltpu.VMEM((16, 8, LANES), F32),
            pltpu.VMEM((16, 8, LANES), F32),
            pltpu.VMEM((16, 8, LANES), F32),
            pltpu.VMEM((16, 8, LANES), F32),
            pltpu.VMEM((16, 8, LANES), F32),
            pltpu.VMEM((PLANES, 8, 8, LANES), F32),
            pltpu.VMEM((LOC, 2 * HALF), BF16),
            pltpu.VMEM((64, 2 * HALF), BF16),
            pltpu.VMEM((LANES, 4 * HALF), BF16),
            pltpu.VMEM((len(PAIRS) * LOC, 4 * HALF), BF16),
            dma((6,)),
            dma,
            dma,
            dma,
            dma((PLANES,)),
            dma,
            dma((PLANES,)),
            dma,
            dma,
            dma((2, NG)),
            dma((2, NG)),
            dma((NG,)),
            dma((NG,)),
        ],
        compiler_params=pltpu.CompilerParams(collective_id=0, has_side_effects=True),
        name="step",
    )(point_count, corr_scan, corr_tile, corr_src, samples.transpose(0, 2, 1, 3))
    hessian, gradient = pl.pallas_call(
        finish_kernel,
        out_shape=(
            jax.ShapeDtypeStruct((6, 6, LOC, LANES), F32),
            jax.ShapeDtypeStruct((4, 6), F32),
        ),
        in_specs=vmem(2),
        out_specs=tuple(vmem(2)),
        compiler_params=pltpu.CompilerParams(vmem_limit_bytes=8 * 1024 * 1024),
        name="finish",
    )(block, parts)
    return hessian.transpose(2, 0, 1, 3), gradient


def solution(mesh):
    placed = (
        P("scan", "grp", None, None),
        P("scan"),
        P("scan", "grp"),
        P("scan", "grp"),
        P("scan", "grp", None),
    )
    return jax.shard_map(
        local,
        mesh=mesh,
        in_specs=placed,
        out_specs=(P("scan", None, None, "grp"), P(("scan", "grp"), None)),
        check_vma=False,
    )
```

```python
import functools

import jax
import jax.numpy as jnp
from jax import lax
from jax.experimental import pallas as pl
from jax.experimental.pallas import tpu as pltpu
from jax.sharding import PartitionSpec as P

F32 = jnp.float32
BF16 = jnp.bfloat16
I32 = jnp.int32
MESH = pl.DeviceIdType.MESH

NS = 32
NG = 4
ND = NS * NG
LOC = 16
TL = 16
CT = 16
REQ = LOC * CT
CAP = 4
FAR = 1000.0
LANES = 128
PAIRS = [(i, j) for i in range(6) for j in range(i, 6)]
PLANES = 4
SLOTS = ND * CAP
HALF = PLANES * LANES
SPOT = {(i, j): (i, j) for i in range(4) for j in range(i, 7)}
SPOT |= {(5, 5): (1, 0), (5, 6): (1, 7), (4, 4): (2, 1), (4, 5): (2, 0), (4, 6): (2, 7)}


def iota(shape, dim):
    return lax.broadcasted_iota(I32, shape, dim)


def dot(a, b):
    return lax.dot_general(a, b, (((1,), (0,)), ((), ())), preferred_element_type=F32)


def dot_t(a, b):
    return lax.dot_general(a, b, (((1,), (1,)), ((), ())), preferred_element_type=F32)


def parts_of(x, count):
    terms = []
    for _ in range(count):
        term = x.astype(BF16)
        terms.append(term)
        x = x - term.astype(F32)
    return terms


def onehot(cond):
    return jnp.where(cond, 1.0, 0.0).astype(BF16)


def low(x, bits):
    return lax.bitwise_and(x, (1 << bits) - 1)


def high(x, bits):
    return lax.shift_right_logical(x, bits)


def pick_points(pc_ref, src_ref, sm_ref, pay_ref, group):
    first = group * (TL * LANES)
    for s in range(LOC):
        picks = src_ref[s]
        halves = []
        for h in range(2):
            part = picks[h * 8 : h * 8 + 8]
            tile = high(part, 7)
            lane = low(part, 7)
            acc = [jnp.zeros((8, LANES), F32) for _ in range(3)]
            for t in range(TL):
                here = tile == t
                for x in range(3):
                    row = jnp.broadcast_to(sm_ref[s, x, t : t + 1, :], (8, LANES))
                    got = jnp.take_along_axis(row, lane, axis=1, mode="promise_in_bounds")
                    acc[x] = jnp.where(here, got, acc[x])
            acc[0] = jnp.where(first + part < pc_ref[s], acc[0], FAR)
            halves.append(acc)
        for x in range(3):
            both = jnp.concatenate([halves[0][x], halves[1][x]], axis=0)
            for n, term in enumerate(parts_of(both, 3)):
                pay_ref[n * REQ + s * CT : n * REQ + (s + 1) * CT, x * LANES : (x + 1) * LANES] = term


def route(cs_ref, ct_ref, take_ref, code_ref, group):
    cs = cs_ref[...]
    ct = ct_ref[...]
    dest = (high(cs, 4) * NG + high(ct, 4)).astype(F32)
    code = (low(cs, 4) * TL + low(ct, 4) + 1).astype(F32)
    wide = dot(dest.astype(BF16), onehot(iota((CT, REQ), 1) % CT == iota((CT, REQ), 0)))
    wide = jnp.where(iota((LOC, REQ), 1) // CT == iota((LOC, REQ), 0), wide, 0.0)
    dest_t = dot(jnp.ones((ND, LOC), BF16), wide.astype(BF16))
    to_me = dest_t == iota((ND, REQ), 0).astype(F32)
    rank = dot(onehot(to_me), onehot(iota((REQ, REQ), 0) < iota((REQ, REQ), 1)))
    takes = [onehot(to_me & (rank == float(r))) for r in range(CAP)]
    for r in range(CAP):
        for n in range(3):
            take_ref[r * ND : (r + 1) * ND, n * REQ : (n + 1) * REQ] = takes[r]
    tall = dot(onehot(iota((REQ, LOC), 0) // CT == iota((REQ, LOC), 1)), code.astype(BF16))
    tall = jnp.where(iota((REQ, CT), 0) % CT == iota((REQ, CT), 1), tall, 0.0)
    code_b = dot(tall.astype(BF16), jnp.ones((CT, LANES), BF16))
    target = high(code_b.astype(I32) - 1, 4).astype(F32)
    source = (iota((REQ, LANES), 0) // CT).astype(F32)
    lane = iota((REQ, LANES), 1)
    codes = jnp.where(lane < 16, source, jnp.where(lane < 32, target, code_b)).astype(BF16)
    lane = iota((ND, LANES), 1)
    row = jnp.zeros((ND, LANES), F32)
    for r in range(CAP):
        at = group * CAP + r
        here = (lane == at) | (lane == 16 + at) | (lane == 32 + r)
        row = jnp.where(here, dot(takes[r], codes), row)
    code_ref[...] = row


def pack(take_ref, pay_ref, msg_ref):
    got = dot(take_ref[...], pay_ref[...])
    for r in range(CAP):
        for x in range(3):
            msg_ref[x, pl.ds(r, ND, stride=CAP), :] = got[r * ND : (r + 1) * ND, x * LANES : (x + 1) * LANES]


def tile_table(pc_ref, sm_ref, table_ref, group):
    point = (group * TL + iota((TL, LANES), 0)) * LANES + iota((TL, LANES), 1)

    @pl.loop(0, LOC)
    def _(s):
        valid = point < pc_ref[s]
        at = pl.multiple_of(s * TL, TL)
        for x in range(6):
            value = sm_ref[s, x]
            if x >= 3:
                value = jnp.where(valid, value, 0.0)
            for n, term in enumerate(parts_of(value, 3)):
                table_ref[pl.ds(n * LOC * TL + at, TL), x * LANES : (x + 1) * LANES] = term


def fetch_tiles(code_ref, table_ref, tile_ref, note_ref):
    codes = code_ref[...].astype(BF16)
    spread = dot(onehot(iota((SLOTS, ND), 0) // CAP == iota((SLOTS, ND), 1)), codes)
    spread = jnp.where(iota((SLOTS, LANES), 1) == 32 + iota((SLOTS, LANES), 0) % CAP, spread, 0.0)
    wanted = dot(spread.astype(BF16), jnp.ones((LANES, LOC * TL), BF16))
    take = onehot(wanted == (iota((SLOTS, LOC * TL), 1) + 1).astype(F32))
    tile_ref[...] = dot(jnp.concatenate([take] * 3, axis=1), table_ref[...])
    here = iota((ND, ND), 0)
    note_ref[...] = dot(onehot((here // 4 == iota((ND, ND), 1) // 4) & (here % 4 == 3)), codes)


def fold(a, b, clear, shift):
    return jnp.where(clear, a, b) + pltpu.roll(jnp.where(clear, b, a), shift, 0)


def group_sums(group, recv_ref, tile_ref, note_ref, left_ref, right_ref, back_ref):
    at = pl.multiple_of(group * LANES, LANES)
    p = [recv_ref[x, pl.ds(at, LANES), :] for x in range(3)]
    tile = [tile_ref[pl.ds(at, LANES), x * LANES : (x + 1) * LANES] for x in range(6)]
    q, n = tile[:3], tile[3:]
    counts = p[0] < 0.5 * FAR
    p[0] = jnp.where(counts, p[0], 0.0)
    res = n[0] * (p[0] - q[0]) + n[1] * (p[1] - q[1]) + n[2] * (p[2] - q[2])
    w = jnp.where(counts, 1.0 / (1.0 + res * res), 0.0)
    jac = [
        p[1] * n[2] - p[2] * n[1],
        p[2] * n[0] - p[0] * n[2],
        p[0] * n[1] - p[1] * n[0],
        n[0],
        n[1],
        n[2],
    ]
    for i in range(6):
        big, small = parts_of(w * jac[i], 2)
        for r in range(8):
            for k, term in enumerate((big, big, small)):
                left_ref[r, i * 16 : (i + 1) * 16, k * LANES : (k + 1) * LANES] = term[r * 16 : (r + 1) * 16]
    for j, value in enumerate(jac + [res]):
        big, small = parts_of(value, 2)
        spots = [j] + {4: [9], 5: [8], 6: [15]}.get(j, [])
        for r in range(8):
            for k, term in enumerate((big, small, big)):
                for spot in spots:
                    right_ref[r, spot * 16 : (spot + 1) * 16, k * LANES : (k + 1) * LANES] = term[r * 16 : (r + 1) * 16]
    lane = iota((8, LANES), 1)
    sub = iota((8, LANES), 0)
    spot = lane // 16
    first = [spot < 8, (spot >= 1) & (spot <= 6), (spot >= 2) & (spot <= 6), spot < 8]
    other = [None, 5, 4, None]
    for chip in range(4):
        arrays = []
        for c in range(2):
            r = chip * 2 + c
            every = dot_t(left_ref[r], right_ref[r])
            for i in range(4):
                kept = jnp.zeros((8, LANES), F32)
                for h in range(2):
                    value = every[i * 16 + h * 8 : i * 16 + h * 8 + 8, :LANES]
                    if other[i] is not None:
                        o = other[i] * 16 + h * 8
                        value = jnp.where(first[i], value, every[o : o + 8, LANES:])
                    kept = jnp.where(lane % 16 == h * 8 + sub, value, kept)
                arrays.append(kept)
        for level in range(3):
            clear = (sub // (1 << level)) % 2 == 0
            arrays = [fold(arrays[n], arrays[n + 1], clear, 1 << level) for n in range(0, len(arrays), 2)]
        note = note_ref[pl.ds(group * 32 + chip * 8, 8), :]
        back_ref[chip * 4 + low(group - chip + 4, 2)] = jnp.where((sub % 4 == 3) & (spot < 3), note, arrays[0])


def turn(blocks, signs, turn_ref, at):
    lane = iota((8, LANES), 1)
    for bit in range(3):
        shift = 16 << bit
        clear = (lane // shift) % 2 == 0
        for m in range(8):
            if (m >> bit) % 2 == 0:
                a, b = blocks[m], blocks[m + (1 << bit)]
                blocks[m] = jnp.where(clear, a, pltpu.roll(b, shift, 1))
                blocks[m + (1 << bit)] = jnp.where(clear, pltpu.roll(a, LANES - shift, 1), b)
    for n in range(8):
        turn_ref[at, n] = jnp.where(lane < 64, blocks[n], -blocks[n]) if signs and n >= 6 else blocks[n]


def arrange(turn_ref, count, signs, owner_ref, sums_ref, column_ref):
    lane = iota((1, LANES), 1)
    y = (lane // 16) % 4
    half = count * LANES
    for t in range(count):
        source = turn_ref[t, 0]
        target = turn_ref[t, 1]
        for c in range(2):
            s = source[c * 4 + 3 : c * 4 + 4, :]
            b = target[c * 4 + 3 : c * 4 + 4, :]
            owner = jnp.broadcast_to(jnp.where(lane < 64, s, b) if signs else s, (LOC, LANES))
            at = c * half + t * LANES
            owner_ref[:, at : at + LANES] = onehot(owner == iota((LOC, LANES), 0).astype(F32))
            if column_ref is not None:
                column = jnp.where(lane < 64, b, s) + (16 * (2 * y + c)).astype(F32)
                there = jnp.broadcast_to(column, (LANES, LANES)) == iota((LANES, LANES), 0).astype(F32)
                there = jnp.where(there, -1.0, 0.0).astype(BF16)
                for n in range(2):
                    column_ref[:, n * 2 * half + at : n * 2 * half + at + LANES] = there
        for p in range(0, 8, 2):
            pair = jnp.concatenate([turn_ref[t, p], turn_ref[t, p + 1]], axis=0)
            for n, term in enumerate(parts_of(pair, 2)):
                sums_ref[p * 8 : p * 8 + 16, n * half + t * LANES : n * half + (t + 1) * LANES] = term


def scan_sums(count, owner_ref, sums_ref):
    half = count * LANES
    owners = [jnp.concatenate([owner_ref[:, c * half : (c + 1) * half]] * 2, axis=1) for c in range(2)]
    both = dot_t(jnp.concatenate(owners, axis=0), sums_ref[:, : 2 * half])
    lane = iota((LOC, 64), 1)
    part = jnp.where((lane // 4) % 2 == 0, both[:LOC], both[LOC:])
    return jnp.concatenate([part, jnp.zeros((LOC, LANES - 64), F32)], axis=1)


def matrix(owner_ref, sums_ref, column_ref, lhs_ref, block_ref):
    for k, pair in enumerate(PAIRS):
        i, p = SPOT[pair]
        for c in range(2):
            at = p * 8 + c * 4 + i
            mine = owner_ref[:, c * HALF : (c + 1) * HALF]
            for n in range(2):
                row = sums_ref[at : at + 1, n * HALF : (n + 1) * HALF]
                lhs_ref[k * LOC : (k + 1) * LOC, (2 * n + c) * HALF : (2 * n + c + 1) * HALF] = (
                    jnp.broadcast_to(row, (LOC, HALF)) * mine
                )
    block_ref[...] = dot_t(lhs_ref[...], column_ref[...])


def far(p):
    return 2 * (1 - low(p, 1)) + low(p + high(p, 1), 1)


def order(p):
    return 2 * high(p, 1) + low(p + high(p, 1), 1)


def step_kernel(
    pc_any, cs_any, ct_any, src_any, sm_any, block_ref, part_ref,
    pc_ref, cs_ref, ct_ref, src_ref, sm_ref, take_ref, pay_ref, code_ref, msg_ref, codes_ref, recv_ref, table_ref, tile_ref,
    note_ref, left_ref, right_ref, back_ref, mid_ref, out_ref, in_ref, last_ref, turn_ref, owner_ref, sums_ref, column_ref, lhs_ref,
    load_sem, send_n, send_p, recv_n, recv_p, send_a, recv_a, send_l, recv_l, send_b, recv_b, send_c, recv_c,
):
    row = lax.axis_index("scan")
    col = lax.axis_index("grp")
    z, y, core = high(row, 3), low(high(row, 1), 2), low(row, 1)
    me = row * NG + col
    chip = high(row, 1)
    group = low(y + z, 2)
    place = group * 32 + z * 8 + core * NG + col
    barrier = pltpu.get_barrier_semaphore()
    loads = [
        pltpu.make_async_copy(a, b, load_sem.at[n])
        for n, (a, b) in enumerate(
            [
                (cs_any, cs_ref),
                (ct_any, ct_ref),
                (src_any, src_ref),
                (pc_any, pc_ref),
                (sm_any.at[:, pl.ds(0, 3)], sm_ref.at[:, pl.ds(0, 3)]),
                (sm_any.at[:, pl.ds(3, 3)], sm_ref.at[:, pl.ds(3, 3)]),
            ]
        )
    ]
    for load in loads:
        load.start()

    def to_some(first, last, act):
        @pl.loop(first, last)
        def _(u):
            dz = low(u + 2 + 2 * core + col, 2)
            uz = low(z + dz, 2)
            uy = low(y + order(high(u, 2)) - dz + 4, 2)
            for dx in (2, 1, 3, 0):
                for dc in (1, 0):
                    there = ((uz * 4 + uy) * 2 + low(core + dc, 1), low(col + dx, 2))
                    if dc == 0 and dx == 0:

                        @pl.when(jnp.logical_or(u >= 4, dz != 0))
                        def _():
                            act(*there)

                    else:
                        act(*there)

    @pl.loop(0, 16)
    def _(u):
        far_z = low(z + far(high(u, 2)), 2)
        far_y = low(y + far(low(u, 2)), 2)
        for dx in (2, 1, 3, 0):
            for dc in (1, 0):

                def greet():
                    there = ((far_z * 4 + far_y) * 2 + low(core + dc, 1), low(col + dx, 2))
                    pl.semaphore_signal(barrier, inc=1, device_id=there, device_id_type=MESH)

                if dc == 0 and dx == 0:
                    pl.when(u < 15)(greet)
                else:
                    greet()


    def send_codes(r, c):
        pltpu.make_async_remote_copy(
            src_ref=code_ref.at[pl.ds(r * NG + c, 1)],
            dst_ref=codes_ref.at[pl.ds(place, 1)],
            send_sem=send_n,
            recv_sem=recv_n,
            device_id=(r, c),
            device_id_type=MESH,
        ).start()

    def send_points(r, c):
        for x in range(3):
            pltpu.make_async_remote_copy(
                src_ref=msg_ref.at[x, pl.ds((r * NG + c) * CAP, CAP)],
                dst_ref=recv_ref.at[x, pl.ds(place * CAP, CAP)],
                send_sem=send_p,
                recv_sem=recv_p.at[group],
                device_id=(r, c),
                device_id_type=MESH,
            ).start()

    for n in range(5):
        loads[n].wait()
    route(cs_ref, ct_ref, take_ref, code_ref, col)
    pick_points(pc_ref, src_ref, sm_ref, pay_ref, col)
    pack(take_ref, pay_ref, msg_ref)
    pl.semaphore_wait(barrier, ND - 1)
    to_some(0, 4, send_points)
    to_some(0, 16, send_codes)
    to_some(4, 16, send_points)
    pltpu.make_async_copy(code_ref.at[pl.ds(me, 1)], codes_ref.at[pl.ds(place, 1)], recv_n).start()
    pltpu.make_async_copy(
        msg_ref.at[:, pl.ds(me * CAP, CAP)], recv_ref.at[:, pl.ds(place * CAP, CAP)], recv_p.at[group]
    ).start()

    loads[5].wait()
    tile_table(pc_ref, sm_ref, table_ref, col)
    for spot in (7, 10, 11, 12, 13, 14):
        right_ref[:, spot * 16 : (spot + 1) * 16, :] = jnp.zeros((8, 16, 3 * LANES), BF16)
    pltpu.make_async_copy(codes_ref, codes_ref, recv_n).wait()
    fetch_tiles(codes_ref, table_ref, tile_ref, note_ref)

    def cross_all(block_of, which, got, kind):
        for plane in range(PLANES):
            at = low(which - plane + 4, 2)
            src = block_of(plane, at)

            @pl.when(plane != col)
            def _():
                pltpu.make_async_remote_copy(
                    src_ref=src,
                    dst_ref=got.at[col * 4 + at],
                    send_sem=send_b.at[kind, plane],
                    recv_sem=recv_b.at[kind, col],
                    device_id=(row, plane),
                    device_id_type=MESH,
                ).start()

            @pl.when(plane == col)
            def _():
                pltpu.make_async_copy(src, got.at[plane * 4 + at], recv_b.at[kind, plane]).start()

    def serve(u):
        which = low(group - order(u) + 4, 2)
        arrived = recv_ref.at[:, pl.ds(which * LANES, LANES)]
        pltpu.make_async_copy(arrived, arrived, recv_p.at[which]).wait()
        group_sums(which, recv_ref, tile_ref, note_ref, left_ref, right_ref, back_ref)
        return which

    @pl.loop(0, PLANES - 1)
    def _(u):
        which = serve(u)
        for n in range(8):
            to_z = n // 2
            to_chip = to_z * 4 + low(which - to_z + 4, 2)
            to_row = to_chip * 2 + n % 2
            src = back_ref.at[to_chip, pl.ds(n % 2 * 4, 4)]
            dst = mid_ref.at[group * 4 + z, pl.ds(core * 4, 4)]

            @pl.when(to_row != row)
            def _():
                pltpu.make_async_remote_copy(
                    src_ref=src,
                    dst_ref=dst,
                    send_sem=send_a,
                    recv_sem=recv_a.at[group],
                    device_id=(to_row, col),
                    device_id_type=MESH,
                ).start()

            @pl.when(to_row == row)
            def _():
                pltpu.make_async_copy(src, dst, recv_a.at[group]).start()

        cross_all(lambda plane, at: back_ref.at[plane * 4 + at], which, in_ref, 0)

    which = serve(PLANES - 1)
    for n in range(8):
        to_z = n // 2
        to_chip = to_z * 4 + low(which - to_z + 4, 2)
        for step in (2, 1, 3, 0):
            pltpu.make_async_remote_copy(
                src_ref=back_ref.at[to_chip, pl.ds(n % 2 * 4, 4)],
                dst_ref=last_ref.at[col * 4 + z, pl.ds(core * 4, 4)],
                send_sem=send_l,
                recv_sem=recv_l,
                device_id=(to_chip * 2 + n % 2, low(col + step, 2)),
                device_id_type=MESH,
            ).start()
    cross_all(lambda plane, at: back_ref.at[plane * 4 + at], which, in_ref, 0)

    @pl.loop(0, PLANES - 1)
    def _(u):
        which = low(group + order(u), 2)
        arrived = mid_ref.at[pl.ds(which * 4, 4)]
        pltpu.make_async_copy(arrived, arrived, recv_a.at[which]).wait()
        cross_all(lambda plane, at: mid_ref.at[which * 4 + plane], which, out_ref, 1)

    def spread(to_col, at):
        return pltpu.make_async_remote_copy(
            src_ref=part_ref.at[col],
            dst_ref=part_ref.at[at],
            send_sem=send_c.at[to_col],
            recv_sem=recv_c.at[at],
            device_id=(row, to_col),
            device_id_type=MESH,
        )

    late = low(group + order(PLANES - 1), 2)
    for m in range(4):
        mid_ref[late * 4 + m] = jnp.zeros((8, LANES), F32)
    for t in range(PLANES):
        turn([ref[t * 4 + m] for ref in (mid_ref, back_ref) for m in range(4)], True, turn_ref, t)
    arrange(turn_ref, PLANES, True, owner_ref, sums_ref, None)
    part_ref[col] = scan_sums(PLANES, owner_ref, sums_ref)
    for step in (2, 1, 3):
        spread(low(col + step, 2), col).start()

    left = code_ref.at[pl.ds(0, ND - 1)]
    pltpu.make_async_copy(left, left, send_n).wait()
    left = msg_ref.at[:, pl.ds(0, (ND - 1) * CAP)]
    pltpu.make_async_copy(left, left, send_p).wait()
    for left in (back_ref.at[pl.ds(0, 11)], back_ref.at[11, pl.ds(0, 4)]):
        pltpu.make_async_copy(left, left, send_a).wait()
    pltpu.make_async_copy(last_ref, last_ref, send_l).wait()

    for source in range(NG):
        arrived = in_ref.at[pl.ds(source * 4, 4)]
        pltpu.make_async_copy(arrived, arrived, recv_b.at[0, source]).wait()
        arrived = out_ref.at[pl.ds(source * 4, 3)]
        pltpu.make_async_copy(arrived, arrived, recv_b.at[1, source]).wait()
    pltpu.make_async_copy(last_ref, last_ref, recv_l).wait()
    for t in range(PLANES):
        out_ref[t * 4 + low(late - col + 4, 2)] = last_ref[t * 4 + col]
    for t in range(2):
        turn([last_ref[t * 8 + m] for m in range(8)], False, turn_ref, t)
    arrange(turn_ref, 2, False, owner_ref, sums_ref, None)
    part_ref[NG] = scan_sums(2, owner_ref, sums_ref)
    for t in range(PLANES):
        turn([ref[t * 4 + m] for ref in (out_ref, in_ref) for m in range(4)], True, turn_ref, t)
    arrange(turn_ref, PLANES, True, owner_ref, sums_ref, column_ref)
    matrix(owner_ref, sums_ref, column_ref, lhs_ref, block_ref)
    for step in range(1, NG):
        other = low(col + step, 2)
        for kind in range(2):
            left = back_ref.at[pl.ds(0, 4 - kind)]
            pltpu.make_async_copy(left, left, send_b.at[kind, other]).wait()
        spread(other, col).wait_send()
        spread(other, other).wait_recv()


def finish_kernel(block_ref, part_ref, hess_ref, grad_ref):
    row = lax.axis_index("scan")
    col = lax.axis_index("grp")
    total = part_ref[0] + part_ref[1] + part_ref[2] + part_ref[3] + part_ref[4]
    total = total + pltpu.roll(total, LANES - 4, 1)
    lane = iota((LOC, LANES), 1)
    diag = (lane == iota((LOC, LANES), 0) + LOC * (row % 8)) & (row // 8 == col)
    for k, (i, j) in enumerate(PAIRS):
        at = SPOT[i, j][1] * 8 + SPOT[i, j][0]
        value = block_ref[k * LOC : (k + 1) * LOC, :] + jnp.where(
            diag, jnp.broadcast_to(total[:, at : at + 1], (LOC, LANES)), 0.0
        )
        hess_ref[i, j] = value
        if i != j:
            hess_ref[j, i] = value
    some = jnp.zeros((4, LANES), F32)
    for n in range(NG):
        some = jnp.where(col == n, total[n * 4 : (n + 1) * 4, :], some)
    at = [SPOT[i, 6][1] * 8 + SPOT[i, 6][0] for i in range(6)]
    grad_ref[...] = jnp.concatenate([some[:, a : a + 1] for a in at], axis=1)


def vmem(count):
    return [pl.BlockSpec(memory_space=pltpu.VMEM)] * count


def local(samples, point_count, corr_scan, corr_tile, corr_src):
    dma = pltpu.SemaphoreType.DMA
    block, parts = pl.pallas_call(
        step_kernel,
        out_shape=(
            pltpu.VMEM((len(PAIRS) * LOC, LANES), F32),
            pltpu.VMEM((NG + 1, LOC, LANES), F32),
        ),
        in_specs=[pl.BlockSpec(memory_space=pl.ANY)] * 5,
        out_specs=tuple(vmem(2)),
        scratch_shapes=[
            pltpu.SMEM((LOC,), I32),
            pltpu.VMEM((LOC, CT), I32),
            pltpu.VMEM((LOC, CT), I32),
            pltpu.VMEM((LOC, CT, LANES), I32),
            pltpu.VMEM((LOC, 6, TL, LANES), F32),
            pltpu.VMEM((SLOTS, 3 * REQ), BF16),
            pltpu.VMEM((3 * REQ, 3 * LANES), BF16),
            pltpu.VMEM((ND, LANES), F32),
            pltpu.VMEM((3, SLOTS, LANES), F32),
            pltpu.VMEM((ND, LANES), F32),
            pltpu.VMEM((3, SLOTS, LANES), F32),
            pltpu.VMEM((3 * LOC * TL, 6 * LANES), BF16),
            pltpu.VMEM((SLOTS, 6 * LANES), F32),
            pltpu.VMEM((ND, LANES), F32),
            pltpu.VMEM((8, 6 * 16, 3 * LANES), BF16),
            pltpu.VMEM((8, 16 * 16, 3 * LANES), BF16),
            pltpu.VMEM((16, 8, LANES), F32),
            pltpu.VMEM((16, 8, LANES), F32),
            pltpu.VMEM((16, 8, LANES), F32),
            pltpu.VMEM((16, 8, LANES), F32),
            pltpu.VMEM((16, 8, LANES), F32),
            pltpu.VMEM((PLANES, 8, 8, LANES), F32),
            pltpu.VMEM((LOC, 2 * HALF), BF16),
            pltpu.VMEM((64, 2 * HALF), BF16),
            pltpu.VMEM((LANES, 4 * HALF), BF16),
            pltpu.VMEM((len(PAIRS) * LOC, 4 * HALF), BF16),
            dma((6,)),
            dma,
            dma,
            dma,
            dma((PLANES,)),
            dma,
            dma((PLANES,)),
            dma,
            dma,
            dma((2, NG)),
            dma((2, NG)),
            dma((NG,)),
            dma((NG,)),
        ],
        compiler_params=pltpu.CompilerParams(collective_id=0, has_side_effects=True),
        name="step",
    )(point_count, corr_scan, corr_tile, corr_src, samples.transpose(0, 2, 1, 3))
    hessian, gradient = pl.pallas_call(
        finish_kernel,
        out_shape=(
            jax.ShapeDtypeStruct((6, 6, LOC, LANES), F32),
            jax.ShapeDtypeStruct((4, 6), F32),
        ),
        in_specs=vmem(2),
        out_specs=tuple(vmem(2)),
        compiler_params=pltpu.CompilerParams(vmem_limit_bytes=8 * 1024 * 1024),
        name="finish",
    )(block, parts)
    return hessian.transpose(2, 0, 1, 3), gradient


def solution(mesh):
    placed = (
        P("scan", "grp", None, None),
        P("scan"),
        P("scan", "grp"),
        P("scan", "grp"),
        P("scan", "grp", None),
    )
    return jax.shard_map(
        local,
        mesh=mesh,
        in_specs=placed,
        out_specs=(P("scan", None, None, "grp"), P(("scan", "grp"), None)),
        check_vma=False,
    )
```

```python
import functools

import jax
import jax.numpy as jnp
from jax import lax
from jax.experimental import pallas as pl
from jax.experimental.pallas import tpu as pltpu
from jax.sharding import PartitionSpec as P

F32 = jnp.float32
BF16 = jnp.bfloat16
I32 = jnp.int32
MESH = pl.DeviceIdType.MESH

NS = 32
NG = 4
ND = NS * NG
LOC = 16
TL = 16
CT = 16
REQ = LOC * CT
CAP = 4
FAR = 1000.0
LANES = 128
PAIRS = [(i, j) for i in range(6) for j in range(i, 6)]
PLANES = 4
SLOTS = ND * CAP
HALF = PLANES * LANES
SPOT = {(i, j): (i, j) for i in range(4) for j in range(i, 7)}
SPOT |= {(5, 5): (1, 0), (5, 6): (1, 7), (4, 4): (2, 1), (4, 5): (2, 0), (4, 6): (2, 7)}


def iota(shape, dim):
    return lax.broadcasted_iota(I32, shape, dim)


def dot(a, b):
    return lax.dot_general(a, b, (((1,), (0,)), ((), ())), preferred_element_type=F32)


def dot_t(a, b):
    return lax.dot_general(a, b, (((1,), (1,)), ((), ())), preferred_element_type=F32)


def parts_of(x, count):
    terms = []
    for _ in range(count):
        term = x.astype(BF16)
        terms.append(term)
        x = x - term.astype(F32)
    return terms


def onehot(cond):
    return jnp.where(cond, 1.0, 0.0).astype(BF16)


def low(x, bits):
    return lax.bitwise_and(x, (1 << bits) - 1)


def high(x, bits):
    return lax.shift_right_logical(x, bits)


def pick_points(pc_ref, src_ref, sm_ref, pay_ref, group):
    first = group * (TL * LANES)
    for s in range(LOC):
        picks = src_ref[s]
        halves = []
        for h in range(2):
            part = picks[h * 8 : h * 8 + 8]
            tile = high(part, 7)
            lane = low(part, 7)
            acc = [jnp.zeros((8, LANES), F32) for _ in range(3)]
            for t in range(TL):
                here = tile == t
                for x in range(3):
                    row = jnp.broadcast_to(sm_ref[s, x, t : t + 1, :], (8, LANES))
                    got = jnp.take_along_axis(row, lane, axis=1, mode="promise_in_bounds")
                    acc[x] = jnp.where(here, got, acc[x])
            acc[0] = jnp.where(first + part < pc_ref[s], acc[0], FAR)
            halves.append(acc)
        for x in range(3):
            both = jnp.concatenate([halves[0][x], halves[1][x]], axis=0)
            for n, term in enumerate(parts_of(both, 3)):
                pay_ref[n * REQ + s * CT : n * REQ + (s + 1) * CT, x * LANES : (x + 1) * LANES] = term


def route(cs_ref, ct_ref, take_ref, code_ref, group):
    cs = cs_ref[...]
    ct = ct_ref[...]
    dest = (high(cs, 4) * NG + high(ct, 4)).astype(F32)
    code = (low(cs, 4) * TL + low(ct, 4) + 1).astype(F32)
    wide = dot(dest.astype(BF16), onehot(iota((CT, REQ), 1) % CT == iota((CT, REQ), 0)))
    wide = jnp.where(iota((LOC, REQ), 1) // CT == iota((LOC, REQ), 0), wide, 0.0)
    dest_t = dot(jnp.ones((ND, LOC), BF16), wide.astype(BF16))
    to_me = dest_t == iota((ND, REQ), 0).astype(F32)
    rank = dot(onehot(to_me), onehot(iota((REQ, REQ), 0) < iota((REQ, REQ), 1)))
    takes = [onehot(to_me & (rank == float(r))) for r in range(CAP)]
    for r in range(CAP):
        for n in range(3):
            take_ref[r * ND : (r + 1) * ND, n * REQ : (n + 1) * REQ] = takes[r]
    tall = dot(onehot(iota((REQ, LOC), 0) // CT == iota((REQ, LOC), 1)), code.astype(BF16))
    tall = jnp.where(iota((REQ, CT), 0) % CT == iota((REQ, CT), 1), tall, 0.0)
    code_b = dot(tall.astype(BF16), jnp.ones((CT, LANES), BF16))
    target = high(code_b.astype(I32) - 1, 4).astype(F32)
    source = (iota((REQ, LANES), 0) // CT).astype(F32)
    lane = iota((REQ, LANES), 1)
    codes = jnp.where(lane < 16, source, jnp.where(lane < 32, target, code_b)).astype(BF16)
    lane = iota((ND, LANES), 1)
    row = jnp.zeros((ND, LANES), F32)
    for r in range(CAP):
        at = group * CAP + r
        here = (lane == at) | (lane == 16 + at) | (lane == 32 + r)
        row = jnp.where(here, dot(takes[r], codes), row)
    code_ref[...] = row


def pack(take_ref, pay_ref, msg_ref):
    got = dot(take_ref[...], pay_ref[...])
    for r in range(CAP):
        for x in range(3):
            msg_ref[x, pl.ds(r, ND, stride=CAP), :] = got[r * ND : (r + 1) * ND, x * LANES : (x + 1) * LANES]


def tile_table(pc_ref, sm_ref, table_ref, group):
    point = (group * TL + iota((TL, LANES), 0)) * LANES + iota((TL, LANES), 1)

    @pl.loop(0, LOC)
    def _(s):
        valid = point < pc_ref[s]
        at = pl.multiple_of(s * TL, TL)
        for x in range(6):
            value = sm_ref[s, x]
            if x >= 3:
                value = jnp.where(valid, value, 0.0)
            for n, term in enumerate(parts_of(value, 3)):
                table_ref[pl.ds(n * LOC * TL + at, TL), x * LANES : (x + 1) * LANES] = term


def fetch_tiles(code_ref, table_ref, tile_ref, note_ref):
    codes = code_ref[...].astype(BF16)
    spread = dot(onehot(iota((SLOTS, ND), 0) // CAP == iota((SLOTS, ND), 1)), codes)
    spread = jnp.where(iota((SLOTS, LANES), 1) == 32 + iota((SLOTS, LANES), 0) % CAP, spread, 0.0)
    wanted = dot(spread.astype(BF16), jnp.ones((LANES, LOC * TL), BF16))
    take = onehot(wanted == (iota((SLOTS, LOC * TL), 1) + 1).astype(F32))
    tile_ref[...] = dot(jnp.concatenate([take] * 3, axis=1), table_ref[...])
    here = iota((ND, ND), 0)
    note_ref[...] = dot(onehot((here // 4 == iota((ND, ND), 1) // 4) & (here % 4 == 3)), codes)


def fold(a, b, clear, shift):
    return jnp.where(clear, a, b) + pltpu.roll(jnp.where(clear, b, a), shift, 0)


def group_sums(group, recv_ref, tile_ref, note_ref, left_ref, right_ref, back_ref):
    at = pl.multiple_of(group * LANES, LANES)
    p = [recv_ref[x, pl.ds(at, LANES), :] for x in range(3)]
    tile = [tile_ref[pl.ds(at, LANES), x * LANES : (x + 1) * LANES] for x in range(6)]
    q, n = tile[:3], tile[3:]
    counts = p[0] < 0.5 * FAR
    p[0] = jnp.where(counts, p[0], 0.0)
    res = n[0] * (p[0] - q[0]) + n[1] * (p[1] - q[1]) + n[2] * (p[2] - q[2])
    w = jnp.where(counts, 1.0 / (1.0 + res * res), 0.0)
    jac = [
        p[1] * n[2] - p[2] * n[1],
        p[2] * n[0] - p[0] * n[2],
        p[0] * n[1] - p[1] * n[0],
        n[0],
        n[1],
        n[2],
    ]
    for i in range(6):
        big, small = parts_of(w * jac[i], 2)
        for r in range(8):
            for k, term in enumerate((big, big, small)):
                left_ref[r, i * 16 : (i + 1) * 16, k * LANES : (k + 1) * LANES] = term[r * 16 : (r + 1) * 16]
    for j, value in enumerate(jac + [res]):
        big, small = parts_of(value, 2)
        spots = [j] + {4: [9], 5: [8], 6: [15]}.get(j, [])
        for r in range(8):
            for k, term in enumerate((big, small, big)):
                for spot in spots:
                    right_ref[r, spot * 16 : (spot + 1) * 16, k * LANES : (k + 1) * LANES] = term[r * 16 : (r + 1) * 16]
    lane = iota((8, LANES), 1)
    sub = iota((8, LANES), 0)
    spot = lane // 16
    first = [spot < 8, (spot >= 1) & (spot <= 6), (spot >= 2) & (spot <= 6), spot < 8]
    other = [None, 5, 4, None]
    for chip in range(4):
        arrays = []
        for c in range(2):
            r = chip * 2 + c
            every = dot_t(left_ref[r], right_ref[r])
            for i in range(4):
                kept = jnp.zeros((8, LANES), F32)
                for h in range(2):
                    value = every[i * 16 + h * 8 : i * 16 + h * 8 + 8, :LANES]
                    if other[i] is not None:
                        o = other[i] * 16 + h * 8
                        value = jnp.where(first[i], value, every[o : o + 8, LANES:])
                    kept = jnp.where(lane % 16 == h * 8 + sub, value, kept)
                arrays.append(kept)
        for level in range(3):
            clear = (sub // (1 << level)) % 2 == 0
            arrays = [fold(arrays[n], arrays[n + 1], clear, 1 << level) for n in range(0, len(arrays), 2)]
        note = note_ref[pl.ds(group * 32 + chip * 8, 8), :]
        back_ref[chip * 4 + low(group - chip + 4, 2)] = jnp.where((sub % 4 == 3) & (spot < 3), note, arrays[0])


def turn(blocks, signs, turn_ref, at):
    lane = iota((8, LANES), 1)
    for bit in range(3):
        shift = 16 << bit
        clear = (lane // shift) % 2 == 0
        for m in range(8):
            if (m >> bit) % 2 == 0:
                a, b = blocks[m], blocks[m + (1 << bit)]
                blocks[m] = jnp.where(clear, a, pltpu.roll(b, shift, 1))
                blocks[m + (1 << bit)] = jnp.where(clear, pltpu.roll(a, LANES - shift, 1), b)
    for n in range(8):
        turn_ref[at, n] = jnp.where(lane < 64, blocks[n], -blocks[n]) if signs and n >= 6 else blocks[n]


def arrange(turn_ref, count, signs, owner_ref, sums_ref, column_ref):
    lane = iota((1, LANES), 1)
    y = (lane // 16) % 4
    half = count * LANES
    for t in range(count):
        source = turn_ref[t, 0]
        target = turn_ref[t, 1]
        for c in range(2):
            s = source[c * 4 + 3 : c * 4 + 4, :]
            b = target[c * 4 + 3 : c * 4 + 4, :]
            owner = jnp.broadcast_to(jnp.where(lane < 64, s, b) if signs else s, (LOC, LANES))
            at = c * half + t * LANES
            owner_ref[:, at : at + LANES] = onehot(owner == iota((LOC, LANES), 0).astype(F32))
            if column_ref is not None:
                column = jnp.where(lane < 64, b, s) + (16 * (2 * y + c)).astype(F32)
                there = jnp.broadcast_to(column, (LANES, LANES)) == iota((LANES, LANES), 0).astype(F32)
                there = jnp.where(there, -1.0, 0.0).astype(BF16)
                for n in range(2):
                    column_ref[:, n * 2 * half + at : n * 2 * half + at + LANES] = there
        for p in range(0, 8, 2):
            pair = jnp.concatenate([turn_ref[t, p], turn_ref[t, p + 1]], axis=0)
            for n, term in enumerate(parts_of(pair, 2)):
                sums_ref[p * 8 : p * 8 + 16, n * half + t * LANES : n * half + (t + 1) * LANES] = term


def scan_sums(count, owner_ref, sums_ref):
    half = count * LANES
    owners = [jnp.concatenate([owner_ref[:, c * half : (c + 1) * half]] * 2, axis=1) for c in range(2)]
    both = dot_t(jnp.concatenate(owners, axis=0), sums_ref[:, : 2 * half])
    lane = iota((LOC, 64), 1)
    part = jnp.where((lane // 4) % 2 == 0, both[:LOC], both[LOC:])
    return jnp.concatenate([part, jnp.zeros((LOC, LANES - 64), F32)], axis=1)


def matrix(owner_ref, sums_ref, column_ref, lhs_ref, block_ref):
    for k, pair in enumerate(PAIRS):
        i, p = SPOT[pair]
        for c in range(2):
            at = p * 8 + c * 4 + i
            mine = owner_ref[:, c * HALF : (c + 1) * HALF]
            for n in range(2):
                row = sums_ref[at : at + 1, n * HALF : (n + 1) * HALF]
                lhs_ref[k * LOC : (k + 1) * LOC, (2 * n + c) * HALF : (2 * n + c + 1) * HALF] = (
                    jnp.broadcast_to(row, (LOC, HALF)) * mine
                )
    block_ref[...] = dot_t(lhs_ref[...], column_ref[...])


def far(p):
    return 2 * (1 - low(p, 1)) + low(p + high(p, 1), 1)


def order(p):
    return 2 * high(p, 1) + low(p + high(p, 1), 1)


def step_kernel(
    pc_any, cs_any, ct_any, src_any, sm_any, block_ref, part_ref,
    pc_ref, cs_ref, ct_ref, src_ref, sm_ref, take_ref, pay_ref, code_ref, msg_ref, codes_ref, recv_ref, table_ref, tile_ref,
    note_ref, left_ref, right_ref, back_ref, mid_ref, out_ref, in_ref, last_ref, turn_ref, owner_ref, sums_ref, column_ref, lhs_ref,
    load_sem, send_n, send_p, recv_n, recv_p, send_a, recv_a, send_l, recv_l, send_b, recv_b, send_c, recv_c,
):
    row = lax.axis_index("scan")
    col = lax.axis_index("grp")
    z, y, core = high(row, 3), low(high(row, 1), 2), low(row, 1)
    me = row * NG + col
    chip = high(row, 1)
    group = low(y + z, 2)
    place = group * 32 + z * 8 + core * NG + col
    barrier = pltpu.get_barrier_semaphore()
    loads = [
        pltpu.make_async_copy(a, b, load_sem.at[n])
        for n, (a, b) in enumerate(
            [
                (cs_any, cs_ref),
                (ct_any, ct_ref),
                (src_any, src_ref),
                (pc_any, pc_ref),
                (sm_any.at[:, pl.ds(0, 3)], sm_ref.at[:, pl.ds(0, 3)]),
                (sm_any.at[:, pl.ds(3, 3)], sm_ref.at[:, pl.ds(3, 3)]),
            ]
        )
    ]
    for load in loads:
        load.start()

    def to_some(first, last, act):
        @pl.loop(first, last)
        def _(u):
            dz = low(u + 2 + 2 * core + col, 2)
            uz = low(z + dz, 2)
            uy = low(y + order(high(u, 2)) - dz + 4, 2)
            for dx in (2, 1, 3, 0):
                for dc in (1, 0):
                    there = ((uz * 4 + uy) * 2 + low(core + dc, 1), low(col + dx, 2))
                    if dc == 0 and dx == 0:

                        @pl.when(jnp.logical_or(u >= 4, dz != 0))
                        def _():
                            act(*there)

                    else:
                        act(*there)

    @pl.loop(0, 16)
    def _(u):
        far_z = low(z + far(high(u, 2)), 2)
        far_y = low(y + far(low(u, 2)), 2)
        for dx in (2, 1, 3, 0):
            for dc in (1, 0):

                def greet():
                    there = ((far_z * 4 + far_y) * 2 + low(core + dc, 1), low(col + dx, 2))
                    pl.semaphore_signal(barrier, inc=1, device_id=there, device_id_type=MESH)

                if dc == 0 and dx == 0:
                    pl.when(u < 15)(greet)
                else:
                    greet()


    def send_codes(r, c):
        pltpu.make_async_remote_copy(
            src_ref=code_ref.at[pl.ds(r * NG + c, 1)],
            dst_ref=codes_ref.at[pl.ds(place, 1)],
            send_sem=send_n,
            recv_sem=recv_n,
            device_id=(r, c),
            device_id_type=MESH,
        ).start()

    def send_points(r, c):
        for x in range(3):
            pltpu.make_async_remote_copy(
                src_ref=msg_ref.at[x, pl.ds((r * NG + c) * CAP, CAP)],
                dst_ref=recv_ref.at[x, pl.ds(place * CAP, CAP)],
                send_sem=send_p,
                recv_sem=recv_p.at[group],
                device_id=(r, c),
                device_id_type=MESH,
            ).start()

    for n in range(5):
        loads[n].wait()
    route(cs_ref, ct_ref, take_ref, code_ref, col)
    pick_points(pc_ref, src_ref, sm_ref, pay_ref, col)
    pack(take_ref, pay_ref, msg_ref)
    pl.semaphore_wait(barrier, ND - 1)
    to_some(0, 4, send_points)
    to_some(0, 16, send_codes)
    to_some(4, 16, send_points)
    pltpu.make_async_copy(code_ref.at[pl.ds(me, 1)], codes_ref.at[pl.ds(place, 1)], recv_n).start()
    pltpu.make_async_copy(
        msg_ref.at[:, pl.ds(me * CAP, CAP)], recv_ref.at[:, pl.ds(place * CAP, CAP)], recv_p.at[group]
    ).start()

    loads[5].wait()
    tile_table(pc_ref, sm_ref, table_ref, col)
    for spot in (7, 10, 11, 12, 13, 14):
        right_ref[:, spot * 16 : (spot + 1) * 16, :] = jnp.zeros((8, 16, 3 * LANES), BF16)
    pltpu.make_async_copy(codes_ref, codes_ref, recv_n).wait()
    fetch_tiles(codes_ref, table_ref, tile_ref, note_ref)

    def cross_all(block_of, which, got, kind):
        for plane in range(PLANES):
            at = low(which - plane + 4, 2)
            src = block_of(plane, at)

            @pl.when(plane != col)
            def _():
                pltpu.make_async_remote_copy(
                    src_ref=src,
                    dst_ref=got.at[col * 4 + at],
                    send_sem=send_b.at[kind, plane],
                    recv_sem=recv_b.at[kind, col],
                    device_id=(row, plane),
                    device_id_type=MESH,
                ).start()

            @pl.when(plane == col)
            def _():
                pltpu.make_async_copy(src, got.at[plane * 4 + at], recv_b.at[kind, plane]).start()

    def serve(u):
        which = low(group - order(u) + 4, 2)
        arrived = recv_ref.at[:, pl.ds(which * LANES, LANES)]
        pltpu.make_async_copy(arrived, arrived, recv_p.at[which]).wait()
        group_sums(which, recv_ref, tile_ref, note_ref, left_ref, right_ref, back_ref)
        return which

    @pl.loop(0, PLANES - 1)
    def _(u):
        which = serve(u)
        for n in range(8):
            to_z = n // 2
            to_chip = to_z * 4 + low(which - to_z + 4, 2)
            to_row = to_chip * 2 + n % 2
            src = back_ref.at[to_chip, pl.ds(n % 2 * 4, 4)]
            dst = mid_ref.at[group * 4 + z, pl.ds(core * 4, 4)]

            @pl.when(to_row != row)
            def _():
                pltpu.make_async_remote_copy(
                    src_ref=src,
                    dst_ref=dst,
                    send_sem=send_a,
                    recv_sem=recv_a.at[group],
                    device_id=(to_row, col),
                    device_id_type=MESH,
                ).start()

            @pl.when(to_row == row)
            def _():
                pltpu.make_async_copy(src, dst, recv_a.at[group]).start()

        cross_all(lambda plane, at: back_ref.at[plane * 4 + at], which, in_ref, 0)

    which = serve(PLANES - 1)
    for n in range(8):
        to_z = n // 2
        to_chip = to_z * 4 + low(which - to_z + 4, 2)
        for step in (2, 1, 3, 0):
            pltpu.make_async_remote_copy(
                src_ref=back_ref.at[to_chip, pl.ds(n % 2 * 4, 4)],
                dst_ref=last_ref.at[col * 4 + z, pl.ds(core * 4, 4)],
                send_sem=send_l,
                recv_sem=recv_l,
                device_id=(to_chip * 2 + n % 2, low(col + step, 2)),
                device_id_type=MESH,
            ).start()
    cross_all(lambda plane, at: back_ref.at[plane * 4 + at], which, in_ref, 0)

    @pl.loop(0, PLANES - 1)
    def _(u):
        which = low(group + order(u), 2)
        arrived = mid_ref.at[pl.ds(which * 4, 4)]
        pltpu.make_async_copy(arrived, arrived, recv_a.at[which]).wait()
        cross_all(lambda plane, at: mid_ref.at[which * 4 + plane], which, out_ref, 1)

    def spread(to_col, at):
        return pltpu.make_async_remote_copy(
            src_ref=part_ref.at[col],
            dst_ref=part_ref.at[at],
            send_sem=send_c.at[to_col],
            recv_sem=recv_c.at[at],
            device_id=(row, to_col),
            device_id_type=MESH,
        )

    late = low(group + order(PLANES - 1), 2)
    for m in range(4):
        mid_ref[late * 4 + m] = jnp.zeros((8, LANES), F32)
    for t in range(PLANES):
        turn([ref[t * 4 + m] for ref in (mid_ref, back_ref) for m in range(4)], True, turn_ref, t)
    arrange(turn_ref, PLANES, True, owner_ref, sums_ref, None)
    part_ref[col] = scan_sums(PLANES, owner_ref, sums_ref)
    for step in (2, 1, 3):
        spread(low(col + step, 2), col).start()

    left = code_ref.at[pl.ds(0, ND - 1)]
    pltpu.make_async_copy(left, left, send_n).wait()
    left = msg_ref.at[:, pl.ds(0, (ND - 1) * CAP)]
    pltpu.make_async_copy(left, left, send_p).wait()
    for left in (back_ref.at[pl.ds(0, 11)], back_ref.at[11, pl.ds(0, 4)]):
        pltpu.make_async_copy(left, left, send_a).wait()
    pltpu.make_async_copy(last_ref, last_ref, send_l).wait()

    for source in range(NG):
        arrived = in_ref.at[pl.ds(source * 4, 4)]
        pltpu.make_async_copy(arrived, arrived, recv_b.at[0, source]).wait()
        arrived = out_ref.at[pl.ds(source * 4, 3)]
        pltpu.make_async_copy(arrived, arrived, recv_b.at[1, source]).wait()
    pltpu.make_async_copy(last_ref, last_ref, recv_l).wait()
    for t in range(PLANES):
        out_ref[t * 4 + low(late - col + 4, 2)] = last_ref[t * 4 + col]
    for t in range(2):
        turn([last_ref[t * 8 + m] for m in range(8)], False, turn_ref, t)
    arrange(turn_ref, 2, False, owner_ref, sums_ref, None)
    part_ref[NG] = scan_sums(2, owner_ref, sums_ref)
    for t in range(PLANES):
        turn([ref[t * 4 + m] for ref in (out_ref, in_ref) for m in range(4)], True, turn_ref, t)
    arrange(turn_ref, PLANES, True, owner_ref, sums_ref, column_ref)
    matrix(owner_ref, sums_ref, column_ref, lhs_ref, block_ref)
    for step in range(1, NG):
        other = low(col + step, 2)
        for kind in range(2):
            left = back_ref.at[pl.ds(0, 4 - kind)]
            pltpu.make_async_copy(left, left, send_b.at[kind, other]).wait()
        spread(other, col).wait_send()
        spread(other, other).wait_recv()


def finish_kernel(block_ref, part_ref, hess_any, grad_ref, hess_ref, sem):
    row = lax.axis_index("scan")
    col = lax.axis_index("grp")
    total = part_ref[0] + part_ref[1] + part_ref[2] + part_ref[3] + part_ref[4]
    total = total + pltpu.roll(total, LANES - 4, 1)
    lane = iota((LOC, LANES), 1)
    diag = (lane == iota((LOC, LANES), 0) + LOC * (row % 8)) & (row // 8 == col)
    for k, (i, j) in enumerate(PAIRS):
        at = SPOT[i, j][1] * 8 + SPOT[i, j][0]
        value = block_ref[k * LOC : (k + 1) * LOC, :] + jnp.where(
            diag, jnp.broadcast_to(total[:, at : at + 1], (LOC, LANES)), 0.0
        )
        hess_ref[i, j] = value
        if i != j:
            hess_ref[j, i] = value
        if j == 5:
            pltpu.make_async_copy(hess_ref.at[i], hess_any.at[i], sem.at[i]).start()
    some = jnp.zeros((4, LANES), F32)
    for n in range(NG):
        some = jnp.where(col == n, total[n * 4 : (n + 1) * 4, :], some)
    at = [SPOT[i, 6][1] * 8 + SPOT[i, 6][0] for i in range(6)]
    grad_ref[...] = jnp.concatenate([some[:, a : a + 1] for a in at], axis=1)
    for i in range(6):
        pltpu.make_async_copy(hess_ref.at[i], hess_any.at[i], sem.at[i]).wait()


def vmem(count):
    return [pl.BlockSpec(memory_space=pltpu.VMEM)] * count


def local(samples, point_count, corr_scan, corr_tile, corr_src):
    dma = pltpu.SemaphoreType.DMA
    block, parts = pl.pallas_call(
        step_kernel,
        out_shape=(
            pltpu.VMEM((len(PAIRS) * LOC, LANES), F32),
            pltpu.VMEM((NG + 1, LOC, LANES), F32),
        ),
        in_specs=[pl.BlockSpec(memory_space=pl.ANY)] * 5,
        out_specs=tuple(vmem(2)),
        scratch_shapes=[
            pltpu.SMEM((LOC,), I32),
            pltpu.VMEM((LOC, CT), I32),
            pltpu.VMEM((LOC, CT), I32),
            pltpu.VMEM((LOC, CT, LANES), I32),
            pltpu.VMEM((LOC, 6, TL, LANES), F32),
            pltpu.VMEM((SLOTS, 3 * REQ), BF16),
            pltpu.VMEM((3 * REQ, 3 * LANES), BF16),
            pltpu.VMEM((ND, LANES), F32),
            pltpu.VMEM((3, SLOTS, LANES), F32),
            pltpu.VMEM((ND, LANES), F32),
            pltpu.VMEM((3, SLOTS, LANES), F32),
            pltpu.VMEM((3 * LOC * TL, 6 * LANES), BF16),
            pltpu.VMEM((SLOTS, 6 * LANES), F32),
            pltpu.VMEM((ND, LANES), F32),
            pltpu.VMEM((8, 6 * 16, 3 * LANES), BF16),
            pltpu.VMEM((8, 16 * 16, 3 * LANES), BF16),
            pltpu.VMEM((16, 8, LANES), F32),
            pltpu.VMEM((16, 8, LANES), F32),
            pltpu.VMEM((16, 8, LANES), F32),
            pltpu.VMEM((16, 8, LANES), F32),
            pltpu.VMEM((16, 8, LANES), F32),
            pltpu.VMEM((PLANES, 8, 8, LANES), F32),
            pltpu.VMEM((LOC, 2 * HALF), BF16),
            pltpu.VMEM((64, 2 * HALF), BF16),
            pltpu.VMEM((LANES, 4 * HALF), BF16),
            pltpu.VMEM((len(PAIRS) * LOC, 4 * HALF), BF16),
            dma((6,)),
            dma,
            dma,
            dma,
            dma((PLANES,)),
            dma,
            dma((PLANES,)),
            dma,
            dma,
            dma((2, NG)),
            dma((2, NG)),
            dma((NG,)),
            dma((NG,)),
        ],
        compiler_params=pltpu.CompilerParams(collective_id=0, has_side_effects=True),
        name="step",
    )(point_count, corr_scan, corr_tile, corr_src, samples.transpose(0, 2, 1, 3))
    hessian, gradient = pl.pallas_call(
        finish_kernel,
        out_shape=(
            jax.ShapeDtypeStruct((6, 6, LOC, LANES), F32),
            jax.ShapeDtypeStruct((4, 6), F32),
        ),
        in_specs=vmem(2),
        out_specs=(pl.BlockSpec(memory_space=pl.ANY), *vmem(1)),
        scratch_shapes=[pltpu.VMEM((6, 6, LOC, LANES), F32), pltpu.SemaphoreType.DMA((6,))],
        compiler_params=pltpu.CompilerParams(vmem_limit_bytes=8 * 1024 * 1024),
        name="finish",
    )(block, parts)
    return hessian.transpose(2, 0, 1, 3), gradient


def solution(mesh):
    placed = (
        P("scan", "grp", None, None),
        P("scan"),
        P("scan", "grp"),
        P("scan", "grp"),
        P("scan", "grp", None),
    )
    return jax.shard_map(
        local,
        mesh=mesh,
        in_specs=placed,
        out_specs=(P("scan", None, None, "grp"), P(("scan", "grp"), None)),
        check_vma=False,
    )
```

```python
import functools

import jax
import jax.numpy as jnp
from jax import lax
from jax.experimental import pallas as pl
from jax.experimental.pallas import tpu as pltpu
from jax.sharding import PartitionSpec as P

F32 = jnp.float32
BF16 = jnp.bfloat16
I32 = jnp.int32
MESH = pl.DeviceIdType.MESH

NS = 32
NG = 4
ND = NS * NG
LOC = 16
TL = 16
CT = 16
REQ = LOC * CT
CAP = 4
FAR = 1000.0
LANES = 128
PAIRS = [(i, j) for i in range(6) for j in range(i, 6)]
PLANES = 4
SLOTS = ND * CAP
HALF = PLANES * LANES
SPOT = {(i, j): (i, j) for i in range(4) for j in range(i, 7)}
SPOT |= {(5, 5): (1, 0), (5, 6): (1, 7), (4, 4): (2, 1), (4, 5): (2, 0), (4, 6): (2, 7)}


def iota(shape, dim):
    return lax.broadcasted_iota(I32, shape, dim)


def dot(a, b):
    return lax.dot_general(a, b, (((1,), (0,)), ((), ())), preferred_element_type=F32)


def dot_t(a, b):
    return lax.dot_general(a, b, (((1,), (1,)), ((), ())), preferred_element_type=F32)


def parts_of(x, count):
    terms = []
    for _ in range(count):
        term = x.astype(BF16)
        terms.append(term)
        x = x - term.astype(F32)
    return terms


def onehot(cond):
    return jnp.where(cond, 1.0, 0.0).astype(BF16)


def low(x, bits):
    return lax.bitwise_and(x, (1 << bits) - 1)


def high(x, bits):
    return lax.shift_right_logical(x, bits)


def pick_points(pc_ref, src_ref, sm_ref, pay_ref, group):
    first = group * (TL * LANES)
    for s in range(LOC):
        picks = src_ref[s]
        halves = []
        for h in range(2):
            part = picks[h * 8 : h * 8 + 8]
            tile = high(part, 7)
            lane = low(part, 7)
            acc = [jnp.zeros((8, LANES), F32) for _ in range(3)]
            for t in range(TL):
                here = tile == t
                for x in range(3):
                    row = jnp.broadcast_to(sm_ref[s, x, t : t + 1, :], (8, LANES))
                    got = jnp.take_along_axis(row, lane, axis=1, mode="promise_in_bounds")
                    acc[x] = jnp.where(here, got, acc[x])
            acc[0] = jnp.where(first + part < pc_ref[s], acc[0], FAR)
            halves.append(acc)
        for x in range(3):
            both = jnp.concatenate([halves[0][x], halves[1][x]], axis=0)
            for n, term in enumerate(parts_of(both, 3)):
                pay_ref[n * REQ + s * CT : n * REQ + (s + 1) * CT, x * LANES : (x + 1) * LANES] = term


def route(cs_ref, ct_ref, take_ref, code_ref, group):
    cs = cs_ref[...]
    ct = ct_ref[...]
    dest = (high(cs, 4) * NG + high(ct, 4)).astype(F32)
    code = (low(cs, 4) * TL + low(ct, 4) + 1).astype(F32)
    wide = dot(dest.astype(BF16), onehot(iota((CT, REQ), 1) % CT == iota((CT, REQ), 0)))
    wide = jnp.where(iota((LOC, REQ), 1) // CT == iota((LOC, REQ), 0), wide, 0.0)
    dest_t = dot(jnp.ones((ND, LOC), BF16), wide.astype(BF16))
    to_me = dest_t == iota((ND, REQ), 0).astype(F32)
    rank = dot(onehot(to_me), onehot(iota((REQ, REQ), 0) < iota((REQ, REQ), 1)))
    takes = [onehot(to_me & (rank == float(r))) for r in range(CAP)]
    for r in range(CAP):
        for n in range(3):
            take_ref[r * ND : (r + 1) * ND, n * REQ : (n + 1) * REQ] = takes[r]
    tall = dot(onehot(iota((REQ, LOC), 0) // CT == iota((REQ, LOC), 1)), code.astype(BF16))
    tall = jnp.where(iota((REQ, CT), 0) % CT == iota((REQ, CT), 1), tall, 0.0)
    code_b = dot(tall.astype(BF16), jnp.ones((CT, LANES), BF16))
    target = high(code_b.astype(I32) - 1, 4).astype(F32)
    source = (iota((REQ, LANES), 0) // CT).astype(F32)
    lane = iota((REQ, LANES), 1)
    codes = jnp.where(lane < 16, source, jnp.where(lane < 32, target, code_b)).astype(BF16)
    lane = iota((ND, LANES), 1)
    row = jnp.zeros((ND, LANES), F32)
    for r in range(CAP):
        at = group * CAP + r
        here = (lane == at) | (lane == 16 + at) | (lane == 32 + r)
        row = jnp.where(here, dot(takes[r], codes), row)
    code_ref[...] = row


def pack(take_ref, pay_ref, msg_ref):
    got = dot(take_ref[...], pay_ref[...])
    for r in range(CAP):
        for x in range(3):
            msg_ref[x, pl.ds(r, ND, stride=CAP), :] = got[r * ND : (r + 1) * ND, x * LANES : (x + 1) * LANES]


def tile_table(pc_ref, sm_ref, table_ref, group):
    point = (group * TL + iota((TL, LANES), 0)) * LANES + iota((TL, LANES), 1)

    @pl.loop(0, LOC)
    def _(s):
        valid = point < pc_ref[s]
        at = pl.multiple_of(s * TL, TL)
        for x in range(6):
            value = sm_ref[s, x]
            if x >= 3:
                value = jnp.where(valid, value, 0.0)
            for n, term in enumerate(parts_of(value, 3)):
                table_ref[pl.ds(n * LOC * TL + at, TL), x * LANES : (x + 1) * LANES] = term


def fetch_tiles(code_ref, table_ref, tile_ref, note_ref):
    codes = code_ref[...].astype(BF16)
    spread = dot(onehot(iota((SLOTS, ND), 0) // CAP == iota((SLOTS, ND), 1)), codes)
    spread = jnp.where(iota((SLOTS, LANES), 1) == 32 + iota((SLOTS, LANES), 0) % CAP, spread, 0.0)
    wanted = dot(spread.astype(BF16), jnp.ones((LANES, LOC * TL), BF16))
    take = onehot(wanted == (iota((SLOTS, LOC * TL), 1) + 1).astype(F32))
    tile_ref[...] = dot(jnp.concatenate([take] * 3, axis=1), table_ref[...])
    here = iota((ND, ND), 0)
    note_ref[...] = dot(onehot((here // 4 == iota((ND, ND), 1) // 4) & (here % 4 == 3)), codes)


def fold(a, b, clear, shift):
    return jnp.where(clear, a, b) + pltpu.roll(jnp.where(clear, b, a), shift, 0)


def group_sums(group, recv_ref, tile_ref, note_ref, left_ref, right_ref, back_ref):
    at = pl.multiple_of(group * LANES, LANES)
    p = [recv_ref[x, pl.ds(at, LANES), :] for x in range(3)]
    tile = [tile_ref[pl.ds(at, LANES), x * LANES : (x + 1) * LANES] for x in range(6)]
    q, n = tile[:3], tile[3:]
    counts = p[0] < 0.5 * FAR
    p[0] = jnp.where(counts, p[0], 0.0)
    res = n[0] * (p[0] - q[0]) + n[1] * (p[1] - q[1]) + n[2] * (p[2] - q[2])
    w = jnp.where(counts, 1.0 / (1.0 + res * res), 0.0)
    jac = [
        p[1] * n[2] - p[2] * n[1],
        p[2] * n[0] - p[0] * n[2],
        p[0] * n[1] - p[1] * n[0],
        n[0],
        n[1],
        n[2],
    ]
    for i in range(6):
        big, small = parts_of(w * jac[i], 2)
        for r in range(8):
            for k, term in enumerate((big, big, small)):
                left_ref[r, i * 16 : (i + 1) * 16, k * LANES : (k + 1) * LANES] = term[r * 16 : (r + 1) * 16]
    for j, value in enumerate(jac + [res]):
        big, small = parts_of(value, 2)
        spots = [j] + {4: [9], 5: [8], 6: [15]}.get(j, [])
        for r in range(8):
            for k, term in enumerate((big, small, big)):
                for spot in spots:
                    right_ref[r, spot * 16 : (spot + 1) * 16, k * LANES : (k + 1) * LANES] = term[r * 16 : (r + 1) * 16]
    lane = iota((8, LANES), 1)
    sub = iota((8, LANES), 0)
    spot = lane // 16
    first = [spot < 8, (spot >= 1) & (spot <= 6), (spot >= 2) & (spot <= 6), spot < 8]
    other = [None, 5, 4, None]
    for chip in range(4):
        arrays = []
        for c in range(2):
            r = chip * 2 + c
            every = dot_t(left_ref[r], right_ref[r])
            for i in range(4):
                kept = jnp.zeros((8, LANES), F32)
                for h in range(2):
                    value = every[i * 16 + h * 8 : i * 16 + h * 8 + 8, :LANES]
                    if other[i] is not None:
                        o = other[i] * 16 + h * 8
                        value = jnp.where(first[i], value, every[o : o + 8, LANES:])
                    kept = jnp.where(lane % 16 == h * 8 + sub, value, kept)
                arrays.append(kept)
        for level in range(3):
            clear = (sub // (1 << level)) % 2 == 0
            arrays = [fold(arrays[n], arrays[n + 1], clear, 1 << level) for n in range(0, len(arrays), 2)]
        note = note_ref[pl.ds(group * 32 + chip * 8, 8), :]
        back_ref[chip * 4 + low(group - chip + 4, 2)] = jnp.where((sub % 4 == 3) & (spot < 3), note, arrays[0])


def turn(blocks, signs, turn_ref, at):
    lane = iota((8, LANES), 1)
    for bit in range(3):
        shift = 16 << bit
        clear = (lane // shift) % 2 == 0
        for m in range(8):
            if (m >> bit) % 2 == 0:
                a, b = blocks[m], blocks[m + (1 << bit)]
                blocks[m] = jnp.where(clear, a, pltpu.roll(b, shift, 1))
                blocks[m + (1 << bit)] = jnp.where(clear, pltpu.roll(a, LANES - shift, 1), b)
    for n in range(8):
        turn_ref[at, n] = jnp.where(lane < 64, blocks[n], -blocks[n]) if signs and n >= 6 else blocks[n]


def arrange(turn_ref, count, signs, owner_ref, sums_ref, column_ref):
    lane = iota((1, LANES), 1)
    y = (lane // 16) % 4
    half = count * LANES
    for t in range(count):
        source = turn_ref[t, 0]
        target = turn_ref[t, 1]
        for c in range(2):
            s = source[c * 4 + 3 : c * 4 + 4, :]
            b = target[c * 4 + 3 : c * 4 + 4, :]
            owner = jnp.broadcast_to(jnp.where(lane < 64, s, b) if signs else s, (LOC, LANES))
            at = c * half + t * LANES
            owner_ref[:, at : at + LANES] = onehot(owner == iota((LOC, LANES), 0).astype(F32))
            if column_ref is not None:
                column = jnp.where(lane < 64, b, s) + (16 * (2 * y + c)).astype(F32)
                there = jnp.broadcast_to(column, (LANES, LANES)) == iota((LANES, LANES), 0).astype(F32)
                there = jnp.where(there, -1.0, 0.0).astype(BF16)
                for n in range(2):
                    column_ref[:, n * 2 * half + at : n * 2 * half + at + LANES] = there
        for p in range(0, 8, 2):
            pair = jnp.concatenate([turn_ref[t, p], turn_ref[t, p + 1]], axis=0)
            for n, term in enumerate(parts_of(pair, 2)):
                sums_ref[p * 8 : p * 8 + 16, n * half + t * LANES : n * half + (t + 1) * LANES] = term


def scan_sums(count, owner_ref, sums_ref):
    half = count * LANES
    owners = [jnp.concatenate([owner_ref[:, c * half : (c + 1) * half]] * 2, axis=1) for c in range(2)]
    both = dot_t(jnp.concatenate(owners, axis=0), sums_ref[:, : 2 * half])
    lane = iota((LOC, 64), 1)
    part = jnp.where((lane // 4) % 2 == 0, both[:LOC], both[LOC:])
    return jnp.concatenate([part, jnp.zeros((LOC, LANES - 64), F32)], axis=1)


def matrix(owner_ref, sums_ref, column_ref, lhs_ref, block_ref):
    for k, pair in enumerate(PAIRS):
        i, p = SPOT[pair]
        for c in range(2):
            at = p * 8 + c * 4 + i
            mine = owner_ref[:, c * HALF : (c + 1) * HALF]
            for n in range(2):
                row = sums_ref[at : at + 1, n * HALF : (n + 1) * HALF]
                lhs_ref[k * LOC : (k + 1) * LOC, (2 * n + c) * HALF : (2 * n + c + 1) * HALF] = (
                    jnp.broadcast_to(row, (LOC, HALF)) * mine
                )
    block_ref[...] = dot_t(lhs_ref[...], column_ref[...])


def far(p):
    return 2 * (1 - low(p, 1)) + low(p + high(p, 1), 1)


def order(p):
    return 2 * high(p, 1) + low(p + high(p, 1), 1)


def step_kernel(
    pc_any, cs_any, ct_any, src_any, sm_any, block_ref, part_ref,
    pc_ref, cs_ref, ct_ref, src_ref, sm_ref, take_ref, pay_ref, code_ref, msg_ref, codes_ref, recv_ref, table_ref, tile_ref,
    note_ref, left_ref, right_ref, back_ref, mid_ref, out_ref, in_ref, last_ref, turn_ref, owner_ref, sums_ref, column_ref, lhs_ref,
    load_sem, send_n, send_p, recv_n, recv_p, send_a, recv_a, send_l, recv_l, send_b, recv_b, send_c, recv_c,
):
    row = lax.axis_index("scan")
    col = lax.axis_index("grp")
    z, y, core = high(row, 3), low(high(row, 1), 2), low(row, 1)
    me = row * NG + col
    chip = high(row, 1)
    group = low(y + z, 2)
    place = group * 32 + z * 8 + core * NG + col
    barrier = pltpu.get_barrier_semaphore()
    loads = [
        pltpu.make_async_copy(a, b, load_sem.at[n])
        for n, (a, b) in enumerate(
            [
                (cs_any, cs_ref),
                (ct_any, ct_ref),
                (src_any, src_ref),
                (pc_any, pc_ref),
                (sm_any.at[:, pl.ds(0, 3)], sm_ref.at[:, pl.ds(0, 3)]),
                (sm_any.at[:, pl.ds(3, 3)], sm_ref.at[:, pl.ds(3, 3)]),
            ]
        )
    ]
    for load in loads:
        load.start()

    def to_some(first, last, act):
        @pl.loop(first, last)
        def _(u):
            dz = low(u + 2 + core + col, 2)
            uz = low(z + dz, 2)
            uy = low(y + order(high(u, 2)) - dz + 4, 2)
            for dx in (2, 1, 3, 0):
                for dc in (1, 0):
                    there = ((uz * 4 + uy) * 2 + low(core + dc, 1), low(col + dx, 2))
                    if dc == 0 and dx == 0:

                        @pl.when(jnp.logical_or(u >= 4, dz != 0))
                        def _():
                            act(*there)

                    else:
                        act(*there)

    @pl.loop(0, 16)
    def _(u):
        far_z = low(z + far(high(u, 2)), 2)
        far_y = low(y + far(low(u, 2)), 2)
        for dx in (2, 1, 3, 0):
            for dc in (1, 0):

                def greet():
                    there = ((far_z * 4 + far_y) * 2 + low(core + dc, 1), low(col + dx, 2))
                    pl.semaphore_signal(barrier, inc=1, device_id=there, device_id_type=MESH)

                if dc == 0 and dx == 0:
                    pl.when(u < 15)(greet)
                else:
                    greet()


    def send_codes(r, c):
        pltpu.make_async_remote_copy(
            src_ref=code_ref.at[pl.ds(r * NG + c, 1)],
            dst_ref=codes_ref.at[pl.ds(place, 1)],
            send_sem=send_n,
            recv_sem=recv_n,
            device_id=(r, c),
            device_id_type=MESH,
        ).start()

    def send_points(r, c):
        for x in range(3):
            pltpu.make_async_remote_copy(
                src_ref=msg_ref.at[x, pl.ds((r * NG + c) * CAP, CAP)],
                dst_ref=recv_ref.at[x, pl.ds(place * CAP, CAP)],
                send_sem=send_p,
                recv_sem=recv_p.at[group],
                device_id=(r, c),
                device_id_type=MESH,
            ).start()

    for n in range(5):
        loads[n].wait()
    route(cs_ref, ct_ref, take_ref, code_ref, col)
    pick_points(pc_ref, src_ref, sm_ref, pay_ref, col)
    pack(take_ref, pay_ref, msg_ref)
    pl.semaphore_wait(barrier, ND - 1)
    to_some(0, 4, send_points)
    to_some(0, 16, send_codes)
    to_some(4, 16, send_points)
    pltpu.make_async_copy(code_ref.at[pl.ds(me, 1)], codes_ref.at[pl.ds(place, 1)], recv_n).start()
    pltpu.make_async_copy(
        msg_ref.at[:, pl.ds(me * CAP, CAP)], recv_ref.at[:, pl.ds(place * CAP, CAP)], recv_p.at[group]
    ).start()

    loads[5].wait()
    tile_table(pc_ref, sm_ref, table_ref, col)
    for spot in (7, 10, 11, 12, 13, 14):
        right_ref[:, spot * 16 : (spot + 1) * 16, :] = jnp.zeros((8, 16, 3 * LANES), BF16)
    pltpu.make_async_copy(codes_ref, codes_ref, recv_n).wait()
    fetch_tiles(codes_ref, table_ref, tile_ref, note_ref)

    def cross_all(block_of, which, got, kind):
        for plane in range(PLANES):
            at = low(which - plane + 4, 2)
            src = block_of(plane, at)

            @pl.when(plane != col)
            def _():
                pltpu.make_async_remote_copy(
                    src_ref=src,
                    dst_ref=got.at[col * 4 + at],
                    send_sem=send_b.at[kind, plane],
                    recv_sem=recv_b.at[kind, col],
                    device_id=(row, plane),
                    device_id_type=MESH,
                ).start()

            @pl.when(plane == col)
            def _():
                pltpu.make_async_copy(src, got.at[plane * 4 + at], recv_b.at[kind, plane]).start()

    def serve(u):
        which = low(group - order(u) + 4, 2)
        arrived = recv_ref.at[:, pl.ds(which * LANES, LANES)]
        pltpu.make_async_copy(arrived, arrived, recv_p.at[which]).wait()
        group_sums(which, recv_ref, tile_ref, note_ref, left_ref, right_ref, back_ref)
        return which

    @pl.loop(0, PLANES - 1)
    def _(u):
        which = serve(u)
        for n in range(8):
            to_z = n // 2
            to_chip = to_z * 4 + low(which - to_z + 4, 2)
            to_row = to_chip * 2 + n % 2
            src = back_ref.at[to_chip, pl.ds(n % 2 * 4, 4)]
            dst = mid_ref.at[group * 4 + z, pl.ds(core * 4, 4)]

            @pl.when(to_row != row)
            def _():
                pltpu.make_async_remote_copy(
                    src_ref=src,
                    dst_ref=dst,
                    send_sem=send_a,
                    recv_sem=recv_a.at[group],
                    device_id=(to_row, col),
                    device_id_type=MESH,
                ).start()

            @pl.when(to_row == row)
            def _():
                pltpu.make_async_copy(src, dst, recv_a.at[group]).start()

        cross_all(lambda plane, at: back_ref.at[plane * 4 + at], which, in_ref, 0)

    which = serve(PLANES - 1)
    for n in range(8):
        to_z = n // 2
        to_chip = to_z * 4 + low(which - to_z + 4, 2)
        for step in (2, 1, 3, 0):
            pltpu.make_async_remote_copy(
                src_ref=back_ref.at[to_chip, pl.ds(n % 2 * 4, 4)],
                dst_ref=last_ref.at[col * 4 + z, pl.ds(core * 4, 4)],
                send_sem=send_l,
                recv_sem=recv_l,
                device_id=(to_chip * 2 + n % 2, low(col + step, 2)),
                device_id_type=MESH,
            ).start()
    cross_all(lambda plane, at: back_ref.at[plane * 4 + at], which, in_ref, 0)

    @pl.loop(0, PLANES - 1)
    def _(u):
        which = low(group + order(u), 2)
        arrived = mid_ref.at[pl.ds(which * 4, 4)]
        pltpu.make_async_copy(arrived, arrived, recv_a.at[which]).wait()
        cross_all(lambda plane, at: mid_ref.at[which * 4 + plane], which, out_ref, 1)

    def spread(to_col, at):
        return pltpu.make_async_remote_copy(
            src_ref=part_ref.at[col],
            dst_ref=part_ref.at[at],
            send_sem=send_c.at[to_col],
            recv_sem=recv_c.at[at],
            device_id=(row, to_col),
            device_id_type=MESH,
        )

    late = low(group + order(PLANES - 1), 2)
    for m in range(4):
        mid_ref[late * 4 + m] = jnp.zeros((8, LANES), F32)
    for t in range(PLANES):
        turn([ref[t * 4 + m] for ref in (mid_ref, back_ref) for m in range(4)], True, turn_ref, t)
    arrange(turn_ref, PLANES, True, owner_ref, sums_ref, None)
    part_ref[col] = scan_sums(PLANES, owner_ref, sums_ref)
    for step in (2, 1, 3):
        spread(low(col + step, 2), col).start()

    left = code_ref.at[pl.ds(0, ND - 1)]
    pltpu.make_async_copy(left, left, send_n).wait()
    left = msg_ref.at[:, pl.ds(0, (ND - 1) * CAP)]
    pltpu.make_async_copy(left, left, send_p).wait()
    for left in (back_ref.at[pl.ds(0, 11)], back_ref.at[11, pl.ds(0, 4)]):
        pltpu.make_async_copy(left, left, send_a).wait()
    pltpu.make_async_copy(last_ref, last_ref, send_l).wait()

    for source in range(NG):
        arrived = in_ref.at[pl.ds(source * 4, 4)]
        pltpu.make_async_copy(arrived, arrived, recv_b.at[0, source]).wait()
        arrived = out_ref.at[pl.ds(source * 4, 3)]
        pltpu.make_async_copy(arrived, arrived, recv_b.at[1, source]).wait()
    pltpu.make_async_copy(last_ref, last_ref, recv_l).wait()
    for t in range(PLANES):
        out_ref[t * 4 + low(late - col + 4, 2)] = last_ref[t * 4 + col]
    for t in range(2):
        turn([last_ref[t * 8 + m] for m in range(8)], False, turn_ref, t)
    arrange(turn_ref, 2, False, owner_ref, sums_ref, None)
    part_ref[NG] = scan_sums(2, owner_ref, sums_ref)
    for t in range(PLANES):
        turn([ref[t * 4 + m] for ref in (out_ref, in_ref) for m in range(4)], True, turn_ref, t)
    arrange(turn_ref, PLANES, True, owner_ref, sums_ref, column_ref)
    matrix(owner_ref, sums_ref, column_ref, lhs_ref, block_ref)
    for step in range(1, NG):
        other = low(col + step, 2)
        for kind in range(2):
            left = back_ref.at[pl.ds(0, 4 - kind)]
            pltpu.make_async_copy(left, left, send_b.at[kind, other]).wait()
        spread(other, col).wait_send()
        spread(other, other).wait_recv()


def finish_kernel(block_ref, part_ref, hess_ref, grad_ref):
    row = lax.axis_index("scan")
    col = lax.axis_index("grp")
    total = part_ref[0] + part_ref[1] + part_ref[2] + part_ref[3] + part_ref[4]
    total = total + pltpu.roll(total, LANES - 4, 1)
    lane = iota((LOC, LANES), 1)
    diag = (lane == iota((LOC, LANES), 0) + LOC * (row % 8)) & (row // 8 == col)
    for k, (i, j) in enumerate(PAIRS):
        at = SPOT[i, j][1] * 8 + SPOT[i, j][0]
        value = block_ref[k * LOC : (k + 1) * LOC, :] + jnp.where(
            diag, jnp.broadcast_to(total[:, at : at + 1], (LOC, LANES)), 0.0
        )
        hess_ref[i, j] = value
        if i != j:
            hess_ref[j, i] = value
    some = jnp.zeros((4, LANES), F32)
    for n in range(NG):
        some = jnp.where(col == n, total[n * 4 : (n + 1) * 4, :], some)
    at = [SPOT[i, 6][1] * 8 + SPOT[i, 6][0] for i in range(6)]
    grad_ref[...] = jnp.concatenate([some[:, a : a + 1] for a in at], axis=1)


def vmem(count):
    return [pl.BlockSpec(memory_space=pltpu.VMEM)] * count


def local(samples, point_count, corr_scan, corr_tile, corr_src):
    dma = pltpu.SemaphoreType.DMA
    block, parts = pl.pallas_call(
        step_kernel,
        out_shape=(
            pltpu.VMEM((len(PAIRS) * LOC, LANES), F32),
            pltpu.VMEM((NG + 1, LOC, LANES), F32),
        ),
        in_specs=[pl.BlockSpec(memory_space=pl.ANY)] * 5,
        out_specs=tuple(vmem(2)),
        scratch_shapes=[
            pltpu.SMEM((LOC,), I32),
            pltpu.VMEM((LOC, CT), I32),
            pltpu.VMEM((LOC, CT), I32),
            pltpu.VMEM((LOC, CT, LANES), I32),
            pltpu.VMEM((LOC, 6, TL, LANES), F32),
            pltpu.VMEM((SLOTS, 3 * REQ), BF16),
            pltpu.VMEM((3 * REQ, 3 * LANES), BF16),
            pltpu.VMEM((ND, LANES), F32),
            pltpu.VMEM((3, SLOTS, LANES), F32),
            pltpu.VMEM((ND, LANES), F32),
            pltpu.VMEM((3, SLOTS, LANES), F32),
            pltpu.VMEM((3 * LOC * TL, 6 * LANES), BF16),
            pltpu.VMEM((SLOTS, 6 * LANES), F32),
            pltpu.VMEM((ND, LANES), F32),
            pltpu.VMEM((8, 6 * 16, 3 * LANES), BF16),
            pltpu.VMEM((8, 16 * 16, 3 * LANES), BF16),
            pltpu.VMEM((16, 8, LANES), F32),
            pltpu.VMEM((16, 8, LANES), F32),
            pltpu.VMEM((16, 8, LANES), F32),
            pltpu.VMEM((16, 8, LANES), F32),
            pltpu.VMEM((16, 8, LANES), F32),
            pltpu.VMEM((PLANES, 8, 8, LANES), F32),
            pltpu.VMEM((LOC, 2 * HALF), BF16),
            pltpu.VMEM((64, 2 * HALF), BF16),
            pltpu.VMEM((LANES, 4 * HALF), BF16),
            pltpu.VMEM((len(PAIRS) * LOC, 4 * HALF), BF16),
            dma((6,)),
            dma,
            dma,
            dma,
            dma((PLANES,)),
            dma,
            dma((PLANES,)),
            dma,
            dma,
            dma((2, NG)),
            dma((2, NG)),
            dma((NG,)),
            dma((NG,)),
        ],
        compiler_params=pltpu.CompilerParams(collective_id=0, has_side_effects=True),
        name="step",
    )(point_count, corr_scan, corr_tile, corr_src, samples.transpose(0, 2, 1, 3))
    hessian, gradient = pl.pallas_call(
        finish_kernel,
        out_shape=(
            jax.ShapeDtypeStruct((6, 6, LOC, LANES), F32),
            jax.ShapeDtypeStruct((4, 6), F32),
        ),
        in_specs=vmem(2),
        out_specs=tuple(vmem(2)),
        compiler_params=pltpu.CompilerParams(vmem_limit_bytes=8 * 1024 * 1024),
        name="finish",
    )(block, parts)
    return hessian.transpose(2, 0, 1, 3), gradient


def solution(mesh):
    placed = (
        P("scan", "grp", None, None),
        P("scan"),
        P("scan", "grp"),
        P("scan", "grp"),
        P("scan", "grp", None),
    )
    return jax.shard_map(
        local,
        mesh=mesh,
        in_specs=placed,
        out_specs=(P("scan", None, None, "grp"), P(("scan", "grp"), None)),
        check_vma=False,
    )
```
